32 devices in a mesh: wide: 8 (over y, x, core), narrow: 4 (over z).
Axes of the slice: x: 2, y: 2, z: 4, core: 2. Of those that a mesh axis runs over, the one named last changes fastest.
Arguments:
- inputs: bfloat16 [3152, 1024], P('wide', 'narrow'), may hold values from -6 to 6
- norm_gain: float32 [2, 2, 1024], P(None, None, 'narrow'), may hold values from 0.5 to 1.5
- norm_bias: float32 [2, 2, 1024], P(None, None, 'narrow'), may hold values from -3 to 3
- w_qkv: bfloat16 [2, 1024, 3, 1024], P(None, 'wide', None, 'narrow')
- b_qv: float32 [2, 2, 1024], P(None, None, 'narrow'), may hold values from -3 to 3
- w_out: bfloat16 [2, 1024, 1024], P(None, 'narrow', 'wide'), may hold values from -0.75 to 0.75
- b_out: float32 [2, 1024], P(None, 'narrow'), may hold values from -3 to 3
- w_up: bfloat16 [2, 1024, 4096], P(None, 'wide', 'narrow'), may hold values from -0.1875 to 0.1875
- b_up: float32 [2, 4096], P(None, 'narrow'), may hold values from -3 to 3
- w_down: bfloat16 [2, 4096, 1024], P(None, 'narrow', 'wide'), may hold values from -0.09375 to 0.09375
- b_down: float32 [2, 1024], P(None, 'narrow'), may hold values from -3 to 3
- cotangent: bfloat16 [3152, 1024], P('wide', 'narrow'), may hold values from -6 to 6
Outputs:
- output: float32 [3152, 1024], P('wide', 'narrow')
- grad_input: float32 [3152, 1024], P('wide', 'narrow')
- grad_norm_gain: float32 [2, 2, 1024], P(None, None, 'narrow')
- grad_norm_bias: float32 [2, 2, 1024], P(None, None, 'narrow')
- grad_w_qkv: float32 [2, 1024, 3, 1024], P(None, 'wide', None, 'narrow')
- grad_b_qv: float32 [2, 2, 1024], P(None, None, 'narrow')
- grad_w_out: float32 [2, 1024, 1024], P(None, 'narrow', 'wide')
- grad_b_out: float32 [2, 1024], P(None, 'narrow')
- grad_w_up: float32 [2, 1024, 4096], P(None, 'wide', 'narrow')
- grad_b_up: float32 [2, 4096], P(None, 'narrow')
- grad_w_down: float32 [2, 4096, 1024], P(None, 'narrow', 'wide')
- grad_b_down: float32 [2, 1024], P(None, 'narrow')
The draws below stay inside these ranges and needn't reach their ends.
All inputs are finite; a program needn't handle non-finite values.
Results may differ from the reference program's by a relative error of at most 0.014.
Values may be sent and summed in bfloat16 or wider, within the bound.
A program may use at most 128 MiB of HBM per device.

```python
import math
import jax
import jax.numpy as jnp
from jax import lax

D = 1024
HEAD_DIM = 64
FF = 4096
SEQ = 197
LAYERS = 2
IMG_DEV = 2
TOKENS = 3152
N_WIDE = 8


def draw_w_qkv(key, part):
    sampled = jax.random.truncated_normal(key, -6.0, 6.0, (LAYERS, D, 3, D), jnp.float32) / math.sqrt(D)
    return sampled.astype(jnp.bfloat16)


def steps_of(stream_key, extent, shards, smallest, largest):
    loudness = 1.0
    for dim, parts in shards:
        heights = jax.random.uniform(jax.random.fold_in(jax.random.fold_in(stream_key, 6), dim), (parts,), jnp.float32, smallest / len(shards), largest / len(shards))
        loudness = loudness * jnp.repeat(jnp.exp(heights), extent[dim] // parts).reshape((-1,) + (1,) * (len(extent) - 1 - dim))
    return loudness


def centred(key, extent, deviation, most, cuts=(), held_as=jnp.bfloat16):
    drawn = jax.random.normal(key, extent, jnp.float32) * deviation
    if len(cuts) > 0:
        drawn = steps_of(key, extent, cuts, -0.22, 0.18) * drawn
    return jnp.clip(drawn, min=-most, max=most).astype(held_as)


def setup_inputs(seed: int = 0) -> dict:
    arg_keys = jax.random.split(jax.random.key(seed), 13)
    inputs = centred(arg_keys[0], (TOKENS, D), 1.0, 6.0, ((0, 8), (1, 4)))
    norm_gain = jnp.clip(1.0 + 0.1 * jax.random.normal(arg_keys[1], (LAYERS, 2, D), jnp.float32), 0.5, 1.5)
    norm_bias = centred(arg_keys[2], (LAYERS, 2, D), 0.5, 3.0, ((2, 4),), jnp.float32)
    w_qkv = draw_w_qkv(jax.random.fold_in(arg_keys[12], 71), 0)
    b_qv = centred(arg_keys[4], (LAYERS, 2, D), 0.5, 3.0, ((2, 4),), jnp.float32)
    w_out = centred(arg_keys[5], (LAYERS, D, D), (D // 16) ** -0.5, 0.75, ((1, 4), (2, 8)))
    b_out = centred(arg_keys[6], (LAYERS, D), 0.5, 3.0, ((1, 4),), jnp.float32)
    w_up = centred(arg_keys[7], (LAYERS, D, FF), D ** -0.5, 0.1875, ((1, 8), (2, 4)))
    b_up = centred(arg_keys[8], (LAYERS, FF), 0.5, 3.0, ((1, 4),), jnp.float32)
    w_down = centred(arg_keys[9], (LAYERS, FF, D), FF ** -0.5, 0.09375, ((1, 4), (2, 8)))
    b_down = centred(arg_keys[10], (LAYERS, D), 0.5, 3.0, ((1, 4),), jnp.float32)
    cotangent = centred(arg_keys[11], (TOKENS, D), 1.0, 6.0, ((0, 8), (1, 4)))
    return dict(inputs=inputs, norm_gain=norm_gain, norm_bias=norm_bias, w_qkv=w_qkv, b_qv=b_qv, w_out=w_out, b_out=b_out, w_up=w_up, b_up=b_up, w_down=w_down, b_down=b_down, cotangent=cotangent)


eps = 1e-06

def gelu_value(pre_act):
    return 0.5 * pre_act * (1.0 + lax.erf(pre_act * 0.7071067811865476))

def gelu_slope(pre_act):
    normal_cdf = 0.5 * (1.0 + lax.erf(pre_act * 0.7071067811865476))
    return normal_cdf + pre_act * jnp.exp(-0.5 * pre_act * pre_act) * 0.3989422804014327

def contract_rows(former, latter):
    return lax.dot_general(former, latter, (((0,), (0,)), ((), ())), preferred_element_type=jnp.float32)

def times_transpose(former, latter):
    return lax.dot_general(former, latter, (((1,), (1,)), ((), ())), preferred_element_type=jnp.float32)

def norm_forward(residual, gain_row, shift_row):
    center = lax.optimization_barrier(jnp.sum(residual, axis=1)) / D
    spread = lax.rsqrt(lax.optimization_barrier(jnp.sum(residual * residual, axis=1)) / D - center * center + eps)
    normed = (residual - center[:, None]) * spread[:, None]
    return (normed, spread, (normed * gain_row + shift_row).astype(jnp.bfloat16))

def norm_backward(upstream, normed, spread, gain_row):
    scaled = upstream * gain_row
    first_sum = lax.optimization_barrier(jnp.sum(scaled, axis=1)) / D
    second_sum = lax.optimization_barrier(jnp.sum(scaled * normed, axis=1)) / D
    corrected = scaled - first_sum[:, None] - normed * second_sum[:, None]
    return (corrected * spread[:, None], lax.optimization_barrier(jnp.sum(upstream * normed, axis=0)), lax.optimization_barrier(jnp.sum(upstream, axis=0)))

def split_heads(matrix):
    images = matrix.shape[0] // SEQ
    return matrix.reshape(images, SEQ, matrix.shape[1] // HEAD_DIM, HEAD_DIM)

def attention_forward(queries, key_rows, values):
    factor = 1.0 / math.sqrt(HEAD_DIM)
    scores = jnp.einsum('ishd,ithd->ihst', split_heads(queries), split_heads(key_rows), preferred_element_type=jnp.float32) * factor
    row_max = lax.optimization_barrier(jnp.max(scores, axis=-1, keepdims=True))
    logsum = row_max + jnp.log(lax.optimization_barrier(jnp.sum(jnp.exp(scores - row_max), axis=-1, keepdims=True)))
    rounded_p = jnp.exp(scores - logsum).astype(jnp.bfloat16)
    attended = jnp.einsum('ihst,ithd->ishd', rounded_p, split_heads(values), preferred_element_type=jnp.float32)
    return (attended.reshape(queries.shape).astype(jnp.bfloat16), logsum)

def attention_backward(queries, key_rows, values, logsum, grad_mixed):
    factor = 1.0 / math.sqrt(HEAD_DIM)
    query_heads = split_heads(queries)
    key_heads = split_heads(key_rows)
    value_heads = split_heads(values)
    grad_heads = split_heads(grad_mixed)
    scores = jnp.einsum('ishd,ithd->ihst', query_heads, key_heads, preferred_element_type=jnp.float32) * factor
    probability = jnp.exp(scores - logsum)
    rounded_p = probability.astype(jnp.bfloat16)
    grad_values = jnp.einsum('ihst,ishd->ithd', rounded_p, grad_heads, preferred_element_type=jnp.float32)
    grad_probs = jnp.einsum('ishd,ithd->ihst', grad_heads, value_heads, preferred_element_type=jnp.float32)
    row_dot = lax.optimization_barrier(jnp.sum(probability * grad_probs, axis=-1, keepdims=True))
    grad_scores = (probability * (grad_probs - row_dot) * factor).astype(jnp.bfloat16)
    grad_queries = jnp.einsum('ihst,ithd->ishd', grad_scores, key_heads, preferred_element_type=jnp.float32)
    grad_keys = jnp.einsum('ihst,ishd->ithd', grad_scores, query_heads, preferred_element_type=jnp.float32)
    flat_shape = queries.shape
    return (grad_queries.reshape(flat_shape), grad_keys.reshape(flat_shape), grad_values.reshape(flat_shape))

def one_group(params, group_inputs, group_upstream):
    norm_gain, norm_bias, w_qkv, b_qv, w_out, b_out, w_up, b_up, w_down, b_down = params
    residual = group_inputs.astype(jnp.float32)
    stored = []
    for number in range(LAYERS):
        normed_one, spread_one, act_one = norm_forward(residual, norm_gain[number, 0], norm_bias[number, 0])
        queries = (jnp.dot(act_one, w_qkv[number, :, 0, :], preferred_element_type=jnp.float32) + b_qv[number, 0]).astype(jnp.bfloat16)
        key_rows = jnp.dot(act_one, w_qkv[number, :, 1, :], preferred_element_type=jnp.float32).astype(jnp.bfloat16)
        values = (jnp.dot(act_one, w_qkv[number, :, 2, :], preferred_element_type=jnp.float32) + b_qv[number, 1]).astype(jnp.bfloat16)
        attended, logsum = attention_forward(queries, key_rows, values)
        middle = residual + (jnp.dot(attended, w_out[number], preferred_element_type=jnp.float32) + b_out[number])
        normed_two, spread_two, act_two = norm_forward(middle, norm_gain[number, 1], norm_bias[number, 1])
        pre_hidden = jnp.dot(act_two, w_up[number], preferred_element_type=jnp.float32) + b_up[number]
        hidden = gelu_value(pre_hidden).astype(jnp.bfloat16)
        stored.append((normed_one, spread_one, act_one, queries, key_rows, values, attended, logsum, normed_two, spread_two, act_two, pre_hidden, hidden))
        residual = middle + (jnp.dot(hidden, w_down[number], preferred_element_type=jnp.float32) + b_down[number])
    upstream = group_upstream.astype(jnp.float32)
    collected = [[None] * LAYERS for member in range(10)]
    for number in reversed(range(LAYERS)):
        normed_one, spread_one, act_one, queries, key_rows, values, attended, logsum, normed_two, spread_two, act_two, pre_hidden, hidden = stored[number]
        grad_rounded = upstream.astype(jnp.bfloat16)
        collected[8][number] = contract_rows(hidden, grad_rounded)
        collected[9][number] = lax.optimization_barrier(jnp.sum(upstream, axis=0))
        grad_pre = times_transpose(grad_rounded, w_down[number]) * gelu_slope(pre_hidden)
        collected[7][number] = lax.optimization_barrier(jnp.sum(grad_pre, axis=0))
        grad_pre_b = grad_pre.astype(jnp.bfloat16)
        collected[6][number] = contract_rows(act_two, grad_pre_b)
        grad_act_two = times_transpose(grad_pre_b, w_up[number])
        grad_norm_two, gain_two, shift_two = norm_backward(grad_act_two, normed_two, spread_two, norm_gain[number, 1])
        grad_middle = upstream + grad_norm_two
        middle_rounded = grad_middle.astype(jnp.bfloat16)
        collected[4][number] = contract_rows(attended, middle_rounded)
        collected[5][number] = lax.optimization_barrier(jnp.sum(grad_middle, axis=0))
        grad_mixed = times_transpose(middle_rounded, w_out[number]).astype(jnp.bfloat16)
        grad_queries, grad_keys, grad_values = attention_backward(queries, key_rows, values, logsum, grad_mixed)
        collected[3][number] = jnp.stack([lax.optimization_barrier(jnp.sum(grad_queries, axis=0)), lax.optimization_barrier(jnp.sum(grad_values, axis=0))])
        grad_parts = [grad_queries.astype(jnp.bfloat16), grad_keys.astype(jnp.bfloat16), grad_values.astype(jnp.bfloat16)]
        collected[2][number] = jnp.stack([contract_rows(act_one, grad_part) for grad_part in grad_parts], axis=1)
        grad_act_one = times_transpose(grad_parts[0], w_qkv[number, :, 0, :])
        grad_act_one = grad_act_one + times_transpose(grad_parts[1], w_qkv[number, :, 1, :])
        grad_act_one = grad_act_one + times_transpose(grad_parts[2], w_qkv[number, :, 2, :])
        grad_norm_one, gain_one, shift_one = norm_backward(grad_act_one, normed_one, spread_one, norm_gain[number, 0])
        collected[0][number] = jnp.stack([gain_one, gain_two])
        collected[1][number] = jnp.stack([shift_one, shift_two])
        upstream = grad_middle + grad_norm_one
    grads = tuple((jnp.stack(member_list) for member_list in collected))
    return (residual, upstream, grads)

def reference(inputs, norm_gain, norm_bias, w_qkv, b_qv, w_out, b_out, w_up, b_up, w_down, b_down, cotangent):
    params = (norm_gain, norm_bias, w_qkv, b_qv, w_out, b_out, w_up, b_up, w_down, b_down)
    group_rows = IMG_DEV * SEQ
    input_groups = inputs.reshape(N_WIDE, group_rows, D)
    upstream_groups = cotangent.reshape(N_WIDE, group_rows, D)
    initial = tuple((jnp.zeros(param_array.shape, jnp.float32) for param_array in params))

    def scan_step(running, pair_rows):
        group_out, group_grad, grads = one_group(params, pair_rows[0], pair_rows[1])
        summed = tuple((first_term + second_term for first_term, second_term in zip(running, grads)))
        return (summed, (group_out, group_grad))
    totals, (outputs, grad_rows) = lax.scan(scan_step, initial, (input_groups, upstream_groups))
    return (outputs.reshape(TOKENS, D), grad_rows.reshape(TOKENS, D), totals[0], totals[1], totals[2], totals[3], totals[4], totals[5], totals[6], totals[7], totals[8], totals[9])
```

```python
import functools
import math

import jax
import jax.numpy as jnp
from jax import lax
from jax.experimental import pallas as pl
from jax.experimental.pallas import tpu as pltpu
from jax.sharding import PartitionSpec as P

D = 1024
HEAD_DIM = 64
SEQ = 197
LAYERS = 2
EPS = 1e-06
ROWS = 208
KEYS = 256
MESH = pl.DeviceIdType.MESH
F32 = jnp.float32
BF16 = jnp.bfloat16
CHUNK = 16
HIGHEST = lax.Precision.HIGHEST

V_GAIN, V_BIAS, V_QV, V_OUT, V_DOWN, V_UP = 0, 2, 4, 6, 7, 8
V_ROWS = 16


def dot(a, b):
    return lax.dot_general(a, b, (((1,), (0,)), ((), ())), preferred_element_type=F32)


def dot_t(a, b):
    return lax.dot_general(a, b, (((1,), (1,)), ((), ())), preferred_element_type=F32)


def t_dot(a, b):
    return lax.dot_general(a, b, (((0,), (0,)), ((), ())), preferred_element_type=F32)


def exact_dot(a, b, dims):
    return lax.dot_general(a, b, (dims, ((), ())), precision=HIGHEST, preferred_element_type=F32)


def when(condition):
    return pl.when(condition)


def scratch_of(half, per_row, width, hidden, images):
    tall = images * ROWS
    dma = pltpu.SemaphoreType.DMA
    vm = pltpu.VMEM
    return dict(
        wa=vm((LAYERS, D, 4 * width), BF16),
        wf=vm((LAYERS, D, 2 * hidden), BF16),
        ga=vm((D, 4 * width), BF16),
        gf=vm((D, 2 * hidden), BF16),
        pa=vm((half, per_row, 4 * width), BF16),
        pf=vm((half, per_row, 2 * hidden), BF16),
        ca=vm((half, per_row, 4 * width), BF16),
        cf=vm((half, per_row, 2 * hidden), BF16),
        x=vm((2, tall, D), BF16),
        e=vm((2 * LAYERS, tall, D), BF16),
        act=vm((2 * LAYERS, tall, D), BF16),
        q=vm((LAYERS, tall, width), BF16),
        k=vm((LAYERS, images * KEYS, width), BF16),
        v=vm((LAYERS, images * KEYS, width), BF16),
        o=vm((LAYERS, tall, width), BF16),
        prob=vm((LAYERS * images * (width // HEAD_DIM), ROWS, KEYS), F32),
        slope=vm((LAYERS, tall, hidden), F32),
        u=vm((LAYERS, tall, hidden), BF16),
        n=vm((2 * LAYERS, tall, width), F32),
        spread=vm((2 * LAYERS, tall, 1), F32),
        centre=vm((tall, 1), F32),
        r=vm((tall, width), F32),
        g=vm((tall, width), F32),
        f=vm((tall, hidden), BF16),
        d=vm((tall, 3 * width), BF16),
        do=vm((ROWS, width), BF16),
        tmp=vm((ROWS, width), F32),
        stage=vm((2, images, 3, ROWS, width), BF16),
        slot=vm((2, images, 4, ROWS, width), BF16),
        held=vm((images, 2, ROWS, width), F32),
        own=vm((2, images, ROWS, width), F32),
        vs=vm((2, KEYS, 128), F32),
        ts=vm((images, 8, KEYS), F32),
        tr=vm((images, 3, 8, KEYS), F32),
        gn=vm((4, 8, width), F32),
        sv=vm((LAYERS, V_ROWS, width), F32),
        rv=vm((LAYERS, 2 * half, V_ROWS, width), F32),
        ag_s=dma((4, images, 4)),
        ag_r=dma((4, images, 3)),
        rs_s=dma((2, images, 3)),
        rs_r=dma((2, images, 4)),
        t_s=dma((images, 3)),
        t_r=dma((images, 3)),
        gn_s=dma((3,)),
        gn_r=dma((3,)),
        w_l=dma((LAYERS, 2)),
        w_s=dma((LAYERS, 2, half + 1)),
        w_r=dma((LAYERS, 2, half)),
        w_f=dma((LAYERS, 2, half)),
        w_g=dma((LAYERS, 2, half)),
        p_s=dma((2, half)),
        p_r=dma((2, half)),
        c_s=dma((2, half)),
        c_r=dma((2, half)),
        v_s=dma((LAYERS, 2 * half)),
        v_r=dma((LAYERS, 2 * half)),
    )


IN_NAMES = ("x_in", "cot_in", "gb_in", "bq_in", "bo_in", "bu_in", "bd_in", "wa_in", "wf_in")
OUT_NAMES = ("out", "gin", "gwa", "gwf", "gv")


def kernel(wide, images, width, hidden, names, *refs):
    R = dict(zip(names, refs))
    half = wide // 2
    per_row = D // wide
    heads = width // HEAD_DIM
    w = lax.axis_index("wide")
    z = lax.axis_index("narrow")
    upper = z // 2
    mate = z + 1 - 2 * (z % 2)
    oi = 2 - upper
    oo = 3 * (1 - upper)
    inner_n = (z + upper) % 2
    inner = inner_n == 1
    outer = inner_n == 0
    far = 2 - inner_n
    par = w % 2
    mine = w // 2
    partner = w + 1 - 2 * par

    def rows(i):
        return pl.ds(i * ROWS, ROWS)

    def cols(j):
        return pl.ds(pl.multiple_of(j * width, 128), width)

    def block_rows(j):
        return pl.ds(pl.multiple_of(j * width, 128), width)

    def wrows(j):
        return pl.ds(pl.multiple_of(j * per_row, per_row), per_row)

    def remote(src, dst, s, r, wide_id, narrow_id):
        return pltpu.make_async_remote_copy(
            src_ref=src, dst_ref=dst, send_sem=s, recv_sem=r,
            device_id=(wide_id, narrow_id), device_id_type=MESH,
        )

    def chunks(count, body):
        lax.fori_loop(0, count // CHUNK, lambda c, _: (body(c * CHUNK), 0)[1], 0)

    def at(i, start, size=CHUNK):
        return pl.ds(pl.multiple_of(i * ROWS + start, CHUNK), size)

    def ag_copy(buf, kind, i, block, s, r, to):
        part = buf.at[rows(i), cols(block)]
        return remote(part, part, R["ag_s"].at[kind, i, s], R["ag_r"].at[kind, i, r], w, to)

    def ag_start(buf, kind, i):
        ag_copy(buf, kind, i, z, 0, 0, mate).start()
        ag_copy(buf, kind, i, z, 1, far, oi).start()

    def ag_relay(buf, kind, i):
        @when(inner)
        def _():
            ag_copy(buf, kind, i, oi, 2, 1, mate).wait_recv()
            ag_copy(buf, kind, i, oi, 2, 1, mate).start()
            ag_copy(buf, kind, i, oo, 3, 2, mate).wait_recv()
            ag_copy(buf, kind, i, oo, 3, 2, mate).start()

    def ag_finish(buf, kind, i):
        ag_copy(buf, kind, i, mate, 0, 0, mate).wait_recv()

        @when(outer)
        def _():
            ag_copy(buf, kind, i, oi, 2, 1, mate).wait_recv()
            ag_copy(buf, kind, i, oo, 3, 2, mate).wait_recv()

    def ag_drain(buf, kind, i):
        ag_copy(buf, kind, i, z, 0, 0, mate).wait_send()
        ag_copy(buf, kind, i, z, 1, far, oi).wait_send()

        @when(inner)
        def _():
            ag_copy(buf, kind, i, oi, 2, 1, mate).wait_send()
            ag_copy(buf, kind, i, oo, 3, 2, mate).wait_send()

    def rs_copy(bank, i, q, slot, to):
        return remote(
            R["stage"].at[bank, i, q], R["slot"].at[bank, i, slot],
            R["rs_s"].at[bank, i, q], R["rs_r"].at[bank, i, slot], w, to,
        )

    def rs_blocks(bank, i, block):
        for q, to in ((0, oo), (1, oi)):
            y = block(to)

            @when(outer)
            def _():
                R["stage"][bank, i, q] = y.astype(BF16)
                rs_copy(bank, i, q, q, mate).start()

            @when(inner)
            def _():
                R["held"][i, q] = y

        R["stage"][bank, i, 2] = block(mate).astype(BF16)
        rs_copy(bank, i, 2, 2, mate).start()
        R["own"][bank, i] = block(z)

    def rs_relay(bank, i):
        @when(inner)
        def _():
            for q, to in ((0, oo), (1, oi)):
                rs_copy(bank, i, q, q, mate).wait_recv()

                def body(c):
                    part = pl.ds(pl.multiple_of(c, CHUNK), CHUNK)
                    total = R["held"][i, q, part] + R["slot"][bank, i, q, part].astype(F32)
                    R["stage"][bank, i, q, part] = total.astype(BF16)

                chunks(ROWS, body)
                rs_copy(bank, i, q, 3, to).start()

    def rs_wait(bank, i):
        rs_copy(bank, i, 2, 2, mate).wait_recv()
        rs_copy(bank, i, 0, 3, mate).wait_recv()
        for q in range(3):
            rs_copy(bank, i, q, 2, mate).wait_send()

    def rs_sum(bank, i, part):
        slots = R["slot"]
        return (
            R["own"][bank, i, part]
            + slots[bank, i, 2, part].astype(F32)
            + slots[bank, i, 3, part].astype(F32)
        )

    def t_copy(i, q, r, to):
        return remote(
            R["ts"].at[i], R["tr"].at[i, r], R["t_s"].at[i, q], R["t_r"].at[i, r], w, to
        )

    def t_send(i):
        lane = lax.broadcasted_iota(jnp.int32, (8, 128), 0)
        first = jnp.where(lane < 4, 1.0, 0.0).astype(F32)
        second = 1.0 - first
        R["ts"][i] = exact_dot(first, R["vs"][0], ((1,), (1,))) + exact_dot(
            second, R["vs"][1], ((1,), (1,))
        )
        t_copy(i, 0, 0, mate).start()
        t_copy(i, 1, far, oi).start()
        t_copy(i, 2, far, oo).start()

    def t_total(i):
        for q in range(3):
            t_copy(i, q, q, mate).wait_recv()
        for q in range(3):
            t_copy(i, q, q, mate).wait_send()
        total = (R["ts"][i] + R["tr"][i, 0]) + (R["tr"][i, 1] + R["tr"][i, 2])
        row = lax.broadcasted_iota(jnp.int32, (8, 128), 0)
        lane = lax.broadcasted_iota(jnp.int32, (8, 128), 1)
        pick = ((row == 0) & (lane < 64)) | ((row == 4) & (lane >= 64))
        back = exact_dot(total, jnp.where(pick, 1.0, 0.0).astype(F32), ((0,), (0,)))
        R["vs"][0] = back

    def weights(piece):
        return (R["wa"], R["wa_in"]) if piece == 0 else (R["wf"], R["wf_in"])

    def w_local(l, piece):
        full, shard = weights(piece)
        return pltpu.make_async_copy(shard.at[l], full.at[l, wrows(w)], R["w_l"].at[l, piece])

    def w_send(l, piece, s, to):
        full, shard = weights(piece)
        return remote(
            shard.at[l], full.at[l, wrows(w)],
            R["w_s"].at[l, piece, s], R["w_r"].at[l, piece, mine], to, z,
        )

    def w_cross(l, piece, k):
        full, _ = weights(piece)
        part = full.at[l, wrows(2 * k + par)]
        return remote(
            part, part, R["w_g"].at[l, piece, k], R["w_f"].at[l, piece, k], partner, z
        )

    def w_start(l, piece):
        full, shard = weights(piece)
        for j in range(1, half):
            k = (mine + j) % half
            w_send(l, piece, j - 1, 2 * k + par).start()
        remote(
            shard.at[l], full.at[l, wrows(w)],
            R["w_s"].at[l, piece, half - 1], R["w_f"].at[l, piece, mine], partner, z,
        ).start()
        w_local(l, piece).start()

    def w_relay(l, piece):
        full, shard = weights(piece)
        for j in range(1, half):
            k = (mine + j) % half
            remote(
                shard.at[l], full.at[l, wrows(2 * k + par)],
                R["w_s"].at[l, piece, 0], R["w_r"].at[l, piece, k], partner, z,
            ).wait_recv()
            w_cross(l, piece, k).start()

    def w_finish(l, piece):
        full, shard = weights(piece)
        for j in range(half):
            k = (mine + j) % half
            part = full.at[l, wrows(2 * k + 1 - par)]
            remote(
                part, part, R["w_g"].at[l, piece, k], R["w_f"].at[l, piece, k], partner, z
            ).wait_recv()
        w_local(l, piece).wait()
        for s in range(half):
            w_send(l, piece, s, partner).wait_send()
        for j in range(1, half):
            w_cross(l, piece, (mine + j) % half).wait_send()

    def grads(piece):
        if piece == 0:
            return R["ga"], R["pa"], R["ca"], R["gwa"]
        return R["gf"], R["pf"], R["cf"], R["gwf"]

    def p_copy(piece, k):
        full, theirs, _, _ = grads(piece)
        return remote(
            full.at[wrows(2 * k + 1 - par)], theirs.at[k],
            R["p_s"].at[piece, k], R["p_r"].at[piece, k], partner, z,
        )

    def c_copy(piece, k, source):
        full, _, came, _ = grads(piece)
        return remote(
            full.at[wrows(2 * k + par)], came.at[source],
            R["c_s"].at[piece, k], R["c_r"].at[piece, source], 2 * k + par, z,
        )

    def g_start(piece):
        for k in range(half):
            p_copy(piece, k).start()

    def g_mid(piece):
        full, theirs, _, _ = grads(piece)
        for j in range(1, half + 1):
            k = (mine + j) % half
            p_copy(piece, k).wait_recv()

            def body(c):
                here = pl.ds(pl.multiple_of((2 * k + par) * per_row + c, CHUNK), CHUNK)
                total = full[here].astype(F32) + theirs[
                    k, pl.ds(pl.multiple_of(c, CHUNK), CHUNK)
                ].astype(F32)
                full[here] = total.astype(BF16)

            chunks(per_row, body)
            if j < half:
                c_copy(piece, k, mine).start()

    def g_end(l, piece):
        full, _, came, result = grads(piece)
        for j in range(1, half):
            k = (mine + j) % half
            c_copy(piece, k, k).wait_recv()

        def body(c):
            here = pl.ds(pl.multiple_of(w * per_row + c, CHUNK), CHUNK)
            part = pl.ds(pl.multiple_of(c, CHUNK), CHUNK)
            total = full[here].astype(F32)
            for j in range(1, half):
                total = total + came[(mine + j) % half, part].astype(F32)
            result[l, part] = total

        chunks(per_row, body)
        for k in range(half):
            p_copy(piece, k).wait_send()
        for j in range(1, half):
            c_copy(piece, (mine + j) % half, mine).wait_send()

    def v_copy(l, j, source):
        to = (w + j) % wide
        return remote(
            R["sv"].at[l], R["rv"].at[l, source],
            R["v_s"].at[l, j], R["v_r"].at[l, source], to, z,
        )

    def v_start(l):
        for j in range(1, wide):
            v_copy(l, j, w).start()

    def v_end(l):
        total = R["sv"][l]
        for j in range(1, wide):
            source = (w + j) % wide
            v_copy(l, j, source).wait_recv()
            total = total + R["rv"][l, source]
        R["gv"][l] = total
        for j in range(1, wide):
            v_copy(l, j, w).wait_send()

    def norm_in(buf, l, branch, i):
        at_norm = 2 * l + branch
        scale = [R["gn"][j, pl.ds(2 * l + branch, 1)] for j in range(4)]
        shift = [R["gn"][j, pl.ds(4 + 2 * l + branch, 1)] for j in range(4)]
        scale = jnp.concatenate(scale, axis=1)
        shift = jnp.concatenate(shift, axis=1)

        def body(c):
            here = at(i, c)
            raw = buf[here, :].astype(F32)
            mean = jnp.sum(raw, axis=1, keepdims=True) * (1.0 / D)
            square = jnp.sum(raw * raw, axis=1, keepdims=True) * (1.0 / D)
            s = lax.rsqrt(square - mean * mean + EPS)
            R["act"][at_norm, here] = ((raw - mean) * s * scale + shift).astype(BF16)
            centre = R["centre"][here] + mean
            R["centre"][here] = centre
            R["spread"][at_norm, here] = s
            R["n"][at_norm, here] = (R["r"][here] - centre) * s

        chunks(ROWS, body)

    def norm_back(bank, l, branch, i, v_out_row):
        at_norm = 2 * l + branch
        scale = R["gn"][z, pl.ds(2 * l + branch, 1)]
        rs_wait(bank, i)
        t_total(i)

        def body(c, carry):
            gain_sum, bias_sum, g_sum = carry
            c = c * CHUNK
            here = at(i, c)
            part = pl.ds(pl.multiple_of(c, CHUNK), CHUNK)
            upstream = rs_sum(bank, i, part)
            normed = R["n"][at_norm, here]
            first = R["vs"][0, part, 0:1] * (1.0 / D)
            second = R["vs"][0, part, 64:65] * (1.0 / D)
            grown = R["g"][here] + (upstream * scale - first - normed * second) * R["spread"][
                at_norm, here
            ]
            R["g"][here] = grown
            gain_sum = gain_sum + jnp.sum(upstream * normed, axis=0, keepdims=True)
            bias_sum = bias_sum + jnp.sum(upstream, axis=0, keepdims=True)
            g_sum = g_sum + jnp.sum(grown, axis=0, keepdims=True)
            return gain_sum, bias_sum, g_sum

        zero = jnp.zeros((1, width), F32)
        gain_sum, bias_sum, g_sum = lax.fori_loop(0, ROWS // CHUNK, body, (zero, zero, zero))
        small_add(l, V_GAIN + branch, gain_sum)
        small_add(l, V_BIAS + branch, bias_sum)
        if v_out_row is not None:
            small_add(l, v_out_row, g_sum)

    def small_add(l, row, value):
        R["sv"][l, row : row + 1] = R["sv"][l, row : row + 1] + value

    def send_sums(at_norm, i, block_of):
        R["vs"][0, 0:ROWS] = jnp.zeros((ROWS, 128), F32)
        R["vs"][1, 0:ROWS] = jnp.zeros((ROWS, 128), F32)
        l, branch = at_norm

        def block(j):
            y = block_of(j)
            R["tmp"][...] = y
            scale = R["gn"][j, pl.ds(2 * l + branch, 1)]
            shift = R["gn"][j, pl.ds(4 + 2 * l + branch, 1)]

            def body(c):
                part = pl.ds(pl.multiple_of(c, CHUNK), CHUNK)
                value = R["tmp"][part]
                normed = R["act"][2 * l + branch, at(i, c), cols(j)].astype(F32) - shift
                first = value * scale
                second = value * normed
                for m in range(width // 128):
                    lanes = slice(m * 128, (m + 1) * 128)
                    R["vs"][0, part] = R["vs"][0, part] + first[:, lanes]
                    R["vs"][1, part] = R["vs"][1, part] + second[:, lanes]

            chunks(ROWS, body)
            return R["tmp"][...]

        return block

    def attention(l, i):
        keys = pl.ds(i * KEYS, KEYS)
        column = lax.broadcasted_iota(jnp.int32, (ROWS, KEYS), 1)
        for h in range(heads):
            lanes = slice(h * HEAD_DIM, (h + 1) * HEAD_DIM)
            scores = dot_t(R["q"][l, rows(i), lanes], R["k"][l, keys, lanes]) * (
                1.0 / math.sqrt(HEAD_DIM)
            )
            scores = jnp.where(column < SEQ, scores, -jnp.inf)
            top = jnp.max(scores, axis=1, keepdims=True)
            grown = jnp.exp(scores - top)
            prob = grown / jnp.sum(grown, axis=1, keepdims=True)
            R["prob"][(l * images + i) * heads + h] = prob
            R["o"][l, rows(i), lanes] = dot(prob.astype(BF16), R["v"][l, keys, lanes]).astype(BF16)

    def f1(l, i):
        buf = R["x"].at[0]
        ag_finish(buf, 0, i)
        norm_in(buf, l, 0, i)
        act = R["act"].at[2 * l, rows(i)]
        kept = pl.ds(i * KEYS, ROWS)
        bq = R["bq_in"][pl.ds(2 * l, 1)]
        bv = R["bq_in"][pl.ds(2 * l + 1, 1)]
        R["q"][l, rows(i)] = (dot(act[...], R["wa"][l, :, 0:width]) + bq).astype(BF16)
        R["k"][l, kept] = dot(act[...], R["wa"][l, :, width : 2 * width]).astype(BF16)
        R["v"][l, kept] = (dot(act[...], R["wa"][l, :, 2 * width : 3 * width]) + bv).astype(BF16)
        attention(l, i)

        def block(j):
            return dot_t(R["o"][l, rows(i)], R["wa"][l, block_rows(j), 3 * width : 4 * width])

        rs_blocks(0, i, block)

    def f2(l, i):
        buf = R["x"].at[1]
        ag_finish(buf, 1, i)
        norm_in(buf, l, 1, i)

        def body(b, _):
            lanes = cols(b)
            pre = dot(R["act"][2 * l + 1, rows(i)], R["wf"][l, :, lanes])
            pre = pre + R["bu_in"][pl.ds(l, 1), lanes]
            cdf = 0.5 * (1.0 + lax.erf(pre * 0.7071067811865476))
            R["u"][l, rows(i), lanes] = (pre * cdf).astype(BF16)
            R["slope"][l, rows(i), lanes] = (
                cdf + pre * jnp.exp(-0.5 * pre * pre) * 0.3989422804014327
            )
            return 0

        lax.fori_loop(0, hidden // width, body, 0)

        def block(j):
            return dot_t(R["u"][l, rows(i)], R["wf"][l, block_rows(j), hidden : 2 * hidden])

        rs_blocks(1, i, block)

    def residual(bank, i, bias):
        rs_wait(bank, i)

        def body(c):
            here = at(i, c)
            part = pl.ds(pl.multiple_of(c, CHUNK), CHUNK)
            R["r"][here] = R["r"][here] + (rs_sum(bank, i, part) + bias)

        chunks(ROWS, body)

    def send_residual(kind, i):
        buf = R["x"].at[kind]

        def body(c):
            here = at(i, c)
            buf[here, cols(z)] = (R["r"][here] - R["centre"][here]).astype(BF16)

        chunks(ROWS, body)
        ag_start(buf, kind, i)

    def post_f1(l, i):
        ag_drain(R["x"].at[0], 0, i)
        residual(0, i, R["bo_in"][pl.ds(l, 1)])
        send_residual(1, i)

    def post_f2(l, i, last):
        ag_drain(R["x"].at[1], 1, i)
        residual(1, i, R["bd_in"][pl.ds(l, 1)])
        if last:
            R["out"][rows(i)] = R["r"][rows(i)]
        else:
            send_residual(0, i)

    def send_grad(slot, kind, i):
        buf = R["e"].at[slot]

        def body(c):
            here = at(i, c)
            buf[here, cols(z)] = R["g"][here].astype(BF16)

        chunks(ROWS, body)
        ag_start(buf, kind, i)

    def b2(l, i):
        e = R["e"].at[2 * l + 1]
        ag_finish(e, 2, i)

        def body(b, _):
            lanes = cols(b)
            back = pl.ds(pl.multiple_of(hidden + b * width, 128), width)
            dz = dot(e[rows(i), :], R["wf"][l, :, back]) * R["slope"][l, rows(i), lanes]
            R["f"][rows(i), lanes] = dz.astype(BF16)
            row = pl.ds(V_UP + b, 1)
            R["sv"][l, row] = R["sv"][l, row] + jnp.sum(dz, axis=0, keepdims=True)
            return 0

        lax.fori_loop(0, hidden // width, body, 0)

        def block(j):
            return dot_t(R["f"][rows(i)], R["wf"][l, block_rows(j), 0:hidden])

        rs_blocks(0, i, send_sums((l, 1), i, block))
        t_send(i)

    def b1(l, i):
        e = R["e"].at[2 * l]
        ag_finish(e, 3, i)
        keys = pl.ds(i * KEYS, KEYS)
        R["do"][...] = dot(e[rows(i), :], R["wa"][l, :, 3 * width : 4 * width]).astype(BF16)
        for h in range(heads):
            lanes = slice(h * HEAD_DIM, (h + 1) * HEAD_DIM)
            prob = R["prob"][(l * images + i) * heads + h]
            do = R["do"][:, lanes]
            dv = t_dot(prob.astype(BF16), do)[0:ROWS]
            dp = dot_t(do, R["v"][l, keys, lanes])
            delta = jnp.sum(prob * dp, axis=1, keepdims=True)
            ds = (prob * (dp - delta) * (1.0 / math.sqrt(HEAD_DIM))).astype(BF16)
            dq = dot(ds, R["k"][l, keys, lanes])
            dk = t_dot(ds, R["q"][l, rows(i), lanes])[0:ROWS]
            for part, value in ((0, dq), (1, dk), (2, dv)):
                there = slice(part * width + h * HEAD_DIM, part * width + (h + 1) * HEAD_DIM)
                R["d"][rows(i), there] = value.astype(BF16)
            for row, value in ((V_QV, dq), (V_QV + 1, dv)):
                total = jnp.sum(value, axis=0, keepdims=True)
                R["sv"][l, row : row + 1, lanes] = R["sv"][l, row : row + 1, lanes] + total

        def block(j):
            return dot_t(R["d"][rows(i)], R["wa"][l, block_rows(j), 0 : 3 * width])

        rs_blocks(1, i, send_sums((l, 0), i, block))
        t_send(i)

    def add_down(l, i):
        def body(c, total):
            return total + jnp.sum(R["g"][at(i, c * CHUNK)], axis=0, keepdims=True)

        total = lax.fori_loop(0, ROWS // CHUNK, body, jnp.zeros((1, width), F32))
        small_add(l, V_DOWN, total)

    def post_b2(l, i):
        add_down(l, i)
        ag_drain(R["e"].at[2 * l + 1], 2, i)
        norm_back(0, l, 1, i, V_OUT)
        send_grad(2 * l, 3, i)

    def post_b1(l, i):
        ag_drain(R["e"].at[2 * l], 3, i)
        norm_back(1, l, 0, i, None)

        @when(l > 0)
        def _():
            send_grad(2 * l - 1, 2, i)

        @when(l == 0)
        def _():
            R["gin"][rows(i)] = R["g"][rows(i)]

    def grad_ffn(l, first, last):
        def body(b, _):
            lanes = pl.ds(pl.multiple_of(b * 256, 256), 256)
            up = t_dot(R["act"][2 * l + 1, :, lanes], R["f"][...])
            R["gf"][lanes, 0:hidden] = up.astype(BF16)
            down = t_dot(R["e"][2 * l + 1, :, lanes], R["u"][l])
            R["gf"][lanes, hidden : 2 * hidden] = down.astype(BF16)
            return 0

        lax.fori_loop(first, last, body, 0)

    def grad_attention(l, first, last):
        def body(b, _):
            lanes = pl.ds(pl.multiple_of(b * 256, 256), 256)
            qkv = t_dot(R["act"][2 * l, :, lanes], R["d"][...])
            R["ga"][lanes, 0 : 3 * width] = qkv.astype(BF16)
            out = t_dot(R["e"][2 * l, :, lanes], R["o"][l])
            R["ga"][lanes, 3 * width : 4 * width] = out.astype(BF16)
            return 0

        lax.fori_loop(first, last, body, 0)

    barrier = pltpu.get_barrier_semaphore()
    for j in range(1, 4):
        pl.semaphore_signal(barrier, 1, device_id=(w, (z + j) % 4), device_id_type=MESH)
    for j in range(1, wide):
        pl.semaphore_signal(barrier, 1, device_id=((w + j) % wide, z), device_id_type=MESH)
    pl.semaphore_wait(barrier, 3 + wide - 1)

    w_start(0, 0)
    image = range(images)
    for i in image:
        R["x"][0, rows(i), cols(z)] = R["x_in"][rows(i)]
        ag_start(R["x"].at[0], 0, i)

    def gn_copy(q, r, to):
        return remote(R["gb_in"], R["gn"].at[z], R["gn_s"].at[q], R["gn_r"].at[r], w, to)

    gn_copy(0, 0, mate).start()
    gn_copy(1, far, oi).start()
    gn_copy(2, far, oo).start()
    R["gn"][z] = R["gb_in"][...]
    R["r"][...] = R["x_in"][...].astype(F32)
    R["g"][...] = R["cot_in"][...].astype(F32)
    R["centre"][...] = jnp.zeros_like(R["centre"])
    R["sv"][...] = jnp.zeros_like(R["sv"])
    R["vs"][...] = jnp.zeros_like(R["vs"])
    for name in ("k", "v"):
        for i in image:
            empty = jnp.zeros((LAYERS, KEYS - ROWS, width), BF16)
            R[name][:, i * KEYS + ROWS : (i + 1) * KEYS] = empty
    for i in image:
        ag_relay(R["x"].at[0], 0, i)
    last_e = R["e"].at[2 * LAYERS - 1]
    for i in image:
        last_e[rows(i), cols(z)] = R["cot_in"][rows(i)]
        ag_start(last_e, 2, i)
    for q in range(3):
        gn_copy(q, q, mate).wait_recv()
    for q in range(3):
        gn_copy(q, q, mate).wait_send()
    w_relay(0, 0)
    w_finish(0, 0)
    w_start(0, 1)
    for i in image:
        ag_relay(last_e, 2, i)

    def forward(l, _):
        f1(l, 0)

        @when(l > 0)
        def _():
            ag_relay(R["x"].at[0], 0, 1)

        rs_relay(0, 0)
        f1(l, 1)
        post_f1(l, 0)
        w_relay(l, 1)
        rs_relay(0, 1)
        ag_relay(R["x"].at[1], 1, 0)
        post_f1(l, 1)
        w_finish(l, 1)

        @when(l < LAYERS - 1)
        def _():
            w_start(l + 1, 0)

        f2(l, 0)
        ag_relay(R["x"].at[1], 1, 1)
        rs_relay(1, 0)
        f2(l, 1)

        @when(l < LAYERS - 1)
        def _():
            w_relay(l + 1, 0)
            post_f2(l, 0, False)
            rs_relay(1, 1)
            ag_relay(R["x"].at[0], 0, 0)
            post_f2(l, 1, False)
            w_finish(l + 1, 0)
            w_start(l + 1, 1)

        return 0

    lax.fori_loop(0, LAYERS, forward, 0)

    def backward(step, _):
        l = LAYERS - 1 - step
        top = l == LAYERS - 1
        e2 = R["e"].at[2 * l + 1]
        e1 = R["e"].at[2 * l]
        b2(l, 0)

        @when(top)
        def _():
            rs_relay(1, 1)

        @when(l < LAYERS - 1)
        def _():
            ag_relay(e2, 2, 1)

        rs_relay(0, 0)
        b2(l, 1)

        @when(top)
        def _():
            post_f2(l, 0, True)
            post_f2(l, 1, True)

        post_b2(l, 0)
        grad_ffn(l, 0, 2)
        rs_relay(0, 1)
        ag_relay(e1, 3, 0)
        post_b2(l, 1)
        grad_ffn(l, 2, 4)
        g_start(1)
        b1(l, 0)
        ag_relay(e1, 3, 1)
        rs_relay(1, 0)

        @when(l < LAYERS - 1)
        def _():
            g_end(l + 1, 0)

        g_mid(1)
        b1(l, 1)
        post_b1(l, 0)
        grad_attention(l, 0, 4)
        g_start(0)
        rs_relay(1, 1)

        @when(l > 0)
        def _():
            ag_relay(R["e"].at[2 * l - 1], 2, 0)

        post_b1(l, 1)
        g_end(l, 1)
        g_mid(0)
        v_start(l)
        return 0

    lax.fori_loop(0, LAYERS, backward, 0)
    for l in range(LAYERS):
        v_end(l)
    g_end(0, 0)


def body(wide, inputs, norm_gain, norm_bias, w_qkv, b_qv, w_out, b_out, w_up, b_up, w_down, b_down, cotangent):
    tokens, width = inputs.shape
    images = tokens // SEQ
    hidden = w_up.shape[2]
    per_row = w_up.shape[1]
    half = wide // 2
    tall = images * ROWS

    def padded(matrix):
        shaped = matrix.reshape(images, SEQ, width)
        return jnp.pad(shaped, ((0, 0), (0, ROWS - SEQ), (0, 0))).reshape(tall, width)

    def unpadded(matrix):
        return matrix.reshape(images, ROWS, width)[:, :SEQ].reshape(tokens, width)

    wa = jnp.concatenate(
        [w_qkv.reshape(LAYERS, per_row, 3 * width), w_out.transpose(0, 2, 1)], axis=2
    )
    wf = jnp.concatenate([w_up, w_down.transpose(0, 2, 1)], axis=2)
    gb = jnp.concatenate(
        [norm_gain.reshape(2 * LAYERS, width), norm_bias.reshape(2 * LAYERS, width)], axis=0
    )
    scratch = scratch_of(half, per_row, width, hidden, images)
    names = IN_NAMES + OUT_NAMES + tuple(scratch)
    vmem = pl.BlockSpec(memory_space=pltpu.VMEM)
    anywhere = pl.BlockSpec(memory_space=pl.ANY)
    out, gin, gwa, gwf, gv = pl.pallas_call(
        functools.partial(kernel, wide, images, width, hidden, names),
        out_shape=(
            jax.ShapeDtypeStruct((tall, width), F32),
            jax.ShapeDtypeStruct((tall, width), F32),
            jax.ShapeDtypeStruct((LAYERS, per_row, 4 * width), F32),
            jax.ShapeDtypeStruct((LAYERS, per_row, 2 * hidden), F32),
            jax.ShapeDtypeStruct((LAYERS, V_ROWS, width), F32),
        ),
        in_specs=[vmem] * 7 + [anywhere] * 2,
        out_specs=(vmem,) * 5,
        scratch_shapes=list(scratch.values()),
        compiler_params=pltpu.CompilerParams(
            collective_id=0, has_side_effects=True, vmem_limit_bytes=67043328
        ),
        name="encoder_step",
    )(
        padded(inputs), padded(cotangent), gb, b_qv.reshape(2 * LAYERS, width), b_out, b_up,
        b_down, wa, wf,
    )
    return (
        unpadded(out),
        unpadded(gin),
        gv[:, V_GAIN : V_GAIN + 2],
        gv[:, V_BIAS : V_BIAS + 2],
        gwa[:, :, : 3 * width].reshape(LAYERS, per_row, 3, width),
        gv[:, V_QV : V_QV + 2],
        gwa[:, :, 3 * width :].transpose(0, 2, 1),
        gv[:, V_OUT],
        gwf[:, :, :hidden],
        gv[:, V_UP : V_UP + hidden // width].reshape(LAYERS, hidden),
        gwf[:, :, hidden:].transpose(0, 2, 1),
        gv[:, V_DOWN],
    )


def solution(mesh):
    rows = P("wide", "narrow")
    vector2 = P(None, None, "narrow")
    vector = P(None, "narrow")
    down_cols = P(None, "narrow", "wide")
    up_rows = P(None, "wide", "narrow")
    qkv = P(None, "wide", None, "narrow")
    return jax.shard_map(
        functools.partial(body, mesh.shape["wide"]),
        mesh=mesh,
        in_specs=(
            rows, vector2, vector2, qkv, vector2, down_cols, vector, up_rows, vector, down_cols,
            vector, rows,
        ),
        out_specs=(
            rows, rows, vector2, vector2, qkv, vector2, down_cols, vector, up_rows, vector,
            down_cols, vector,
        ),
        check_vma=False,
    )
```

```python
import functools
import math

import jax
import jax.numpy as jnp
from jax import lax
from jax.experimental import pallas as pl
from jax.experimental.pallas import tpu as pltpu
from jax.sharding import PartitionSpec as P

D = 1024
HEAD_DIM = 64
SEQ = 197
LAYERS = 2
EPS = 1e-06
ROWS = 208
KEYS = 256
MESH = pl.DeviceIdType.MESH
F32 = jnp.float32
BF16 = jnp.bfloat16
CHUNK = 16
HIGHEST = lax.Precision.HIGHEST

V_GAIN, V_BIAS, V_OUT, V_DOWN, V_QV, V_UP = 0, 2, 4, 5, 8, 10
V_ROWS = 16
G_GAIN, G_BIAS, G_OUT, G_DOWN = 0, 4, 8, 10
G_ROWS = 16


def dot(a, b):
    return lax.dot_general(a, b, (((1,), (0,)), ((), ())), preferred_element_type=F32)


def dot_t(a, b):
    return lax.dot_general(a, b, (((1,), (1,)), ((), ())), preferred_element_type=F32)


def t_dot(a, b):
    return lax.dot_general(a, b, (((0,), (0,)), ((), ())), preferred_element_type=F32)


def exact_dot(a, b, dims):
    return lax.dot_general(a, b, (dims, ((), ())), precision=HIGHEST, preferred_element_type=F32)


def when(condition):
    return pl.when(condition)


def scratch_of(half, per_row, width, hidden, images):
    tall = images * ROWS
    dma = pltpu.SemaphoreType.DMA
    vm = pltpu.VMEM
    return dict(
        wa=vm((LAYERS, D, 4 * width), BF16),
        wf=vm((LAYERS, D, 2 * hidden), BF16),
        ga=vm((D, 4 * width), BF16),
        gf=vm((D, 2 * hidden), BF16),
        pa=vm((LAYERS * half, per_row, 4 * width), BF16),
        pf=vm((half, per_row, 2 * hidden), BF16),
        ca=vm((LAYERS * half, per_row, 4 * width), BF16),
        cf=vm((half, per_row, 2 * hidden), BF16),
        e=vm((2 * LAYERS, tall, D), BF16),
        act=vm((2 * LAYERS, tall, D), BF16),
        q=vm((LAYERS, tall, width), BF16),
        k=vm((LAYERS, images * KEYS, width), BF16),
        v=vm((LAYERS, images * KEYS, width), BF16),
        o=vm((LAYERS, tall, width), BF16),
        prob=vm((LAYERS * images * (width // HEAD_DIM), ROWS, KEYS), F32),
        slope=vm((LAYERS, tall, hidden), F32),
        u=vm((LAYERS, tall, hidden), BF16),
        n=vm((2 * LAYERS, tall, 2 * width), F32),
        spread=vm((2 * LAYERS, tall, 1), F32),
        centre=vm((tall, 1), F32),
        r=vm((tall, 2 * width), F32),
        g=vm((tall, 2 * width), F32),
        f=vm((tall, hidden), BF16),
        d=vm((tall, 3 * width), BF16),
        do=vm((ROWS, width), BF16),
        tmp=vm((ROWS, width), F32),
        stage=vm((2, images, 4, ROWS, width), BF16),
        slot=vm((2, images, 6, ROWS, width), BF16),
        held=vm((images, 2, ROWS, width), F32),
        own=vm((2, images, 2, ROWS, width), F32),
        vs=vm((2, KEYS, 128), F32),
        ts=vm((images, 8, KEYS), F32),
        tr=vm((images, 3, 8, KEYS), F32),
        gb=vm((G_ROWS, width), F32),
        gn=vm((4, G_ROWS, width), F32),
        ra=vm((per_row, 4 * width), F32),
        rf=vm((per_row, 2 * hidden), F32),
        wo=vm((LAYERS, per_row, width), BF16),
        wd=vm((LAYERS, per_row, hidden), BF16),
        sh=vm((LAYERS, 2, 8, width), F32),
        sm=vm((LAYERS, 8, width), F32),
        sv=vm((LAYERS, V_ROWS, width), F32),
        rv=vm((LAYERS, 2 * half, V_ROWS, width), F32),
        a0_s=dma((2, images, 4)),
        a0_r=dma((2, images, 3)),
        ag_s=dma((4, images, 6)),
        ag_r=dma((4, images, 4)),
        rs_s=dma((2, images, 4)),
        rs_r=dma((2, images, 6)),
        t_s=dma((images, 2)),
        t_r=dma((images, 3)),
        gn_s=dma((3,)),
        gn_r=dma((3,)),
        sm_s=dma((LAYERS,)),
        sm_r=dma((LAYERS,)),
        fin_s=dma((2, images)),
        fin_r=dma((2, images)),
        w_l=dma((LAYERS, 4)),
        w_s=dma((LAYERS, 4, half)),
        w_r=dma((LAYERS, 4, half)),
        w_f=dma((LAYERS, 4, half)),
        w_g=dma((LAYERS, 4, half)),
        p_s=dma((2, half)),
        p_r=dma((LAYERS, 2, half)),
        c_s=dma((2, half)),
        c_r=dma((LAYERS, 2, half)),
        r_s=dma((LAYERS, 2)),
        v_s=dma((LAYERS, 2 * half)),
        v_r=dma((LAYERS, 2 * half)),
    )


IN_NAMES = (
    "x_in", "cot_in", "ng_in", "nb_in", "bq_in", "bo_in", "bu_in", "bd_in", "wo_in", "wd_in",
    "wq_in", "wu_in",
)
OUT_NAMES = ("out", "gin", "gwa", "gwf", "gv")


def kernel(wide, images, width, hidden, names, *refs):
    R = dict(zip(names, refs))
    R["x"] = R["e"].at[0:2]
    half = wide // 2
    per_row = D // wide
    heads = width // HEAD_DIM
    w = lax.axis_index("wide")
    z = lax.axis_index("narrow")
    upper = z // 2
    mate = z + 1 - 2 * (z % 2)
    oi = 2 - upper
    oo = 3 * (1 - upper)
    inner_n = (z + upper) % 2
    inner = inner_n == 1
    outer = inner_n == 0
    far = 2 - inner_n
    near_half = 2 * upper
    far_half = 2 - near_half
    inside = z % 2
    half_cols = pl.ds(pl.multiple_of(near_half * width, 128), 2 * width)
    par = w % 2
    mine = w // 2
    partner = w + 1 - 2 * par

    def rows(i):
        return pl.ds(i * ROWS, ROWS)

    def cols(j):
        return pl.ds(pl.multiple_of(j * width, 128), width)

    def block_rows(j):
        return pl.ds(pl.multiple_of(j * width, 128), width)

    def wrows(j):
        return pl.ds(pl.multiple_of(j * per_row, per_row), per_row)

    def remote(src, dst, s, r, wide_id, narrow_id):
        return pltpu.make_async_remote_copy(
            src_ref=src, dst_ref=dst, send_sem=s, recv_sem=r,
            device_id=(wide_id, narrow_id), device_id_type=MESH,
        )

    def chunks(count, body, unroll=False):
        lax.fori_loop(
            0, count // CHUNK, lambda c, _: (body(c * CHUNK), 0)[1], 0, unroll=unroll
        )

    def at(i, start, size=CHUNK):
        return pl.ds(pl.multiple_of(i * ROWS + start, CHUNK), size)

    def a0_copy(buf, kind, i, block, s, r, to):
        part = buf.at[rows(i), cols(block)]
        return remote(part, part, R["a0_s"].at[kind, i, s], R["a0_r"].at[kind, i, r], w, to)

    def a0_start(buf, kind, i):
        a0_copy(buf, kind, i, z, 0, 0, mate).start()
        a0_copy(buf, kind, i, z, 1, far, oi).start()

    def a0_relay(buf, kind, i):
        @when(inner)
        def _():
            for r, block in ((1, oi), (2, oo)):
                a0_copy(buf, kind, i, block, r + 1, r, mate).wait_recv()
                a0_copy(buf, kind, i, block, r + 1, r, mate).start()

    def a0_finish(buf, kind, i):
        a0_copy(buf, kind, i, mate, 0, 0, mate).wait_recv()

        @when(outer)
        def _():
            for r, block in ((1, oi), (2, oo)):
                a0_copy(buf, kind, i, block, r + 1, r, mate).wait_recv()

        a0_copy(buf, kind, i, z, 0, 0, mate).wait_send()
        a0_copy(buf, kind, i, z, 1, far, oi).wait_send()

        @when(inner)
        def _():
            for r, block in ((1, oi), (2, oo)):
                a0_copy(buf, kind, i, block, r + 1, r, mate).wait_send()

    def ag_copy(buf, kind, i, block, s, r, to):
        part = buf.at[rows(i), cols(block)]
        return remote(part, part, R["ag_s"].at[kind, i, s], R["ag_r"].at[kind, i, r], w, to)

    def ag_start(buf, kind, i):
        @when(inner)
        def _():
            for u in range(2):
                ag_copy(buf, kind, i, near_half + u, u, u, oi).start()
            for u in range(2):
                ag_copy(buf, kind, i, near_half + u, 2 + u, 2 + u, mate).start()

    def ag_relay(buf, kind, i):
        @when(inner)
        def _():
            for u in range(2):
                ag_copy(buf, kind, i, far_half + u, 4 + u, u, mate).wait_recv()
                ag_copy(buf, kind, i, far_half + u, 4 + u, u, mate).start()

    def ag_finish(buf, kind, i):
        @when(outer)
        def _():
            for u in range(2):
                ag_copy(buf, kind, i, near_half + u, 2 + u, 2 + u, mate).wait_recv()
            for u in range(2):
                ag_copy(buf, kind, i, far_half + u, 4 + u, u, mate).wait_recv()

    def ag_drain(buf, kind, i):
        @when(inner)
        def _():
            for u in range(2):
                ag_copy(buf, kind, i, near_half + u, u, u, oi).wait_send()
                ag_copy(buf, kind, i, near_half + u, 2 + u, 2 + u, mate).wait_send()
                ag_copy(buf, kind, i, far_half + u, 4 + u, u, mate).wait_send()

    def rs_copy(bank, i, q, slot, to):
        return remote(
            R["stage"].at[bank, i, q], R["slot"].at[bank, i, slot],
            R["rs_s"].at[bank, i, q], R["rs_r"].at[bank, i, slot], w, to,
        )

    def rs_blocks(bank, i, block):
        for q in range(4):
            y = block((far_half if q < 2 else near_half) + q % 2)

            @when(outer)
            def _():
                R["stage"][bank, i, q] = y.astype(BF16)
                rs_copy(bank, i, q, q, mate).start()

            @when(inner)
            def _():
                if q < 2:
                    R["held"][i, q] = y
                else:
                    R["own"][bank, i, q - 2] = y

    def rs_relay(bank, i):
        @when(inner)
        def _():
            for q in range(2):
                rs_copy(bank, i, q, q, mate).wait_recv()

                def body(c):
                    part = pl.ds(pl.multiple_of(c, CHUNK), CHUNK)
                    total = R["held"][i, q, part] + R["slot"][bank, i, q, part].astype(F32)
                    R["stage"][bank, i, q, part] = total.astype(BF16)

                chunks(ROWS, body, True)
                rs_copy(bank, i, q, 4 + q, oi).start()

    def rs_wait(bank, i):
        @when(inner)
        def _():
            for q in range(2, 4):
                rs_copy(bank, i, q, q, mate).wait_recv()
            for q in range(2):
                rs_copy(bank, i, q, 4 + q, oi).wait_recv()
            for q in range(2):
                rs_copy(bank, i, q, 4 + q, oi).wait_send()

        @when(outer)
        def _():
            for q in range(4):
                rs_copy(bank, i, q, q, mate).wait_send()

    def rs_sum(bank, i, part):
        slots = R["slot"]
        return jnp.concatenate(
            [
                R["own"][bank, i, u, part]
                + slots[bank, i, 2 + u, part].astype(F32)
                + slots[bank, i, 4 + u, part].astype(F32)
                for u in range(2)
            ],
            axis=1,
        )

    def near_row(row):
        return jnp.concatenate([R["gn"][near_half + u, row] for u in range(2)], axis=1)

    def t_copy(i, q, r, to):
        return remote(
            R["ts"].at[i], R["tr"].at[i, r], R["t_s"].at[i, q], R["t_r"].at[i, r], w, to
        )

    def t_send(i):
        lane = lax.broadcasted_iota(jnp.int32, (8, 128), 0)
        first = jnp.where(lane < 4, 1.0, 0.0).astype(F32)
        second = 1.0 - first
        R["ts"][i] = exact_dot(first, R["vs"][0], ((1,), (1,))) + exact_dot(
            second, R["vs"][1], ((1,), (1,))
        )
        @when(outer)
        def _():
            t_copy(i, 0, 0, mate).start()

        t_copy(i, 1, far, oi).start()

    def t_total(i):
        for q in range(3):
            t_copy(i, 0, q, mate).wait_recv()
        total = (R["ts"][i] + R["tr"][i, 0]) + (R["tr"][i, 1] + R["tr"][i, 2])
        row = lax.broadcasted_iota(jnp.int32, (8, 128), 0)
        lane = lax.broadcasted_iota(jnp.int32, (8, 128), 1)
        pick = ((row == 0) & (lane < 64)) | ((row == 4) & (lane >= 64))
        R["vs"][0] = exact_dot(total, jnp.where(pick, 1.0, 0.0).astype(F32), ((0,), (0,)))

    def t_drain(i):
        @when(outer)
        def _():
            t_copy(i, 0, 0, mate).wait_send()

        t_copy(i, 1, far, oi).wait_send()

    def weights(l, piece):
        if piece == 0:
            return R["wa"].at[l, :, 0 : 3 * width], R["wq_in"].at[l]
        if piece == 1:
            return R["wa"].at[l, :, 3 * width : 4 * width], R["wo"].at[l]
        if piece == 2:
            return R["wf"].at[l, :, 0:hidden], R["wu_in"].at[l]
        return R["wf"].at[l, :, hidden : 2 * hidden], R["wd"].at[l]

    def w_local(l, piece):
        full, shard = weights(l, piece)
        return pltpu.make_async_copy(shard, full.at[wrows(w)], R["w_l"].at[l, piece])

    def w_send(l, piece, s, to):
        full, shard = weights(l, piece)
        return remote(
            shard, full.at[wrows(w)], R["w_s"].at[l, piece, s], R["w_r"].at[l, piece, mine], to, z
        )

    def w_pair(l, piece):
        full, shard = weights(l, piece)
        return remote(
            shard, full.at[wrows(w)],
            R["w_s"].at[l, piece, half - 1], R["w_f"].at[l, piece, mine], partner, z,
        )

    def w_cross(l, piece, k, parity):
        full, _ = weights(l, piece)
        part = full.at[wrows(2 * k + parity)]
        return remote(
            part, part, R["w_g"].at[l, piece, k], R["w_f"].at[l, piece, k], partner, z
        )

    def w_start(l, piece):
        for j in range(1, half):
            w_send(l, piece, j - 1, 2 * ((mine + j) % half) + par).start()
        w_pair(l, piece).start()
        w_local(l, piece).start()

    def w_relay(l, piece):
        full, shard = weights(l, piece)
        for j in range(1, half):
            k = (mine + half - j) % half
            remote(
                shard, full.at[wrows(2 * k + par)],
                R["w_s"].at[l, piece, 0], R["w_r"].at[l, piece, k], partner, z,
            ).wait_recv()
            w_cross(l, piece, k, par).start()

    def w_finish(l, piece):
        for j in range(half):
            w_cross(l, piece, (mine + half - j) % half, 1 - par).wait_recv()
        w_local(l, piece).wait()
        for s in range(half - 1):
            w_send(l, piece, s, partner).wait_send()
        w_pair(l, piece).wait_send()
        for j in range(1, half):
            w_cross(l, piece, (mine + j) % half, par).wait_send()

    def grads(l, piece):
        if piece == 0:
            room = pl.ds(l * half, half)
            return R["ga"], R["pa"].at[room], R["ca"].at[room], R["ra"], R["gwa"].at[l]
        return R["gf"], R["pf"], R["cf"], R["rf"], R["gwf"].at[l]

    def p_copy(l, piece, k):
        full, theirs, _, _, _ = grads(l, piece)
        return remote(
            full.at[wrows(2 * k + 1 - par)], theirs.at[k],
            R["p_s"].at[piece, k], R["p_r"].at[l, piece, k], partner, z,
        )

    def c_copy(l, piece, k, source):
        full, _, came, _, _ = grads(l, piece)
        return remote(
            full.at[wrows(2 * k + par)], came.at[source],
            R["c_s"].at[piece, k], R["c_r"].at[l, piece, source], 2 * k + par, z,
        )

    def r_copy(l, piece):
        _, _, _, total, result = grads(l, piece)
        return pltpu.make_async_copy(total, result, R["r_s"].at[l, piece])

    def g_start(l, piece, b):
        pairs = half * 256 // D
        for k in range(pairs):
            p_copy(l, piece, b * pairs + k).start()

    def g_mid(l, piece):
        full, theirs, _, _, _ = grads(l, piece)
        for j in range(1, half + 1):
            k = (mine + j) % half
            p_copy(l, piece, k).wait_recv()

            def body(c):
                here = pl.ds(pl.multiple_of((2 * k + par) * per_row + c, CHUNK), CHUNK)
                total = full[here].astype(F32) + theirs[
                    k, pl.ds(pl.multiple_of(c, CHUNK), CHUNK)
                ].astype(F32)
                full[here] = total.astype(BF16)

            chunks(per_row, body)
            if j < half:
                c_copy(l, piece, k, mine).start()

    def g_end(l, piece):
        full, _, came, result, _ = grads(l, piece)
        for j in range(1, half):
            k = (mine + half - j) % half
            c_copy(l, piece, k, k).wait_recv()

        @when(l < LAYERS - 1)
        def _():
            r_copy(l + 1, piece).wait()

        def body(c):
            here = pl.ds(pl.multiple_of(w * per_row + c, CHUNK), CHUNK)
            part = pl.ds(pl.multiple_of(c, CHUNK), CHUNK)
            total = full[here].astype(F32)
            for j in range(1, half):
                total = total + came[(mine + j) % half, part].astype(F32)
            result[part] = total

        chunks(per_row, body)
        r_copy(l, piece).start()
        for k in range(half):
            p_copy(l, piece, k).wait_send()
        for j in range(1, half):
            c_copy(l, piece, (mine + j) % half, mine).wait_send()

    def v_copy(l, j, source):
        to = (w + j) % wide
        return remote(
            R["sv"].at[l], R["rv"].at[l, source],
            R["v_s"].at[l, j], R["v_r"].at[l, source], to, z,
        )

    def sm_copy(l):
        return remote(
            R["sh"].at[l, 1 - inside], R["sm"].at[l], R["sm_s"].at[l], R["sm_r"].at[l], w, mate
        )

    def v_start(l):
        @when(inner)
        def _():
            sm_copy(l).start()
            R["sv"][l, 0:8] = R["sh"][l, inside]
            sm_copy(l).wait_send()

        @when(outer)
        def _():
            sm_copy(l).wait_recv()
            R["sv"][l, 0:8] = R["sm"][l]

        for j in range(1, wide):
            v_copy(l, j, w).start()

    def v_end(l):
        total = R["sv"][l]
        for j in range(1, wide):
            source = (w + j) % wide
            v_copy(l, j, source).wait_recv()
            total = total + R["rv"][l, source]
        R["gv"][l] = total
        for j in range(1, wide):
            v_copy(l, j, w).wait_send()

    def norm_in(buf, l, branch, i):
        at_norm = 2 * l + branch
        scale = [R["gn"][j, pl.ds(G_GAIN + at_norm, 1)] for j in range(4)]
        shift = [R["gn"][j, pl.ds(G_BIAS + at_norm, 1)] for j in range(4)]
        scale = jnp.concatenate(scale, axis=1)
        shift = jnp.concatenate(shift, axis=1)

        def body(c):
            here = at(i, c)
            raw = buf[here, :].astype(F32)
            mean = jnp.sum(raw, axis=1, keepdims=True) * (1.0 / D)
            square = jnp.sum(raw * raw, axis=1, keepdims=True) * (1.0 / D)
            s = lax.rsqrt(square - mean * mean + EPS)
            R["act"][at_norm, here] = ((raw - mean) * s * scale + shift).astype(BF16)
            R["centre"][here] = R["centre"][here] + mean
            R["spread"][at_norm, here] = s

        chunks(ROWS, body, True)

    def norm_keep(l, branch, i):
        at_norm = 2 * l + branch

        @when(inner)
        def _():
            def body(c):
                here = at(i, c)
                R["n"][at_norm, here] = (R["r"][here] - R["centre"][here]) * R["spread"][
                    at_norm, here
                ]

            chunks(ROWS, body, True)

    def norm_back(bank, l, branch, i, out_row):
        at_norm = 2 * l + branch
        rs_wait(bank, i)
        t_drain(i)

        @when(inner)
        def _():
            scale = near_row(pl.ds(G_GAIN + at_norm, 1))
            t_total(i)

            def body(c, carry):
                gain_sum, bias_sum, g_sum = carry
                c = c * CHUNK
                here = at(i, c)
                part = pl.ds(pl.multiple_of(c, CHUNK), CHUNK)
                upstream = rs_sum(bank, i, part)
                normed = R["n"][at_norm, here]
                first = R["vs"][0, part, 0:1] * (1.0 / D)
                second = R["vs"][0, part, 64:65] * (1.0 / D)
                grown = R["g"][here] + (
                    upstream * scale - first - normed * second
                ) * R["spread"][at_norm, here]
                R["g"][here] = grown
                gain_sum = gain_sum + jnp.sum(upstream * normed, axis=0, keepdims=True)
                bias_sum = bias_sum + jnp.sum(upstream, axis=0, keepdims=True)
                g_sum = g_sum + jnp.sum(grown, axis=0, keepdims=True)
                return gain_sum, bias_sum, g_sum

            zero = jnp.zeros((1, 2 * width), F32)
            gain_sum, bias_sum, g_sum = lax.fori_loop(
                0, ROWS // CHUNK, body, (zero, zero, zero), unroll=True
            )
            half_add(l, V_GAIN + branch, gain_sum)
            half_add(l, V_BIAS + branch, bias_sum)
            if out_row is not None:
                half_add(l, out_row, g_sum)

    def half_add(l, row, value):
        for u in range(2):
            there = slice(row, row + 1)
            part = value[:, u * width : (u + 1) * width]
            R["sh"][l, u, there] = R["sh"][l, u, there] + part

    def send_sums(at_norm, i, block_of):
        R["vs"][0, 0:ROWS] = jnp.zeros((ROWS, 128), F32)
        R["vs"][1, 0:ROWS] = jnp.zeros((ROWS, 128), F32)
        l, branch = at_norm

        def block(j):
            y = block_of(j)
            R["tmp"][...] = y
            scale = R["gn"][j, pl.ds(G_GAIN + 2 * l + branch, 1)]
            shift = R["gn"][j, pl.ds(G_BIAS + 2 * l + branch, 1)]

            def body(c):
                part = pl.ds(pl.multiple_of(c, CHUNK), CHUNK)
                value = R["tmp"][part]
                normed = R["act"][2 * l + branch, at(i, c), cols(j)].astype(F32) - shift
                first = value * scale
                second = value * normed
                for m in range(width // 128):
                    lanes = slice(m * 128, (m + 1) * 128)
                    R["vs"][0, part] = R["vs"][0, part] + first[:, lanes]
                    R["vs"][1, part] = R["vs"][1, part] + second[:, lanes]

            chunks(ROWS, body, True)
            return R["tmp"][...]

        return block

    head_lanes = [slice(h * HEAD_DIM, (h + 1) * HEAD_DIM) for h in range(heads)]

    def attention(l, i):
        keys = pl.ds(i * KEYS, KEYS)
        column = lax.broadcasted_iota(jnp.int32, (ROWS, KEYS), 1)
        factor = 1.0 / math.sqrt(HEAD_DIM)
        scores = [
            dot_t(R["q"][l, rows(i), lanes], R["k"][l, keys, lanes]) for lanes in head_lanes
        ]
        probs = []
        for h in range(heads):
            masked = jnp.where(column < SEQ, scores[h] * factor, -jnp.inf)
            top = jnp.max(masked, axis=1, keepdims=True)
            grown = jnp.exp(masked - top)
            prob = grown / jnp.sum(grown, axis=1, keepdims=True)
            R["prob"][(l * images + i) * heads + h] = prob
            probs.append(prob.astype(BF16))
        mixed = [dot(probs[h], R["v"][l, keys, head_lanes[h]]) for h in range(heads)]
        R["o"][l, rows(i)] = jnp.concatenate(mixed, axis=1).astype(BF16)

    def f1(l, i):
        buf = R["x"].at[0]

        @when(l > 0)
        def _():
            ag_finish(buf, 0, i)

        norm_in(buf, l, 0, i)
        act = R["act"].at[2 * l, rows(i)]
        kept = pl.ds(i * KEYS, ROWS)
        bq = R["bq_in"][l, 0:1]
        bv = R["bq_in"][l, 1:2]
        R["q"][l, rows(i)] = (dot(act[...], R["wa"][l, :, 0:width]) + bq).astype(BF16)
        R["k"][l, kept] = dot(act[...], R["wa"][l, :, width : 2 * width]).astype(BF16)
        R["v"][l, kept] = (dot(act[...], R["wa"][l, :, 2 * width : 3 * width]) + bv).astype(BF16)
        attention(l, i)
        if i == 0:
            w_relay(l, 1)
            w_finish(l, 1)

        def block(j):
            return dot_t(R["o"][l, rows(i)], R["wa"][l, block_rows(j), 3 * width : 4 * width])

        rs_blocks(0, i, block)
        norm_keep(l, 0, i)

    def f2(l, i):
        buf = R["x"].at[1]
        ag_finish(buf, 1, i)
        norm_in(buf, l, 1, i)

        def body(b, _):
            lanes = cols(b)
            pre = dot(R["act"][2 * l + 1, rows(i)], R["wf"][l, :, lanes])
            pre = pre + R["bu_in"][pl.ds(l, 1), lanes]
            cdf = 0.5 * (1.0 + lax.erf(pre * 0.7071067811865476))
            R["u"][l, rows(i), lanes] = (pre * cdf).astype(BF16)
            R["slope"][l, rows(i), lanes] = (
                cdf + pre * jnp.exp(-0.5 * pre * pre) * 0.3989422804014327
            )
            return 0

        lax.fori_loop(0, hidden // width, body, 0)

        def block(j):
            return dot_t(R["u"][l, rows(i)], R["wf"][l, block_rows(j), hidden : 2 * hidden])

        rs_blocks(1, i, block)
        norm_keep(l, 1, i)

    def residual(bank, i, bias_row, kind):
        rs_wait(bank, i)

        @when(inner)
        def _():
            bias = near_row(bias_row)

            def body(c):
                here = at(i, c)
                part = pl.ds(pl.multiple_of(c, CHUNK), CHUNK)
                grown = R["r"][here] + (rs_sum(bank, i, part) + bias)
                R["r"][here] = grown
                if kind is not None:
                    out = (grown - R["centre"][here]).astype(BF16)
                    R["x"][kind, here, half_cols] = out

            chunks(ROWS, body, True)

        if kind is not None:
            ag_start(R["x"].at[kind], kind, i)

    def fin_copy(which, i):
        source = (R["r"], R["g"])[which]
        there = pl.ds(pl.multiple_of((1 - inside) * width, 128), width)
        return remote(
            source.at[rows(i), there], R["held"].at[i, which],
            R["fin_s"].at[which, i], R["fin_r"].at[which, i], w, mate,
        )

    def fin_start(which, i):
        @when(inner)
        def _():
            fin_copy(which, i).start()

    def fin_end(which, i):
        source, result = ((R["r"], R["out"]), (R["g"], R["gin"]))[which]
        there = pl.ds(i * SEQ, SEQ)

        @when(inner)
        def _():
            here = pl.ds(pl.multiple_of(inside * width, 128), width)
            result[there] = source[pl.ds(i * ROWS, SEQ), here]
            fin_copy(which, i).wait_send()

        @when(outer)
        def _():
            fin_copy(which, i).wait_recv()
            result[there] = R["held"][i, which, 0:SEQ]

    def post_f1(l, i):
        @when(l > 0)
        def _():
            ag_drain(R["x"].at[0], 0, i)

        residual(0, i, pl.ds(G_OUT + l, 1), 1)

    def post_f2(l, i, last):
        ag_drain(R["x"].at[1], 1, i)
        residual(1, i, pl.ds(G_DOWN + l, 1), None if last else 0)
        if last:
            fin_start(0, i)

    def send_grad(slot, kind, i):
        buf = R["e"].at[slot]

        @when(inner)
        def _():
            def body(c):
                here = at(i, c)
                buf[here, half_cols] = R["g"][here].astype(BF16)

            chunks(ROWS, body, True)

        ag_start(buf, kind, i)

    def b2(l, i):
        e = R["e"].at[2 * l + 1]

        @when(l < LAYERS - 1)
        def _():
            ag_finish(e, 2, i)

        def body(b, _):
            lanes = cols(b)
            back = pl.ds(pl.multiple_of(hidden + b * width, 128), width)
            dz = dot(e[rows(i), :], R["wf"][l, :, back]) * R["slope"][l, rows(i), lanes]
            R["f"][rows(i), lanes] = dz.astype(BF16)
            row = pl.ds(V_UP + b, 1)
            R["sv"][l, row] = R["sv"][l, row] + jnp.sum(dz, axis=0, keepdims=True)
            return 0

        lax.fori_loop(0, hidden // width, body, 0)

        def block(j):
            return dot_t(R["f"][rows(i)], R["wf"][l, block_rows(j), 0:hidden])

        rs_blocks(0, i, send_sums((l, 1), i, block))
        t_send(i)
        add_down(l, i)

    def b1(l, i):
        e = R["e"].at[2 * l]
        ag_finish(e, 3, i)
        keys = pl.ds(i * KEYS, KEYS)
        R["do"][...] = dot(e[rows(i), :], R["wa"][l, :, 3 * width : 4 * width]).astype(BF16)
        factor = 1.0 / math.sqrt(HEAD_DIM)
        grad_out = [R["do"][:, lanes] for lanes in head_lanes]
        dps = [dot_t(grad_out[h], R["v"][l, keys, head_lanes[h]]) for h in range(heads)]
        dvs, dss = [], []
        for h in range(heads):
            prob = R["prob"][(l * images + i) * heads + h]
            dvs.append(t_dot(prob.astype(BF16), grad_out[h])[0:ROWS])
            delta = jnp.sum(prob * dps[h], axis=1, keepdims=True)
            dss.append((prob * (dps[h] - delta) * factor).astype(BF16))
        dqs = [dot(dss[h], R["k"][l, keys, head_lanes[h]]) for h in range(heads)]
        dks = [t_dot(dss[h], R["q"][l, rows(i), head_lanes[h]])[0:ROWS] for h in range(heads)]
        dq, dk, dv = [jnp.concatenate(parts, axis=1) for parts in (dqs, dks, dvs)]
        for part, value in ((0, dq), (1, dk), (2, dv)):
            R["d"][rows(i), part * width : (part + 1) * width] = value.astype(BF16)
        for row, value in ((V_QV, dq), (V_QV + 1, dv)):
            there = slice(row, row + 1)
            R["sv"][l, there] = R["sv"][l, there] + jnp.sum(value, axis=0, keepdims=True)

        def block(j):
            return dot_t(R["d"][rows(i)], R["wa"][l, block_rows(j), 0 : 3 * width])

        rs_blocks(1, i, send_sums((l, 0), i, block))
        t_send(i)

    def add_down(l, i):
        @when(inner)
        def _():
            def body(c, total):
                return total + jnp.sum(R["g"][at(i, c * CHUNK)], axis=0, keepdims=True)

            zero = jnp.zeros((1, 2 * width), F32)
            half_add(l, V_DOWN, lax.fori_loop(0, ROWS // CHUNK, body, zero, unroll=True))

    def post_b2(l, i):
        @when(l < LAYERS - 1)
        def _():
            ag_drain(R["e"].at[2 * l + 1], 2, i)

        norm_back(0, l, 1, i, V_OUT)
        send_grad(2 * l, 3, i)

    def post_b1(l, i):
        ag_drain(R["e"].at[2 * l], 3, i)
        norm_back(1, l, 0, i, None)

        @when(l > 0)
        def _():
            send_grad(2 * l - 1, 2, i)

        @when(l == 0)
        def _():
            fin_start(1, i)

    def grad_block(b):
        block = (mine * 2 * per_row // 256 + 1 + b) % (D // 256)
        return block, pl.ds(pl.multiple_of(block * 256, 256), 256)

    def grad_ffn(l, first, last):
        def body(b, _):
            block, lanes = grad_block(b)
            up = t_dot(R["act"][2 * l + 1, :, lanes], R["f"][...])
            R["gf"][lanes, 0:hidden] = up.astype(BF16)
            down = t_dot(R["e"][2 * l + 1, :, lanes], R["u"][l])
            R["gf"][lanes, hidden : 2 * hidden] = down.astype(BF16)
            g_start(l, 1, block)
            return 0

        lax.fori_loop(first, last, body, 0)

    def grad_attention(l, first, last):
        def body(b, _):
            block, lanes = grad_block(b)
            qkv = t_dot(R["act"][2 * l, :, lanes], R["d"][...])
            R["ga"][lanes, 0 : 3 * width] = qkv.astype(BF16)
            out = t_dot(R["e"][2 * l, :, lanes], R["o"][l])
            R["ga"][lanes, 3 * width : 4 * width] = out.astype(BF16)
            g_start(l, 0, block)
            return 0

        lax.fori_loop(first, last, body, 0)

    def spread_rows(source, result):
        tokens = images * SEQ
        wide_rows = R["r"].at[:, 0:width]
        wide_rows[0:tokens] = source[...].astype(F32)
        row = lax.broadcasted_iota(jnp.int32, (ROWS, width), 0)
        for i in image:
            part = wide_rows[i * SEQ : i * SEQ + ROWS]
            result[rows(i), cols(z)] = jnp.where(row < SEQ, part, 0.0).astype(BF16)

    barrier = pltpu.get_barrier_semaphore()
    for j in range(1, wide):
        pl.semaphore_signal(barrier, 1, device_id=((w + j) % wide, z), device_id_type=MESH)
    for j in range(1, 4):
        pl.semaphore_signal(barrier, 1, device_id=(w, (z + j) % 4), device_id_type=MESH)
    image = range(images)
    first_x = R["x"].at[0]
    last_e = R["e"].at[2 * LAYERS - 1]
    R["r"][...] = jnp.zeros_like(R["r"])
    spread_rows(R["x_in"], first_x)
    for l in range(LAYERS):
        R["gb"][G_GAIN + 2 * l : G_GAIN + 2 * l + 2] = R["ng_in"][l]
        R["gb"][G_BIAS + 2 * l : G_BIAS + 2 * l + 2] = R["nb_in"][l]
    R["gb"][G_OUT : G_OUT + LAYERS] = R["bo_in"][...]
    R["gb"][G_DOWN : G_DOWN + LAYERS] = R["bd_in"][...]
    R["gn"][z] = R["gb"][...]
    for l in range(LAYERS):
        R["wo"][l] = R["wo_in"][l].T
    pl.semaphore_wait(barrier, 3 + wide - 1)

    w_start(0, 0)
    for i in image:
        a0_start(first_x, 0, i)

    def gn_copy(q, r, to):
        return remote(R["gb"], R["gn"].at[z], R["gn_s"].at[q], R["gn_r"].at[r], w, to)

    gn_copy(0, 0, mate).start()
    gn_copy(1, far, oi).start()
    gn_copy(2, far, oo).start()
    w_start(0, 1)
    for l in range(LAYERS):
        R["wd"][l] = R["wd_in"][l].T
    spread_rows(R["cot_in"], last_e)
    R["centre"][...] = jnp.zeros_like(R["centre"])
    R["sv"][...] = jnp.zeros_like(R["sv"])
    R["sh"][...] = jnp.zeros_like(R["sh"])
    R["vs"][...] = jnp.zeros_like(R["vs"])
    for name in ("k", "v"):
        for i in image:
            empty = jnp.zeros((LAYERS, KEYS - ROWS, width), BF16)
            R[name][:, i * KEYS + ROWS : (i + 1) * KEYS] = empty
    for i in image:
        a0_relay(first_x, 0, i)
    for i in image:
        a0_start(last_e, 1, i)
    w_start(0, 2)
    w_start(0, 3)
    for l in range(1, LAYERS):
        for piece in range(4):
            w_start(l, piece)
    for q in range(3):
        gn_copy(q, q, mate).wait_recv()
    for q in range(3):
        gn_copy(q, q, mate).wait_send()
    w_relay(0, 0)
    for i in image:
        a0_finish(first_x, 0, i)

    @when(inner)
    def _():
        R["r"][...] = first_x[:, half_cols].astype(F32)

    w_finish(0, 0)
    for i in image:
        a0_relay(last_e, 1, i)

    def forward(l, _):
        f1(l, 0)

        @when(l > 0)
        def _():
            ag_relay(R["x"].at[0], 0, 1)

        rs_relay(0, 0)
        f1(l, 1)
        post_f1(l, 0)
        w_relay(l, 2)
        rs_relay(0, 1)
        ag_relay(R["x"].at[1], 1, 0)
        post_f1(l, 1)
        w_finish(l, 2)
        w_relay(l, 3)
        w_finish(l, 3)

        f2(l, 0)
        ag_relay(R["x"].at[1], 1, 1)
        rs_relay(1, 0)
        f2(l, 1)

        @when(l < LAYERS - 1)
        def _():
            w_relay(l + 1, 0)
            post_f2(l, 0, False)
            rs_relay(1, 1)
            ag_relay(R["x"].at[0], 0, 0)
            post_f2(l, 1, False)
            w_finish(l + 1, 0)

        return 0

    lax.fori_loop(0, LAYERS, forward, 0)
    for i in image:
        a0_finish(last_e, 1, i)

    @when(inner)
    def _():
        R["g"][...] = last_e[:, half_cols].astype(F32)

    def backward(step, _):
        l = LAYERS - 1 - step
        top = l == LAYERS - 1
        e2 = R["e"].at[2 * l + 1]
        e1 = R["e"].at[2 * l]
        b2(l, 0)

        @when(top)
        def _():
            rs_relay(1, 1)

        @when(l < LAYERS - 1)
        def _():
            ag_relay(e2, 2, 1)

        rs_relay(0, 0)
        b2(l, 1)

        @when(top)
        def _():
            post_f2(l, 0, True)
            post_f2(l, 1, True)

        post_b2(l, 0)
        grad_ffn(l, 0, 2)
        rs_relay(0, 1)
        ag_relay(e1, 3, 0)
        post_b2(l, 1)
        grad_ffn(l, 2, 4)
        b1(l, 0)
        ag_relay(e1, 3, 1)
        rs_relay(1, 0)

        @when(l < LAYERS - 1)
        def _():
            g_end(l + 1, 0)
            v_end(l + 1)

        g_mid(l, 1)
        b1(l, 1)
        post_b1(l, 0)
        grad_attention(l, 0, 4)
        rs_relay(1, 1)

        @when(l > 0)
        def _():
            ag_relay(R["e"].at[2 * l - 1], 2, 0)

        g_mid(l, 0)
        post_b1(l, 1)
        g_end(l, 1)
        v_start(l)
        return 0

    lax.fori_loop(0, LAYERS, backward, 0)
    g_end(jnp.int32(0), 0)
    for which in range(2):
        for i in image:
            fin_end(which, i)
    v_end(0)
    for piece in range(2):
        r_copy(0, piece).wait()


def body(wide, inputs, norm_gain, norm_bias, w_qkv, b_qv, w_out, b_out, w_up, b_up, w_down, b_down, cotangent):
    tokens, width = inputs.shape
    images = tokens // SEQ
    hidden = w_up.shape[2]
    per_row = w_up.shape[1]
    half = wide // 2
    scratch = scratch_of(half, per_row, width, hidden, images)
    names = IN_NAMES + OUT_NAMES + tuple(scratch)
    vmem = pl.BlockSpec(memory_space=pltpu.VMEM)
    anywhere = pl.BlockSpec(memory_space=pl.ANY)
    out, gin, gwa, gwf, gv = pl.pallas_call(
        functools.partial(kernel, wide, images, width, hidden, names),
        out_shape=(
            jax.ShapeDtypeStruct((tokens, width), F32),
            jax.ShapeDtypeStruct((tokens, width), F32),
            jax.ShapeDtypeStruct((LAYERS, per_row, 4 * width), F32),
            jax.ShapeDtypeStruct((LAYERS, per_row, 2 * hidden), F32),
            jax.ShapeDtypeStruct((LAYERS, V_ROWS, width), F32),
        ),
        in_specs=[vmem] * 10 + [anywhere] * 2,
        out_specs=(vmem, vmem, anywhere, anywhere, vmem),
        scratch_shapes=list(scratch.values()),
        compiler_params=pltpu.CompilerParams(
            collective_id=0, has_side_effects=True, vmem_limit_bytes=67043328
        ),
        name="encoder_step",
    )(
        inputs, cotangent, norm_gain, norm_bias, b_qv, b_out, b_up, b_down, w_out, w_down,
        w_qkv.reshape(LAYERS, per_row, 3 * width), w_up,
    )
    return (
        out,
        gin,
        gv[:, V_GAIN : V_GAIN + 2],
        gv[:, V_BIAS : V_BIAS + 2],
        gwa[:, :, : 3 * width].reshape(LAYERS, per_row, 3, width),
        gv[:, V_QV : V_QV + 2],
        gwa[:, :, 3 * width :].transpose(0, 2, 1),
        gv[:, V_OUT],
        gwf[:, :, :hidden],
        gv[:, V_UP : V_UP + hidden // width].reshape(LAYERS, hidden),
        gwf[:, :, hidden:].transpose(0, 2, 1),
        gv[:, V_DOWN],
    )


def solution(mesh):
    rows = P("wide", "narrow")
    vector2 = P(None, None, "narrow")
    vector = P(None, "narrow")
    down_cols = P(None, "narrow", "wide")
    up_rows = P(None, "wide", "narrow")
    qkv = P(None, "wide", None, "narrow")
    return jax.shard_map(
        functools.partial(body, mesh.shape["wide"]),
        mesh=mesh,
        in_specs=(
            rows, vector2, vector2, qkv, vector2, down_cols, vector, up_rows, vector, down_cols,
            vector, rows,
        ),
        out_specs=(
            rows, rows, vector2, vector2, qkv, vector2, down_cols, vector, up_rows, vector,
            down_cols, vector,
        ),
        check_vma=False,
    )
```

```python
import functools
import math

import jax
import jax.numpy as jnp
from jax import lax
from jax.experimental import pallas as pl
from jax.experimental.pallas import tpu as pltpu
from jax.sharding import PartitionSpec as P

D = 1024
HEAD_DIM = 64
SEQ = 197
LAYERS = 2
EPS = 1e-06
ROWS = 208
KEYS = 256
MESH = pl.DeviceIdType.MESH
F32 = jnp.float32
BF16 = jnp.bfloat16
CHUNK = 16
HIGHEST = lax.Precision.HIGHEST

V_GAIN, V_BIAS, V_OUT, V_DOWN = 0, 2, 4, 5
V_QV, V_UP = 0, 2
V_ROWS = 8
G_GAIN, G_BIAS, G_OUT, G_DOWN = 0, 4, 8, 10
G_ROWS = 16


def dot(a, b):
    return lax.dot_general(a, b, (((1,), (0,)), ((), ())), preferred_element_type=F32)


def dot_t(a, b):
    return lax.dot_general(a, b, (((1,), (1,)), ((), ())), preferred_element_type=F32)


def t_dot(a, b):
    return lax.dot_general(a, b, (((0,), (0,)), ((), ())), preferred_element_type=F32)


def exact_dot(a, b, dims):
    return lax.dot_general(a, b, (dims, ((), ())), precision=HIGHEST, preferred_element_type=F32)


def when(condition):
    return pl.when(condition)


def scratch_of(half, per_row, width, hidden, images):
    tall = images * ROWS
    dma = pltpu.SemaphoreType.DMA
    vm = pltpu.VMEM
    return dict(
        wq=vm((LAYERS, 3, D, width), BF16),
        wp=vm((LAYERS, D, width), BF16),
        wf=vm((LAYERS, D, 2 * hidden), BF16),
        gq=vm((3, D, width), BF16),
        go=vm((D, width), BF16),
        gf=vm((D, 2 * hidden), BF16),
        pq=vm((LAYERS * half, 3, per_row, width), BF16),
        po=vm((LAYERS * half, per_row, width), BF16),
        pf=vm((half, per_row, 2 * hidden), BF16),
        cq=vm((LAYERS * half, 3, per_row, width), BF16),
        co=vm((LAYERS * half, per_row, width), BF16),
        cf=vm((half, per_row, 2 * hidden), BF16),
        e=vm((2 * LAYERS, tall, D), BF16),
        act=vm((2 * LAYERS, tall, D), BF16),
        q=vm((LAYERS, tall, width), BF16),
        k=vm((LAYERS, images * KEYS, width), BF16),
        v=vm((LAYERS, images * KEYS, width), BF16),
        o=vm((LAYERS, tall, width), BF16),
        prob=vm((LAYERS * images * (width // HEAD_DIM), ROWS, KEYS), F32),
        slope=vm((LAYERS, tall, hidden), F32),
        u=vm((LAYERS, tall, hidden), BF16),
        n=vm((2 * LAYERS, tall, 2 * width), F32),
        spread=vm((2 * LAYERS, tall, 1), F32),
        centre=vm((tall, 1), F32),
        r=vm((tall, 2 * width), F32),
        g=vm((tall, 2 * width), F32),
        f=vm((tall, hidden), BF16),
        d=vm((tall, 3 * width), BF16),
        do=vm((ROWS, width), BF16),
        tmp=vm((ROWS, width), F32),
        stage=vm((2, images, 4, ROWS, width), BF16),
        slot=vm((2, images, 6, ROWS, width), BF16),
        held=vm((images, 2, ROWS, width), F32),
        own=vm((2, images, 2, ROWS, width), F32),
        vs=vm((2, KEYS, 128), F32),
        ts=vm((images, 8, KEYS), F32),
        tr=vm((images, 3, 8, KEYS), F32),
        gb=vm((G_ROWS, width), F32),
        gn=vm((4, G_ROWS, width), F32),
        rq=vm((3, per_row, width), F32),
        ro=vm((width, per_row), F32),
        ru=vm((per_row, hidden), F32),
        rd=vm((hidden, per_row), F32),
        wo=vm((LAYERS, per_row, width), BF16),
        wd=vm((LAYERS, per_row, hidden), BF16),
        sh=vm((LAYERS, 2, 8, width), F32),
        rh=vm((LAYERS, 2 * half, 8, width), F32),
        sv=vm((LAYERS, V_ROWS, width), F32),
        rv=vm((LAYERS, 2 * half, V_ROWS, width), F32),
        a0_s=dma((2, images, 4)),
        a0_r=dma((2, images, 3)),
        ag_s=dma((4, images, 6)),
        ag_r=dma((4, images, 4)),
        rs_s=dma((2, images, 4)),
        rs_r=dma((2, images, 6)),
        t_s=dma((images, 2)),
        t_r=dma((images, 3)),
        gn_s=dma((3,)),
        gn_r=dma((3,)),
        h_s=dma((LAYERS, 2, 2 * half)),
        h_r=dma((LAYERS, 2 * half)),
        fin_s=dma((2, images)),
        fin_r=dma((2, images)),
        w_l=dma((LAYERS, 4)),
        w_s=dma((LAYERS, 4, half)),
        w_r=dma((LAYERS, 4, half)),
        w_f=dma((LAYERS, 4, half)),
        w_g=dma((LAYERS, 4, half)),
        p_s=dma((3, half)),
        p_r=dma((LAYERS, 3, half)),
        c_s=dma((3, half)),
        c_r=dma((LAYERS, 3, half)),
        r_s=dma((LAYERS, 4)),
        v_s=dma((LAYERS, 2 * half)),
        v_r=dma((LAYERS, 2 * half)),
    )


IN_NAMES = (
    "x_in", "cot_in", "ng_in", "nb_in", "bq_in", "bo_in", "bu_in", "bd_in", "wo_in", "wd_in",
    "wq_in", "wu_in",
)
OUT_NAMES = (
    "out", "gin", "gng", "gnb", "gwq", "gbqv", "gwo", "gbo", "gwu", "gbup", "gwd", "gbd",
)


def kernel(wide, images, width, hidden, names, *refs):
    R = dict(zip(names, refs))
    R["x"] = R["e"].at[0:2]
    half = wide // 2
    per_row = D // wide
    heads = width // HEAD_DIM
    w = lax.axis_index("wide")
    z = lax.axis_index("narrow")
    upper = z // 2
    mate = z + 1 - 2 * (z % 2)
    oi = 2 - upper
    oo = 3 * (1 - upper)
    inner_n = (z + upper) % 2
    inner = inner_n == 1
    outer = inner_n == 0
    far = 2 - inner_n
    near_half = 2 * upper
    far_half = 2 - near_half
    inside = z % 2
    half_cols = pl.ds(pl.multiple_of(near_half * width, 128), 2 * width)
    par = w % 2
    mine = w // 2
    partner = w + 1 - 2 * par

    def rows(i):
        return pl.ds(i * ROWS, ROWS)

    def cols(j):
        return pl.ds(pl.multiple_of(j * width, 128), width)

    def block_rows(j):
        return pl.ds(pl.multiple_of(j * width, 128), width)

    def wrows(j):
        return pl.ds(pl.multiple_of(j * per_row, per_row), per_row)

    def remote(src, dst, s, r, wide_id, narrow_id):
        return pltpu.make_async_remote_copy(
            src_ref=src, dst_ref=dst, send_sem=s, recv_sem=r,
            device_id=(wide_id, narrow_id), device_id_type=MESH,
        )

    def chunks(count, body, unroll=False):
        lax.fori_loop(
            0, count // CHUNK, lambda c, _: (body(c * CHUNK), 0)[1], 0, unroll=unroll
        )

    def at(i, start, size=CHUNK):
        return pl.ds(pl.multiple_of(i * ROWS + start, CHUNK), size)

    def a0_copy(buf, kind, i, block, s, r, to):
        part = buf.at[rows(i), cols(block)]
        return remote(part, part, R["a0_s"].at[kind, i, s], R["a0_r"].at[kind, i, r], w, to)

    def a0_start(buf, kind, i):
        a0_copy(buf, kind, i, z, 0, 0, mate).start()
        a0_copy(buf, kind, i, z, 1, far, oi).start()

    def a0_relay(buf, kind, i):
        @when(inner)
        def _():
            for r, block in ((1, oi), (2, oo)):
                a0_copy(buf, kind, i, block, r + 1, r, mate).wait_recv()
                a0_copy(buf, kind, i, block, r + 1, r, mate).start()

    def a0_finish(buf, kind, i):
        a0_copy(buf, kind, i, mate, 0, 0, mate).wait_recv()

        @when(outer)
        def _():
            for r, block in ((1, oi), (2, oo)):
                a0_copy(buf, kind, i, block, r + 1, r, mate).wait_recv()

        a0_copy(buf, kind, i, z, 0, 0, mate).wait_send()
        a0_copy(buf, kind, i, z, 1, far, oi).wait_send()

        @when(inner)
        def _():
            for r, block in ((1, oi), (2, oo)):
                a0_copy(buf, kind, i, block, r + 1, r, mate).wait_send()

    def ag_copy(buf, kind, i, block, s, r, to):
        part = buf.at[rows(i), cols(block)]
        return remote(part, part, R["ag_s"].at[kind, i, s], R["ag_r"].at[kind, i, r], w, to)

    def ag_start(buf, kind, i):
        @when(inner)
        def _():
            for u in range(2):
                ag_copy(buf, kind, i, near_half + u, u, u, oi).start()
            for u in range(2):
                ag_copy(buf, kind, i, near_half + u, 2 + u, 2 + u, mate).start()

    def ag_relay(buf, kind, i):
        @when(inner)
        def _():
            for u in range(2):
                ag_copy(buf, kind, i, far_half + u, 4 + u, u, mate).wait_recv()
                ag_copy(buf, kind, i, far_half + u, 4 + u, u, mate).start()

    def ag_finish(buf, kind, i):
        @when(outer)
        def _():
            for u in range(2):
                ag_copy(buf, kind, i, near_half + u, 2 + u, 2 + u, mate).wait_recv()
            for u in range(2):
                ag_copy(buf, kind, i, far_half + u, 4 + u, u, mate).wait_recv()

    def ag_drain(buf, kind, i):
        @when(inner)
        def _():
            for u in range(2):
                ag_copy(buf, kind, i, near_half + u, u, u, oi).wait_send()
                ag_copy(buf, kind, i, near_half + u, 2 + u, 2 + u, mate).wait_send()
                ag_copy(buf, kind, i, far_half + u, 4 + u, u, mate).wait_send()

    def rs_copy(bank, i, q, slot, to):
        return remote(
            R["stage"].at[bank, i, q], R["slot"].at[bank, i, slot],
            R["rs_s"].at[bank, i, q], R["rs_r"].at[bank, i, slot], w, to,
        )

    def rs_blocks(bank, i, block):
        for q in range(4):
            y = block((far_half if q < 2 else near_half) + q % 2)

            @when(outer)
            def _():
                R["stage"][bank, i, q] = y.astype(BF16)
                rs_copy(bank, i, q, q, mate).start()

            @when(inner)
            def _():
                if q < 2:
                    R["held"][i, q] = y
                else:
                    R["own"][bank, i, q - 2] = y

    def rs_relay(bank, i):
        @when(inner)
        def _():
            for q in range(2):
                rs_copy(bank, i, q, q, mate).wait_recv()

                def body(c):
                    part = pl.ds(pl.multiple_of(c, CHUNK), CHUNK)
                    total = R["held"][i, q, part] + R["slot"][bank, i, q, part].astype(F32)
                    R["stage"][bank, i, q, part] = total.astype(BF16)

                chunks(ROWS, body, True)
                rs_copy(bank, i, q, 4 + q, oi).start()

    def rs_wait(bank, i):
        @when(inner)
        def _():
            for q in range(2, 4):
                rs_copy(bank, i, q, q, mate).wait_recv()
            for q in range(2):
                rs_copy(bank, i, q, 4 + q, oi).wait_recv()
            for q in range(2):
                rs_copy(bank, i, q, 4 + q, oi).wait_send()

        @when(outer)
        def _():
            for q in range(4):
                rs_copy(bank, i, q, q, mate).wait_send()

    def rs_sum(bank, i, part):
        slots = R["slot"]
        return jnp.concatenate(
            [
                R["own"][bank, i, u, part]
                + slots[bank, i, 2 + u, part].astype(F32)
                + slots[bank, i, 4 + u, part].astype(F32)
                for u in range(2)
            ],
            axis=1,
        )

    def near_row(row):
        return jnp.concatenate([R["gn"][near_half + u, row] for u in range(2)], axis=1)

    def t_copy(i, q, r, to):
        return remote(
            R["ts"].at[i], R["tr"].at[i, r], R["t_s"].at[i, q], R["t_r"].at[i, r], w, to
        )

    def t_send(i):
        lane = lax.broadcasted_iota(jnp.int32, (8, 128), 0)
        first = jnp.where(lane < 4, 1.0, 0.0).astype(F32)
        second = 1.0 - first
        R["ts"][i] = exact_dot(first, R["vs"][0], ((1,), (1,))) + exact_dot(
            second, R["vs"][1], ((1,), (1,))
        )
        @when(outer)
        def _():
            t_copy(i, 0, 0, mate).start()

        t_copy(i, 1, far, oi).start()

    def t_total(i):
        for q in range(3):
            t_copy(i, 0, q, mate).wait_recv()
        total = (R["ts"][i] + R["tr"][i, 0]) + (R["tr"][i, 1] + R["tr"][i, 2])
        row = lax.broadcasted_iota(jnp.int32, (8, 128), 0)
        lane = lax.broadcasted_iota(jnp.int32, (8, 128), 1)
        pick = ((row == 0) & (lane < 64)) | ((row == 4) & (lane >= 64))
        R["vs"][0] = exact_dot(total, jnp.where(pick, 1.0, 0.0).astype(F32), ((0,), (0,)))

    def t_drain(i):
        @when(outer)
        def _():
            t_copy(i, 0, 0, mate).wait_send()

        t_copy(i, 1, far, oi).wait_send()

    def weights(l, piece):
        if piece == 0:
            return R["wq"].at[l], R["wq_in"].at[l]
        if piece == 1:
            return R["wp"].at[l], R["wo"].at[l]
        if piece == 2:
            return R["wf"].at[l, :, 0:hidden], R["wu_in"].at[l]
        return R["wf"].at[l, :, hidden : 2 * hidden], R["wd"].at[l]

    def rows_of(ref, k):
        return ref.at[wrows(k)] if len(ref.shape) == 2 else ref.at[:, wrows(k)]

    def w_local(l, piece):
        full, shard = weights(l, piece)
        return pltpu.make_async_copy(shard, rows_of(full, w), R["w_l"].at[l, piece])

    def w_send(l, piece, s, to):
        full, shard = weights(l, piece)
        return remote(
            shard, rows_of(full, w), R["w_s"].at[l, piece, s], R["w_r"].at[l, piece, mine], to, z
        )

    def w_pair(l, piece):
        full, shard = weights(l, piece)
        return remote(
            shard, rows_of(full, w),
            R["w_s"].at[l, piece, half - 1], R["w_f"].at[l, piece, mine], partner, z,
        )

    def w_cross(l, piece, k, parity):
        full, _ = weights(l, piece)
        part = rows_of(full, 2 * k + parity)
        return remote(
            part, part, R["w_g"].at[l, piece, k], R["w_f"].at[l, piece, k], partner, z
        )

    def w_start(l, piece):
        for j in range(1, half):
            w_send(l, piece, j - 1, 2 * ((mine + j) % half) + par).start()
        w_pair(l, piece).start()
        w_local(l, piece).start()

    def w_relay(l, piece):
        full, shard = weights(l, piece)
        for j in range(1, half):
            k = (mine + half - j) % half
            remote(
                shard, rows_of(full, 2 * k + par),
                R["w_s"].at[l, piece, 0], R["w_r"].at[l, piece, k], partner, z,
            ).wait_recv()
            w_cross(l, piece, k, par).start()

    def w_finish(l, piece):
        for j in range(half):
            w_cross(l, piece, (mine + half - j) % half, 1 - par).wait_recv()
        w_local(l, piece).wait()
        for s in range(half - 1):
            w_send(l, piece, s, partner).wait_send()
        w_pair(l, piece).wait_send()
        for j in range(1, half):
            w_cross(l, piece, (mine + j) % half, par).wait_send()

    def grads(l, piece):
        if piece == 1:
            return R["gf"], R["pf"], R["cf"]
        room = pl.ds(l * half, half)
        if piece == 0:
            return R["gq"], R["pq"].at[room], R["cq"].at[room]
        return R["go"], R["po"].at[room], R["co"].at[room]

    def p_copy(l, piece, k):
        full, theirs, _ = grads(l, piece)
        return remote(
            rows_of(full, 2 * k + 1 - par), theirs.at[k],
            R["p_s"].at[piece, k], R["p_r"].at[l, piece, k], partner, z,
        )

    def c_copy(l, piece, k, source):
        full, _, came = grads(l, piece)
        return remote(
            rows_of(full, 2 * k + par), came.at[source],
            R["c_s"].at[piece, k], R["c_r"].at[l, piece, source], 2 * k + par, z,
        )

    def r_copies(l, piece):
        pairs = (
            ((R["rq"], R["gwq"]),),
            ((R["ru"], R["gwu"]), (R["rd"], R["gwd"])),
            ((R["ro"], R["gwo"]),),
        )[piece]
        return [
            pltpu.make_async_copy(total, result.at[l], R["r_s"].at[l, piece + 2 * q])
            for q, (total, result) in enumerate(pairs)
        ]

    def g_start(l, piece, b):
        pairs = half * 256 // D
        for k in range(pairs):
            p_copy(l, piece, b * pairs + k).start()

    def g_mid(l, piece):
        full, theirs, _ = grads(l, piece)
        for j in range(1, half + 1):
            k = (mine + j) % half
            p_copy(l, piece, k).wait_recv()

            def body(c):
                here = pl.ds(pl.multiple_of((2 * k + par) * per_row + c, CHUNK), CHUNK)
                part = pl.ds(pl.multiple_of(c, CHUNK), CHUNK)
                ours = full.at[:, here] if piece == 0 else full.at[here]
                other = theirs.at[k, :, part] if piece == 0 else theirs.at[k, part]
                ours[...] = (ours[...].astype(F32) + other[...].astype(F32)).astype(BF16)

            chunks(per_row, body)
            if j < half:
                c_copy(l, piece, k, mine).start()

    def g_end(l, piece):
        full, _, came = grads(l, piece)
        for j in range(1, half):
            k = (mine + half - j) % half
            c_copy(l, piece, k, k).wait_recv()

        @when(l < LAYERS - 1)
        def _():
            for copy in r_copies(l + 1, piece):
                copy.wait()

        others = [(mine + j) % half for j in range(1, half)]
        if piece != 2:
            def body(c):
                part = pl.ds(pl.multiple_of(c, CHUNK), CHUNK)
                here = pl.ds(pl.multiple_of(w * per_row + c, CHUNK), CHUNK)
                if piece == 0:
                    total = full[:, here].astype(F32)
                    for k in others:
                        total = total + came[k, :, part].astype(F32)
                    R["rq"][:, part] = total
                else:
                    total = full[here, 0:hidden].astype(F32)
                    for k in others:
                        total = total + came[k, part, 0:hidden].astype(F32)
                    R["ru"][part] = total

            chunks(per_row, body)
        if piece != 0:
            first = hidden if piece == 1 else 0
            result = R["rd"] if piece == 1 else R["ro"]
            for c in range(0, result.shape[0], 256):
                lanes = slice(first + c, first + c + 256)
                total = full[wrows(w), lanes].astype(F32)
                for k in others:
                    total = total + came[k, :, lanes].astype(F32)
                result[c : c + 256] = total.T
        for copy in r_copies(l, piece):
            copy.start()
        for k in range(half):
            p_copy(l, piece, k).wait_send()
        for j in range(1, half):
            c_copy(l, piece, (mine + j) % half, mine).wait_send()

    def v_copy(l, j, source):
        to = (w + j) % wide
        return remote(
            R["sv"].at[l], R["rv"].at[l, source],
            R["v_s"].at[l, j], R["v_r"].at[l, source], to, z,
        )

    def h_copy(l, j, source, to_mate):
        to = (w + j) % wide
        block, narrow = (1 - inside, mate) if to_mate else (inside, z)
        return remote(
            R["sh"].at[l, block], R["rh"].at[l, source],
            R["h_s"].at[l, 1 if to_mate else 0, j], R["h_r"].at[l, source], to, narrow,
        )

    def v_start(l):
        for j in range(1, wide):
            v_copy(l, j, w).start()

    def h_start(l):
        @when(inner)
        def _():
            for j in range(wide):
                if j > 0:
                    h_copy(l, j, w, False).start()
                h_copy(l, j, w, True).start()
            R["rh"][l, w] = R["sh"][l, inside]

    def v_end(l):
        total = R["sv"][l]
        for j in range(1, wide):
            source = (w + j) % wide
            v_copy(l, j, source).wait_recv()
            total = total + R["rv"][l, source]
        R["gbqv"][l] = total[0:2]
        for b in range(hidden // width):
            R["gbup"][pl.ds(l, 1), b * width : (b + 1) * width] = total[2 + b : 3 + b]
        for j in range(1, wide):
            v_copy(l, j, w).wait_send()

    def h_end(l):
        @when(outer)
        def _():
            h_copy(l, 0, w, True).wait_recv()

        total = R["rh"][l, w]
        for j in range(1, wide):
            source = (w + j) % wide
            h_copy(l, j, source, True).wait_recv()
            total = total + R["rh"][l, source]
        R["gng"][l] = total[V_GAIN : V_GAIN + 2]
        R["gnb"][l] = total[V_BIAS : V_BIAS + 2]
        R["gbo"][pl.ds(l, 1)] = total[V_OUT : V_OUT + 1]
        R["gbd"][pl.ds(l, 1)] = total[V_DOWN : V_DOWN + 1]

        @when(inner)
        def _():
            for j in range(wide):
                if j > 0:
                    h_copy(l, j, w, False).wait_send()
                h_copy(l, j, w, True).wait_send()

    def norm_in(buf, l, branch, i):
        at_norm = 2 * l + branch
        scale = [R["gn"][j, pl.ds(G_GAIN + at_norm, 1)] for j in range(4)]
        shift = [R["gn"][j, pl.ds(G_BIAS + at_norm, 1)] for j in range(4)]
        scale = jnp.concatenate(scale, axis=1)
        shift = jnp.concatenate(shift, axis=1)

        def body(c):
            here = at(i, c)
            raw = buf[here, :].astype(F32)
            mean = jnp.sum(raw, axis=1, keepdims=True) * (1.0 / D)
            square = jnp.sum(raw * raw, axis=1, keepdims=True) * (1.0 / D)
            s = lax.rsqrt(square - mean * mean + EPS)
            R["act"][at_norm, here] = ((raw - mean) * s * scale + shift).astype(BF16)
            R["centre"][here] = R["centre"][here] + mean
            R["spread"][at_norm, here] = s

        chunks(ROWS, body, True)

    def norm_keep(l, branch, i):
        at_norm = 2 * l + branch

        @when(inner)
        def _():
            def body(c):
                here = at(i, c)
                R["n"][at_norm, here] = (R["r"][here] - R["centre"][here]) * R["spread"][
                    at_norm, here
                ]

            chunks(ROWS, body, True)

    def norm_back(bank, l, branch, i, out_row):
        at_norm = 2 * l + branch
        rs_wait(bank, i)
        t_drain(i)

        @when(inner)
        def _():
            scale = near_row(pl.ds(G_GAIN + at_norm, 1))
            t_total(i)

            def body(c, carry):
                gain_sum, bias_sum, g_sum = carry
                c = c * CHUNK
                here = at(i, c)
                part = pl.ds(pl.multiple_of(c, CHUNK), CHUNK)
                upstream = rs_sum(bank, i, part)
                normed = R["n"][at_norm, here]
                first = R["vs"][0, part, 0:1] * (1.0 / D)
                second = R["vs"][0, part, 64:65] * (1.0 / D)
                grown = R["g"][here] + (
                    upstream * scale - first - normed * second
                ) * R["spread"][at_norm, here]
                R["g"][here] = grown
                gain_sum = gain_sum + jnp.sum(upstream * normed, axis=0, keepdims=True)
                bias_sum = bias_sum + jnp.sum(upstream, axis=0, keepdims=True)
                g_sum = g_sum + jnp.sum(grown, axis=0, keepdims=True)
                return gain_sum, bias_sum, g_sum

            zero = jnp.zeros((1, 2 * width), F32)
            gain_sum, bias_sum, g_sum = lax.fori_loop(
                0, ROWS // CHUNK, body, (zero, zero, zero), unroll=True
            )
            half_add(l, V_GAIN + branch, gain_sum)
            half_add(l, V_BIAS + branch, bias_sum)
            if out_row is not None:
                half_add(l, out_row, g_sum)

    def half_add(l, row, value):
        for u in range(2):
            there = slice(row, row + 1)
            part = value[:, u * width : (u + 1) * width]
            R["sh"][l, u, there] = R["sh"][l, u, there] + part

    def send_sums(at_norm, i, block_of):
        R["vs"][0, 0:ROWS] = jnp.zeros((ROWS, 128), F32)
        R["vs"][1, 0:ROWS] = jnp.zeros((ROWS, 128), F32)
        l, branch = at_norm

        def block(j):
            y = block_of(j)
            R["tmp"][...] = y
            scale = R["gn"][j, pl.ds(G_GAIN + 2 * l + branch, 1)]
            shift = R["gn"][j, pl.ds(G_BIAS + 2 * l + branch, 1)]

            def body(c):
                part = pl.ds(pl.multiple_of(c, CHUNK), CHUNK)
                value = R["tmp"][part]
                normed = R["act"][2 * l + branch, at(i, c), cols(j)].astype(F32) - shift
                first = value * scale
                second = value * normed
                for m in range(width // 128):
                    lanes = slice(m * 128, (m + 1) * 128)
                    R["vs"][0, part] = R["vs"][0, part] + first[:, lanes]
                    R["vs"][1, part] = R["vs"][1, part] + second[:, lanes]

            chunks(ROWS, body, True)
            return R["tmp"][...]

        return block

    head_lanes = [slice(h * HEAD_DIM, (h + 1) * HEAD_DIM) for h in range(heads)]

    def attention(l, i):
        keys = pl.ds(i * KEYS, KEYS)
        column = lax.broadcasted_iota(jnp.int32, (ROWS, KEYS), 1)
        factor = 1.0 / math.sqrt(HEAD_DIM)
        scores = [
            dot_t(R["q"][l, rows(i), lanes], R["k"][l, keys, lanes]) for lanes in head_lanes
        ]
        probs = []
        for h in range(heads):
            masked = jnp.where(column < SEQ, scores[h] * factor, -jnp.inf)
            top = jnp.max(masked, axis=1, keepdims=True)
            grown = jnp.exp(masked - top)
            prob = grown / jnp.sum(grown, axis=1, keepdims=True)
            R["prob"][(l * images + i) * heads + h] = prob
            probs.append(prob.astype(BF16))
        mixed = [dot(probs[h], R["v"][l, keys, head_lanes[h]]) for h in range(heads)]
        R["o"][l, rows(i)] = jnp.concatenate(mixed, axis=1).astype(BF16)

    def f1(l, i):
        buf = R["x"].at[0]

        @when(l > 0)
        def _():
            ag_finish(buf, 0, i)

        norm_in(buf, l, 0, i)
        act = R["act"].at[2 * l, rows(i)]
        kept = pl.ds(i * KEYS, ROWS)
        bq = R["bq_in"][l, 0:1]
        bv = R["bq_in"][l, 1:2]
        R["q"][l, rows(i)] = (dot(act[...], R["wq"][l, 0]) + bq).astype(BF16)
        R["k"][l, kept] = dot(act[...], R["wq"][l, 1]).astype(BF16)
        R["v"][l, kept] = (dot(act[...], R["wq"][l, 2]) + bv).astype(BF16)
        if i == 0:
            @when(l == 0)
            def _():
                w_relay(l, 1)

        attention(l, i)
        if i == 0:
            w_finish(l, 1)

        def block(j):
            return dot_t(R["o"][l, rows(i)], R["wp"][l, block_rows(j)])

        rs_blocks(0, i, block)
        norm_keep(l, 0, i)

    def f2(l, i):
        buf = R["x"].at[1]
        ag_finish(buf, 1, i)
        norm_in(buf, l, 1, i)

        def body(b, _):
            lanes = cols(b)
            pre = dot(R["act"][2 * l + 1, rows(i)], R["wf"][l, :, lanes])
            pre = pre + R["bu_in"][pl.ds(l, 1), lanes]
            cdf = 0.5 * (1.0 + lax.erf(pre * 0.7071067811865476))
            R["u"][l, rows(i), lanes] = (pre * cdf).astype(BF16)
            R["slope"][l, rows(i), lanes] = (
                cdf + pre * jnp.exp(-0.5 * pre * pre) * 0.3989422804014327
            )
            return 0

        lax.fori_loop(0, hidden // width, body, 0)
        if i == 0:
            w_finish(l, 3)

        def block(j):
            return dot_t(R["u"][l, rows(i)], R["wf"][l, block_rows(j), hidden : 2 * hidden])

        rs_blocks(1, i, block)
        norm_keep(l, 1, i)

    def residual(bank, i, bias_row, kind):
        rs_wait(bank, i)

        @when(inner)
        def _():
            bias = near_row(bias_row)

            def body(c):
                here = at(i, c)
                part = pl.ds(pl.multiple_of(c, CHUNK), CHUNK)
                grown = R["r"][here] + (rs_sum(bank, i, part) + bias)
                R["r"][here] = grown
                if kind is not None:
                    out = (grown - R["centre"][here]).astype(BF16)
                    R["x"][kind, here, half_cols] = out

            chunks(ROWS, body, True)

        if kind is not None:
            ag_start(R["x"].at[kind], kind, i)

    def fin_copy(which, i):
        source = (R["r"], R["g"])[which]
        there = pl.ds(pl.multiple_of((1 - inside) * width, 128), width)
        return remote(
            source.at[rows(i), there], R["held"].at[i, which],
            R["fin_s"].at[which, i], R["fin_r"].at[which, i], w, mate,
        )

    def fin_start(which, i):
        @when(inner)
        def _():
            fin_copy(which, i).start()

    def fin_end(which, i):
        source, result = ((R["r"], R["out"]), (R["g"], R["gin"]))[which]
        there = pl.ds(i * SEQ, SEQ)

        @when(inner)
        def _():
            here = pl.ds(pl.multiple_of(inside * width, 128), width)
            result[there] = source[pl.ds(i * ROWS, SEQ), here]
            fin_copy(which, i).wait_send()

        @when(outer)
        def _():
            fin_copy(which, i).wait_recv()
            result[there] = R["held"][i, which, 0:SEQ]

    def post_f1(l, i):
        @when(l > 0)
        def _():
            ag_drain(R["x"].at[0], 0, i)

        residual(0, i, pl.ds(G_OUT + l, 1), 1)

    def post_f2(l, i, last):
        ag_drain(R["x"].at[1], 1, i)
        residual(1, i, pl.ds(G_DOWN + l, 1), None if last else 0)
        if last:
            fin_start(0, i)

    def send_grad(slot, kind, i):
        buf = R["e"].at[slot]

        @when(inner)
        def _():
            def body(c):
                here = at(i, c)
                buf[here, half_cols] = R["g"][here].astype(BF16)

            chunks(ROWS, body, True)

        ag_start(buf, kind, i)

    def b2(l, i):
        e = R["e"].at[2 * l + 1]

        @when(l < LAYERS - 1)
        def _():
            ag_finish(e, 2, i)

        def body(b, _):
            lanes = cols(b)
            back = pl.ds(pl.multiple_of(hidden + b * width, 128), width)
            dz = dot(e[rows(i), :], R["wf"][l, :, back]) * R["slope"][l, rows(i), lanes]
            R["f"][rows(i), lanes] = dz.astype(BF16)
            row = pl.ds(V_UP + b, 1)
            R["sv"][l, row] = R["sv"][l, row] + jnp.sum(dz, axis=0, keepdims=True)
            return 0

        lax.fori_loop(0, hidden // width, body, 0)

        def block(j):
            return dot_t(R["f"][rows(i)], R["wf"][l, block_rows(j), 0:hidden])

        rs_blocks(0, i, send_sums((l, 1), i, block))
        t_send(i)
        add_down(l, i)

    def b1(l, i):
        e = R["e"].at[2 * l]
        ag_finish(e, 3, i)
        keys = pl.ds(i * KEYS, KEYS)
        R["do"][...] = dot(e[rows(i), :], R["wp"][l]).astype(BF16)
        if i == images - 1:
            grad_out(l)
        factor = 1.0 / math.sqrt(HEAD_DIM)
        dos = [R["do"][:, lanes] for lanes in head_lanes]
        dps = [dot_t(dos[h], R["v"][l, keys, head_lanes[h]]) for h in range(heads)]
        dvs, dss = [], []
        for h in range(heads):
            prob = R["prob"][(l * images + i) * heads + h]
            dvs.append(t_dot(prob.astype(BF16), dos[h])[0:ROWS])
            delta = jnp.sum(prob * dps[h], axis=1, keepdims=True)
            dss.append((prob * (dps[h] - delta) * factor).astype(BF16))
        dqs = [dot(dss[h], R["k"][l, keys, head_lanes[h]]) for h in range(heads)]
        dks = [t_dot(dss[h], R["q"][l, rows(i), head_lanes[h]])[0:ROWS] for h in range(heads)]
        dq, dk, dv = [jnp.concatenate(parts, axis=1) for parts in (dqs, dks, dvs)]
        for part, value in ((0, dq), (1, dk), (2, dv)):
            R["d"][rows(i), part * width : (part + 1) * width] = value.astype(BF16)
        for row, value in ((V_QV, dq), (V_QV + 1, dv)):
            there = slice(row, row + 1)
            R["sv"][l, there] = R["sv"][l, there] + jnp.sum(value, axis=0, keepdims=True)

        def block(j):
            parts = [
                dot_t(R["d"][rows(i), m * width : (m + 1) * width], R["wq"][l, m, block_rows(j)])
                for m in range(3)
            ]
            return parts[0] + parts[1] + parts[2]

        rs_blocks(1, i, send_sums((l, 0), i, block))
        t_send(i)

    def add_down(l, i):
        @when(inner)
        def _():
            def body(c, total):
                return total + jnp.sum(R["g"][at(i, c * CHUNK)], axis=0, keepdims=True)

            zero = jnp.zeros((1, 2 * width), F32)
            half_add(l, V_DOWN, lax.fori_loop(0, ROWS // CHUNK, body, zero, unroll=True))

    def post_b2(l, i):
        @when(l < LAYERS - 1)
        def _():
            ag_drain(R["e"].at[2 * l + 1], 2, i)

        norm_back(0, l, 1, i, V_OUT)
        send_grad(2 * l, 3, i)

    def post_b1(l, i):
        ag_drain(R["e"].at[2 * l], 3, i)
        norm_back(1, l, 0, i, None)

        @when(l > 0)
        def _():
            send_grad(2 * l - 1, 2, i)

        @when(l == 0)
        def _():
            fin_start(1, i)

    def grad_block(b):
        block = (mine * 2 * per_row // 256 + 1 + b) % (D // 256)
        return block, pl.ds(pl.multiple_of(block * 256, 256), 256)

    def grad_ffn(l, first, last):
        def body(b, _):
            block, lanes = grad_block(b)
            up = t_dot(R["act"][2 * l + 1, :, lanes], R["f"][...])
            R["gf"][lanes, 0:hidden] = up.astype(BF16)
            down = t_dot(R["e"][2 * l + 1, :, lanes], R["u"][l])
            R["gf"][lanes, hidden : 2 * hidden] = down.astype(BF16)
            g_start(l, 1, block)
            return 0

        lax.fori_loop(first, last, body, 0)

    def grad_qkv(l):
        def body(b, _):
            block, lanes = grad_block(b)
            qkv = t_dot(R["act"][2 * l, :, lanes], R["d"][...])
            for m in range(3):
                R["gq"][m, lanes] = qkv[:, m * width : (m + 1) * width].astype(BF16)
            g_start(l, 0, block)
            return 0

        lax.fori_loop(0, D // 256, body, 0)

    def grad_out(l):
        def body(b, _):
            block, lanes = grad_block(b)
            out = t_dot(R["e"][2 * l, :, lanes], R["o"][l])
            R["go"][lanes] = out.astype(BF16)
            g_start(l, 2, block)
            return 0

        lax.fori_loop(0, D // 256, body, 0)

    def spread_rows(source, result):
        tokens = images * SEQ
        wide_rows = R["r"].at[:, 0:width]
        wide_rows[0:tokens] = source[...].astype(F32)
        row = lax.broadcasted_iota(jnp.int32, (ROWS, width), 0)
        for i in image:
            part = wide_rows[i * SEQ : i * SEQ + ROWS]
            result[rows(i), cols(z)] = jnp.where(row < SEQ, part, 0.0).astype(BF16)

    barrier = pltpu.get_barrier_semaphore()
    for j in range(1, wide):
        pl.semaphore_signal(barrier, 1, device_id=((w + j) % wide, z), device_id_type=MESH)
    for j in range(1, 4):
        pl.semaphore_signal(barrier, 1, device_id=(w, (z + j) % 4), device_id_type=MESH)
    image = range(images)
    first_x = R["x"].at[0]
    last_e = R["e"].at[2 * LAYERS - 1]
    R["r"][...] = jnp.zeros_like(R["r"])
    spread_rows(R["x_in"], first_x)
    for l in range(LAYERS):
        R["gb"][G_GAIN + 2 * l : G_GAIN + 2 * l + 2] = R["ng_in"][l]
        R["gb"][G_BIAS + 2 * l : G_BIAS + 2 * l + 2] = R["nb_in"][l]
    R["gb"][G_OUT : G_OUT + LAYERS] = R["bo_in"][...]
    R["gb"][G_DOWN : G_DOWN + LAYERS] = R["bd_in"][...]
    R["gn"][z] = R["gb"][...]
    for l in range(LAYERS):
        R["wo"][l] = R["wo_in"][l].T
    pl.semaphore_wait(barrier, 3 + wide - 1)

    w_start(0, 0)
    for i in image:
        a0_start(first_x, 0, i)

    def gn_copy(q, r, to):
        return remote(R["gb"], R["gn"].at[z], R["gn_s"].at[q], R["gn_r"].at[r], w, to)

    gn_copy(0, 0, mate).start()
    gn_copy(1, far, oi).start()
    gn_copy(2, far, oo).start()
    w_start(0, 1)
    for l in range(LAYERS):
        R["wd"][l] = R["wd_in"][l].T
    spread_rows(R["cot_in"], last_e)
    R["centre"][...] = jnp.zeros_like(R["centre"])
    R["sv"][...] = jnp.zeros_like(R["sv"])
    R["sh"][...] = jnp.zeros_like(R["sh"])
    R["vs"][...] = jnp.zeros_like(R["vs"])
    for name in ("k", "v"):
        for i in image:
            empty = jnp.zeros((LAYERS, KEYS - ROWS, width), BF16)
            R[name][:, i * KEYS + ROWS : (i + 1) * KEYS] = empty
    for i in image:
        a0_relay(first_x, 0, i)
    for i in image:
        a0_start(last_e, 1, i)
    w_start(0, 2)
    w_start(0, 3)
    for l in range(1, LAYERS):
        for piece in range(4):
            w_start(l, piece)
    for q in range(3):
        gn_copy(q, q, mate).wait_recv()
    for q in range(3):
        gn_copy(q, q, mate).wait_send()
    w_relay(0, 0)
    for i in image:
        a0_finish(first_x, 0, i)

    @when(inner)
    def _():
        R["r"][...] = first_x[:, half_cols].astype(F32)

    w_finish(0, 0)
    for i in image:
        a0_relay(last_e, 1, i)

    def forward(l, _):
        f1(l, 0)

        @when(l > 0)
        def _():
            ag_relay(R["x"].at[0], 0, 1)

        rs_relay(0, 0)
        f1(l, 1)
        post_f1(l, 0)
        w_relay(l, 2)
        rs_relay(0, 1)
        ag_relay(R["x"].at[1], 1, 0)
        w_relay(l, 3)
        post_f1(l, 1)
        w_finish(l, 2)
        f2(l, 0)
        ag_relay(R["x"].at[1], 1, 1)
        rs_relay(1, 0)
        f2(l, 1)

        @when(l < LAYERS - 1)
        def _():
            w_relay(l + 1, 0)
            post_f2(l, 0, False)
            rs_relay(1, 1)
            ag_relay(R["x"].at[0], 0, 0)
            w_relay(l + 1, 1)
            post_f2(l, 1, False)
            w_finish(l + 1, 0)

        return 0

    lax.fori_loop(0, LAYERS, forward, 0)
    for i in image:
        a0_finish(last_e, 1, i)

    @when(inner)
    def _():
        R["g"][...] = last_e[:, half_cols].astype(F32)

    def backward(step, _):
        l = LAYERS - 1 - step
        top = l == LAYERS - 1
        e2 = R["e"].at[2 * l + 1]
        e1 = R["e"].at[2 * l]
        b2(l, 0)

        @when(top)
        def _():
            rs_relay(1, 1)

        @when(l < LAYERS - 1)
        def _():
            ag_relay(e2, 2, 1)

        rs_relay(0, 0)
        b2(l, 1)

        @when(top)
        def _():
            post_f2(l, 0, True)
            post_f2(l, 1, True)

        grad_ffn(l, 0, 2)
        post_b2(l, 0)
        grad_ffn(l, 2, 4)
        rs_relay(0, 1)

        @when(l < LAYERS - 1)
        def _():
            g_end(l + 1, 0)
            g_end(l + 1, 2)
            v_end(l + 1)
            h_end(l + 1)

        g_mid(l, 1)
        ag_relay(e1, 3, 0)
        post_b2(l, 1)
        b1(l, 0)
        ag_relay(e1, 3, 1)
        rs_relay(1, 0)

        b1(l, 1)
        post_b1(l, 0)
        grad_qkv(l)
        g_mid(l, 2)
        g_mid(l, 0)
        rs_relay(1, 1)

        @when(l > 0)
        def _():
            ag_relay(R["e"].at[2 * l - 1], 2, 0)

        g_end(l, 1)
        v_start(l)
        post_b1(l, 1)
        h_start(l)
        return 0

    lax.fori_loop(0, LAYERS, backward, 0)
    first = jnp.int32(0)
    g_end(first, 2)
    v_end(0)
    for i in image:
        fin_end(0, i)
    g_end(first, 0)
    for i in image:
        fin_end(1, i)
    h_end(0)
    for piece in range(3):
        for copy in r_copies(0, piece):
            copy.wait()


def deliver(*refs):
    count = (len(refs) - 2) // 3
    sources, results, rooms = (refs[i * count : (i + 1) * count] for i in range(3))
    came, gone = refs[3 * count :]

    def copy(i, inward):
        if inward:
            return pltpu.make_async_copy(sources[i], rooms[i], came.at[i])
        return pltpu.make_async_copy(rooms[i], results[i], gone.at[i])

    for i in range(count):
        copy(i, True).start()
    for i in range(count):
        copy(i, True).wait()
        copy(i, False).start()
    for i in range(count):
        copy(i, False).wait()


def body(wide, inputs, norm_gain, norm_bias, w_qkv, b_qv, w_out, b_out, w_up, b_up, w_down, b_down, cotangent):
    tokens, width = inputs.shape
    images = tokens // SEQ
    hidden = w_up.shape[2]
    per_row = w_up.shape[1]
    half = wide // 2
    scratch = scratch_of(half, per_row, width, hidden, images)
    names = IN_NAMES + OUT_NAMES + tuple(scratch)
    vmem = pl.BlockSpec(memory_space=pltpu.VMEM)
    anywhere = pl.BlockSpec(memory_space=pl.ANY)

    def shaped(*shape):
        return jax.ShapeDtypeStruct(shape, F32)

    results = pl.pallas_call(
        functools.partial(kernel, wide, images, width, hidden, names),
        out_shape=(
            shaped(tokens, width),
            shaped(tokens, width),
            shaped(LAYERS, 2, width),
            shaped(LAYERS, 2, width),
            shaped(LAYERS, 3, per_row, width),
            shaped(LAYERS, 2, width),
            shaped(LAYERS, width, per_row),
            shaped(LAYERS, width),
            shaped(LAYERS, per_row, hidden),
            shaped(LAYERS, hidden),
            shaped(LAYERS, hidden, per_row),
            shaped(LAYERS, width),
        ),
        in_specs=[vmem] * 10 + [anywhere] * 2,
        out_specs=(
            vmem, vmem, vmem, vmem, anywhere, vmem, anywhere, vmem, anywhere, vmem, anywhere, vmem,
        ),
        scratch_shapes=list(scratch.values()),
        compiler_params=pltpu.CompilerParams(
            collective_id=0, has_side_effects=True, vmem_limit_bytes=67043328
        ),
        name="encoder_step",
    )(
        inputs, cotangent, norm_gain, norm_bias, b_qv, b_out, b_up, b_down, w_out, w_down,
        w_qkv.transpose(0, 2, 1, 3), w_up,
    )
    shapes = [result.shape for result in results]
    count = len(shapes)
    done = pl.pallas_call(
        deliver,
        out_shape=[shaped(*shape) for shape in shapes],
        in_specs=[anywhere] * count,
        out_specs=[anywhere] * count,
        scratch_shapes=[pltpu.VMEM(shape, F32) for shape in shapes]
        + [pltpu.SemaphoreType.DMA((count,))] * 2,
        compiler_params=pltpu.CompilerParams(vmem_limit_bytes=67043328),
        name="deliver",
    )(*results)
    return (*done[:4], done[4].transpose(0, 2, 1, 3), *done[5:])


def solution(mesh):
    rows = P("wide", "narrow")
    vector2 = P(None, None, "narrow")
    vector = P(None, "narrow")
    down_cols = P(None, "narrow", "wide")
    up_rows = P(None, "wide", "narrow")
    qkv = P(None, "wide", None, "narrow")
    return jax.shard_map(
        functools.partial(body, mesh.shape["wide"]),
        mesh=mesh,
        in_specs=(
            rows, vector2, vector2, qkv, vector2, down_cols, vector, up_rows, vector, down_cols,
            vector, rows,
        ),
        out_specs=(
            rows, rows, vector2, vector2, qkv, vector2, down_cols, vector, up_rows, vector,
            down_cols, vector,
        ),
        check_vma=False,
    )
```

```python
import functools
import math

import jax
import jax.numpy as jnp
from jax import lax
from jax.experimental import pallas as pl
from jax.experimental.pallas import tpu as pltpu
from jax.sharding import PartitionSpec as P

D = 1024
HEAD_DIM = 64
SEQ = 197
LAYERS = 2
EPS = 1e-06
ROWS = 208
KEYS = 256
MESH = pl.DeviceIdType.MESH
F32 = jnp.float32
BF16 = jnp.bfloat16
CHUNK = 16
HIGHEST = lax.Precision.HIGHEST

V_GAIN, V_BIAS, V_OUT, V_DOWN = 0, 2, 4, 5
V_QV, V_UP = 0, 2
V_ROWS = 8
G_GAIN, G_BIAS, G_OUT, G_DOWN = 0, 4, 8, 10
G_ROWS = 16


def dot(a, b):
    return lax.dot_general(a, b, (((1,), (0,)), ((), ())), preferred_element_type=F32)


def dot_t(a, b):
    return lax.dot_general(a, b, (((1,), (1,)), ((), ())), preferred_element_type=F32)


def t_dot(a, b):
    return lax.dot_general(a, b, (((0,), (0,)), ((), ())), preferred_element_type=F32)


def exact_dot(a, b, dims):
    return lax.dot_general(a, b, (dims, ((), ())), precision=HIGHEST, preferred_element_type=F32)


def when(condition):
    return pl.when(condition)


def scratch_of(half, per_row, width, hidden, images):
    tall = images * ROWS
    dma = pltpu.SemaphoreType.DMA
    vm = pltpu.VMEM
    return dict(
        wq=vm((LAYERS, 3, D, width), BF16),
        wp=vm((LAYERS, D, width), BF16),
        wf=vm((LAYERS, D, 2 * hidden), BF16),
        gq=vm((3, D, width), BF16),
        go=vm((D, width), BF16),
        gf=vm((D, 2 * hidden), BF16),
        pq=vm((LAYERS * half, 3, per_row, width), BF16),
        po=vm((LAYERS * half, per_row, width), BF16),
        pf=vm((half, per_row, 2 * hidden), BF16),
        cq=vm((LAYERS * half, 3, per_row, width), BF16),
        co=vm((LAYERS * half, per_row, width), BF16),
        cf=vm((half, per_row, 2 * hidden), BF16),
        e=vm((2 * LAYERS, tall, D), BF16),
        act=vm((2 * LAYERS, tall, D), BF16),
        q=vm((LAYERS, tall, width), BF16),
        k=vm((LAYERS, images * KEYS, width), BF16),
        v=vm((LAYERS, images * KEYS, width), BF16),
        o=vm((LAYERS, tall, width), BF16),
        prob=vm((LAYERS * images * (width // HEAD_DIM), ROWS, KEYS), F32),
        slope=vm((LAYERS, tall, hidden), F32),
        u=vm((LAYERS, tall, hidden), BF16),
        n=vm((2 * LAYERS, tall, 2 * width), F32),
        spread=vm((2 * LAYERS, tall, 1), F32),
        centre=vm((tall, 1), F32),
        r=vm((tall, 2 * width), F32),
        g=vm((tall, 2 * width), F32),
        f=vm((tall, hidden), BF16),
        d=vm((tall, 3 * width), BF16),
        do=vm((ROWS, width), BF16),
        tmp=vm((ROWS, width), F32),
        stage=vm((2, images, 4, ROWS, width), BF16),
        slot=vm((2, images, 6, ROWS, width), BF16),
        held=vm((images, 2, ROWS, width), F32),
        own=vm((2, images, 2, ROWS, width), F32),
        vs=vm((2, KEYS, 128), F32),
        ts=vm((images, 8, KEYS), F32),
        tr=vm((images, 3, 8, KEYS), F32),
        gb=vm((G_ROWS, width), F32),
        gn=vm((4, G_ROWS, width), F32),
        rq=vm((3, per_row, width), F32),
        ro=vm((width, per_row), F32),
        ru=vm((per_row, hidden), F32),
        rd=vm((hidden, per_row), F32),
        wo=vm((LAYERS, per_row, width), BF16),
        wd=vm((LAYERS, per_row, hidden), BF16),
        sh=vm((LAYERS, 2, 8, width), F32),
        rh=vm((LAYERS, 2 * half, 8, width), F32),
        sv=vm((LAYERS, V_ROWS, width), F32),
        rv=vm((LAYERS, 2 * half, V_ROWS, width), F32),
        a0_s=dma((2, images, 4)),
        a0_r=dma((2, images, 3)),
        ag_s=dma((4, images, 6)),
        ag_r=dma((4, images, 4)),
        rs_s=dma((2, images, 4)),
        rs_r=dma((2, images, 6)),
        t_s=dma((images, 2)),
        t_r=dma((images, 3)),
        gn_s=dma((3,)),
        gn_r=dma((3,)),
        h_s=dma((LAYERS, 2, 2 * half)),
        h_r=dma((LAYERS, 2 * half)),
        fin_s=dma((2, images)),
        fin_r=dma((2, images)),
        w_l=dma((LAYERS, 4)),
        w_s=dma((LAYERS, 4, half)),
        w_r=dma((LAYERS, 4, half)),
        w_f=dma((LAYERS, 4, half)),
        w_g=dma((LAYERS, 4, half)),
        p_s=dma((3, half)),
        p_r=dma((LAYERS, 3, half)),
        c_s=dma((3, half)),
        c_r=dma((LAYERS, 3, half)),
        r_s=dma((LAYERS, 4)),
        v_s=dma((LAYERS, 2 * half)),
        v_r=dma((LAYERS, 2 * half)),
    )


IN_NAMES = (
    "x_in", "cot_in", "ng_in", "nb_in", "bq_in", "bo_in", "bu_in", "bd_in", "wo_in", "wd_in",
    "wq_in", "wu_in",
)
OUT_NAMES = (
    "out", "gin", "gng", "gnb", "gwq", "gbqv", "gwo", "gbo", "gwu", "gbup", "gwd", "gbd",
)


def kernel(wide, images, width, hidden, names, *refs):
    R = dict(zip(names, refs))
    R["x"] = R["e"].at[0:2]
    half = wide // 2
    per_row = D // wide
    heads = width // HEAD_DIM
    w = lax.axis_index("wide")
    z = lax.axis_index("narrow")
    upper = z // 2
    mate = z + 1 - 2 * (z % 2)
    oi = 2 - upper
    oo = 3 * (1 - upper)
    inner_n = (z + upper) % 2
    inner = inner_n == 1
    outer = inner_n == 0
    far = 2 - inner_n
    near_half = 2 * upper
    far_half = 2 - near_half
    inside = z % 2
    half_cols = pl.ds(pl.multiple_of(near_half * width, 128), 2 * width)
    par = w % 2
    mine = w // 2
    partner = w + 1 - 2 * par

    def rows(i):
        return pl.ds(i * ROWS, ROWS)

    def cols(j):
        return pl.ds(pl.multiple_of(j * width, 128), width)

    def block_rows(j):
        return pl.ds(pl.multiple_of(j * width, 128), width)

    def wrows(j):
        return pl.ds(pl.multiple_of(j * per_row, per_row), per_row)

    def remote(src, dst, s, r, wide_id, narrow_id):
        return pltpu.make_async_remote_copy(
            src_ref=src, dst_ref=dst, send_sem=s, recv_sem=r,
            device_id=(wide_id, narrow_id), device_id_type=MESH,
        )

    def chunks(count, body, unroll=False):
        lax.fori_loop(
            0, count // CHUNK, lambda c, _: (body(c * CHUNK), 0)[1], 0, unroll=unroll
        )

    def at(i, start, size=CHUNK):
        return pl.ds(pl.multiple_of(i * ROWS + start, CHUNK), size)

    def a0_copy(buf, kind, i, block, s, r, to):
        part = buf.at[rows(i), cols(block)]
        return remote(part, part, R["a0_s"].at[kind, i, s], R["a0_r"].at[kind, i, r], w, to)

    def a0_start(buf, kind, i):
        a0_copy(buf, kind, i, z, 1, far, oi).start()
        a0_copy(buf, kind, i, z, 0, 0, mate).start()

    def a0_relay(buf, kind, i):
        @when(inner)
        def _():
            for r, block in ((1, oi), (2, oo)):
                a0_copy(buf, kind, i, block, r + 1, r, mate).wait_recv()
                a0_copy(buf, kind, i, block, r + 1, r, mate).start()

    def a0_finish(buf, kind, i):
        a0_copy(buf, kind, i, mate, 0, 0, mate).wait_recv()

        @when(outer)
        def _():
            for r, block in ((1, oi), (2, oo)):
                a0_copy(buf, kind, i, block, r + 1, r, mate).wait_recv()

        a0_copy(buf, kind, i, z, 0, 0, mate).wait_send()
        a0_copy(buf, kind, i, z, 1, far, oi).wait_send()

        @when(inner)
        def _():
            for r, block in ((1, oi), (2, oo)):
                a0_copy(buf, kind, i, block, r + 1, r, mate).wait_send()

    def ag_copy(buf, kind, i, block, s, r, to):
        part = buf.at[rows(i), cols(block)]
        return remote(part, part, R["ag_s"].at[kind, i, s], R["ag_r"].at[kind, i, r], w, to)

    def ag_unit(buf, kind, i, u):
        ag_copy(buf, kind, i, near_half + u, u, u, oi).start()
        ag_copy(buf, kind, i, near_half + u, 2 + u, 2 + u, mate).start()

    def ag_relay(buf, kind, i):
        @when(inner)
        def _():
            for u in range(2):
                ag_copy(buf, kind, i, far_half + u, 4 + u, u, mate).wait_recv()
                ag_copy(buf, kind, i, far_half + u, 4 + u, u, mate).start()

    def ag_finish(buf, kind, i):
        @when(outer)
        def _():
            for u in range(2):
                ag_copy(buf, kind, i, near_half + u, 2 + u, 2 + u, mate).wait_recv()
            for u in range(2):
                ag_copy(buf, kind, i, far_half + u, 4 + u, u, mate).wait_recv()

    def ag_drain(buf, kind, i):
        @when(inner)
        def _():
            for u in range(2):
                ag_copy(buf, kind, i, near_half + u, u, u, oi).wait_send()
                ag_copy(buf, kind, i, near_half + u, 2 + u, 2 + u, mate).wait_send()
                ag_copy(buf, kind, i, far_half + u, 4 + u, u, mate).wait_send()

    def rs_copy(bank, i, q, slot, to):
        return remote(
            R["stage"].at[bank, i, q], R["slot"].at[bank, i, slot],
            R["rs_s"].at[bank, i, q], R["rs_r"].at[bank, i, slot], w, to,
        )

    def rs_blocks(bank, i, block):
        for q in range(4):
            y = block((far_half if q < 2 else near_half) + q % 2)

            @when(outer)
            def _():
                R["stage"][bank, i, q] = y.astype(BF16)
                rs_copy(bank, i, q, q, mate).start()

            @when(inner)
            def _():
                if q < 2:
                    R["held"][i, q] = y
                else:
                    R["own"][bank, i, q - 2] = y

    def rs_relay(bank, i):
        @when(inner)
        def _():
            for q in range(2):
                rs_copy(bank, i, q, q, mate).wait_recv()

                def body(c):
                    part = pl.ds(pl.multiple_of(c, CHUNK), CHUNK)
                    total = R["held"][i, q, part] + R["slot"][bank, i, q, part].astype(F32)
                    R["stage"][bank, i, q, part] = total.astype(BF16)

                chunks(ROWS, body, True)
                rs_copy(bank, i, q, 4 + q, oi).start()

    def rs_unit(bank, i, u):
        rs_copy(bank, i, 2 + u, 2 + u, mate).wait_recv()
        rs_copy(bank, i, u, 4 + u, oi).wait_recv()

    def rs_drain(bank, i):
        @when(inner)
        def _():
            for q in range(2):
                rs_copy(bank, i, q, 4 + q, oi).wait_send()

        @when(outer)
        def _():
            for q in range(4):
                rs_copy(bank, i, q, q, mate).wait_send()

    def rs_sum(bank, i, u, part):
        slots = R["slot"]
        return (
            R["own"][bank, i, u, part]
            + slots[bank, i, 2 + u, part].astype(F32)
            + slots[bank, i, 4 + u, part].astype(F32)
        )

    def t_copy(i, q, r, to):
        return remote(
            R["ts"].at[i], R["tr"].at[i, r], R["t_s"].at[i, q], R["t_r"].at[i, r], w, to
        )

    def t_send(i):
        lane = lax.broadcasted_iota(jnp.int32, (8, 128), 0)
        first = jnp.where(lane < 4, 1.0, 0.0).astype(F32)
        second = 1.0 - first
        R["ts"][i] = exact_dot(first, R["vs"][0], ((1,), (1,))) + exact_dot(
            second, R["vs"][1], ((1,), (1,))
        )
        @when(outer)
        def _():
            t_copy(i, 0, 0, mate).start()

        t_copy(i, 1, far, oi).start()

    def t_total(i):
        for q in range(3):
            t_copy(i, 0, q, mate).wait_recv()
        total = (R["ts"][i] + R["tr"][i, 0]) + (R["tr"][i, 1] + R["tr"][i, 2])
        row = lax.broadcasted_iota(jnp.int32, (8, 128), 0)
        lane = lax.broadcasted_iota(jnp.int32, (8, 128), 1)
        pick = ((row == 0) & (lane < 64)) | ((row == 4) & (lane >= 64))
        R["vs"][0] = exact_dot(total, jnp.where(pick, 1.0, 0.0).astype(F32), ((0,), (0,)))

    def t_drain(i):
        @when(outer)
        def _():
            t_copy(i, 0, 0, mate).wait_send()

        t_copy(i, 1, far, oi).wait_send()

    def weights(l, piece):
        if piece == 0:
            return R["wq"].at[l], R["wq_in"].at[l]
        if piece == 1:
            return R["wp"].at[l], R["wo"].at[l]
        if piece == 2:
            return R["wf"].at[l, :, 0:hidden], R["wu_in"].at[l]
        return R["wf"].at[l, :, hidden : 2 * hidden], R["wd"].at[l]

    def rows_of(ref, k):
        return ref.at[wrows(k)] if len(ref.shape) == 2 else ref.at[:, wrows(k)]

    def w_local(l, piece):
        full, shard = weights(l, piece)
        return pltpu.make_async_copy(shard, rows_of(full, w), R["w_l"].at[l, piece])

    def w_send(l, piece, s, to):
        full, shard = weights(l, piece)
        return remote(
            shard, rows_of(full, w), R["w_s"].at[l, piece, s], R["w_r"].at[l, piece, mine], to, z
        )

    def w_pair(l, piece):
        full, shard = weights(l, piece)
        return remote(
            shard, rows_of(full, w),
            R["w_s"].at[l, piece, half - 1], R["w_f"].at[l, piece, mine], partner, z,
        )

    def w_cross(l, piece, k, parity):
        full, _ = weights(l, piece)
        part = rows_of(full, 2 * k + parity)
        return remote(
            part, part, R["w_g"].at[l, piece, k], R["w_f"].at[l, piece, k], partner, z
        )

    def w_start(l, piece):
        for j in range(1, half):
            w_send(l, piece, j - 1, 2 * ((mine + j) % half) + par).start()
        w_pair(l, piece).start()
        w_local(l, piece).start()

    def w_relay(l, piece):
        full, shard = weights(l, piece)
        for j in range(1, half):
            k = (mine + half - j) % half
            remote(
                shard, rows_of(full, 2 * k + par),
                R["w_s"].at[l, piece, 0], R["w_r"].at[l, piece, k], partner, z,
            ).wait_recv()
            w_cross(l, piece, k, par).start()

    def w_finish(l, piece):
        for j in range(half):
            w_cross(l, piece, (mine + half - j) % half, 1 - par).wait_recv()
        w_local(l, piece).wait()
        for s in range(half - 1):
            w_send(l, piece, s, partner).wait_send()
        w_pair(l, piece).wait_send()
        for j in range(1, half):
            w_cross(l, piece, (mine + j) % half, par).wait_send()

    def grads(l, piece):
        if piece == 1:
            return R["gf"], R["pf"], R["cf"]
        room = pl.ds(l * half, half)
        if piece == 0:
            return R["gq"], R["pq"].at[room], R["cq"].at[room]
        return R["go"], R["po"].at[room], R["co"].at[room]

    def p_copy(l, piece, k):
        full, theirs, _ = grads(l, piece)
        return remote(
            rows_of(full, 2 * k + 1 - par), theirs.at[k],
            R["p_s"].at[piece, k], R["p_r"].at[l, piece, k], partner, z,
        )

    def c_copy(l, piece, k, source):
        full, _, came = grads(l, piece)
        return remote(
            rows_of(full, 2 * k + par), came.at[source],
            R["c_s"].at[piece, k], R["c_r"].at[l, piece, source], 2 * k + par, z,
        )

    def r_copies(l, piece):
        pairs = (
            ((R["rq"], R["gwq"]),),
            ((R["ru"], R["gwu"]), (R["rd"], R["gwd"])),
            ((R["ro"], R["gwo"]),),
        )[piece]
        return [
            pltpu.make_async_copy(total, result.at[l], R["r_s"].at[l, piece + 2 * q])
            for q, (total, result) in enumerate(pairs)
        ]

    def g_start(l, piece, b):
        pairs = half * 256 // D
        for k in range(pairs):
            p_copy(l, piece, b * pairs + k).start()

    def g_mid(l, piece):
        full, theirs, _ = grads(l, piece)
        for j in range(1, half + 1):
            k = (mine + j) % half
            p_copy(l, piece, k).wait_recv()

            def body(c):
                here = pl.ds(pl.multiple_of((2 * k + par) * per_row + c, CHUNK), CHUNK)
                part = pl.ds(pl.multiple_of(c, CHUNK), CHUNK)
                ours = full.at[:, here] if piece == 0 else full.at[here]
                other = theirs.at[k, :, part] if piece == 0 else theirs.at[k, part]
                ours[...] = (ours[...].astype(F32) + other[...].astype(F32)).astype(BF16)

            chunks(per_row, body)
            if j < half:
                c_copy(l, piece, k, mine).start()

    def g_end(l, piece):
        full, _, came = grads(l, piece)
        for j in range(1, half):
            k = (mine + half - j) % half
            c_copy(l, piece, k, k).wait_recv()

        @when(l < LAYERS - 1)
        def _():
            for copy in r_copies(l + 1, piece):
                copy.wait()

        others = [(mine + j) % half for j in range(1, half)]
        if piece != 2:
            def body(c):
                part = pl.ds(pl.multiple_of(c, CHUNK), CHUNK)
                here = pl.ds(pl.multiple_of(w * per_row + c, CHUNK), CHUNK)
                if piece == 0:
                    total = full[:, here].astype(F32)
                    for k in others:
                        total = total + came[k, :, part].astype(F32)
                    R["rq"][:, part] = total
                else:
                    total = full[here, 0:hidden].astype(F32)
                    for k in others:
                        total = total + came[k, part, 0:hidden].astype(F32)
                    R["ru"][part] = total

            chunks(per_row, body)
        if piece != 0:
            first = hidden if piece == 1 else 0
            result = R["rd"] if piece == 1 else R["ro"]
            for c in range(0, result.shape[0], 256):
                lanes = slice(first + c, first + c + 256)
                total = full[wrows(w), lanes].astype(F32)
                for k in others:
                    total = total + came[k, :, lanes].astype(F32)
                result[c : c + 256] = total.T
        for copy in r_copies(l, piece):
            copy.start()
        for k in range(half):
            p_copy(l, piece, k).wait_send()
        for j in range(1, half):
            c_copy(l, piece, (mine + j) % half, mine).wait_send()

    def v_copy(l, j, source):
        to = (w + j) % wide
        return remote(
            R["sv"].at[l], R["rv"].at[l, source],
            R["v_s"].at[l, j], R["v_r"].at[l, source], to, z,
        )

    def h_copy(l, j, source, to_mate):
        to = (w + j) % wide
        block, narrow = (1 - inside, mate) if to_mate else (inside, z)
        return remote(
            R["sh"].at[l, block], R["rh"].at[l, source],
            R["h_s"].at[l, 1 if to_mate else 0, j], R["h_r"].at[l, source], to, narrow,
        )

    def v_start(l):
        for j in range(1, wide):
            v_copy(l, j, w).start()

    def h_start(l):
        @when(inner)
        def _():
            for j in range(wide):
                if j > 0:
                    h_copy(l, j, w, False).start()
                h_copy(l, j, w, True).start()
            R["rh"][l, w] = R["sh"][l, inside]

    def v_end(l):
        total = R["sv"][l]
        for j in range(1, wide):
            source = (w + j) % wide
            v_copy(l, j, source).wait_recv()
            total = total + R["rv"][l, source]
        R["gbqv"][l] = total[0:2]
        for b in range(hidden // width):
            R["gbup"][pl.ds(l, 1), b * width : (b + 1) * width] = total[2 + b : 3 + b]
        for j in range(1, wide):
            v_copy(l, j, w).wait_send()

    def h_end(l):
        @when(outer)
        def _():
            h_copy(l, 0, w, True).wait_recv()

        total = R["rh"][l, w]
        for j in range(1, wide):
            source = (w + j) % wide
            h_copy(l, j, source, True).wait_recv()
            total = total + R["rh"][l, source]
        R["gng"][l] = total[V_GAIN : V_GAIN + 2]
        R["gnb"][l] = total[V_BIAS : V_BIAS + 2]
        R["gbo"][pl.ds(l, 1)] = total[V_OUT : V_OUT + 1]
        R["gbd"][pl.ds(l, 1)] = total[V_DOWN : V_DOWN + 1]

        @when(inner)
        def _():
            for j in range(wide):
                if j > 0:
                    h_copy(l, j, w, False).wait_send()
                h_copy(l, j, w, True).wait_send()

    def norm_in(buf, l, branch, i):
        at_norm = 2 * l + branch
        scale = [R["gn"][j, pl.ds(G_GAIN + at_norm, 1)] for j in range(4)]
        shift = [R["gn"][j, pl.ds(G_BIAS + at_norm, 1)] for j in range(4)]
        scale = jnp.concatenate(scale, axis=1)
        shift = jnp.concatenate(shift, axis=1)

        def body(c):
            here = at(i, c)
            raw = buf[here, :].astype(F32)
            mean = jnp.sum(raw, axis=1, keepdims=True) * (1.0 / D)
            square = jnp.sum(raw * raw, axis=1, keepdims=True) * (1.0 / D)
            s = lax.rsqrt(square - mean * mean + EPS)
            R["act"][at_norm, here] = ((raw - mean) * s * scale + shift).astype(BF16)
            R["centre"][here] = R["centre"][here] + mean
            R["spread"][at_norm, here] = s

        chunks(ROWS, body, True)

    def norm_keep(l, branch, i):
        at_norm = 2 * l + branch

        @when(inner)
        def _():
            def body(c):
                here = at(i, c)
                R["n"][at_norm, here] = (R["r"][here] - R["centre"][here]) * R["spread"][
                    at_norm, here
                ]

            chunks(ROWS, body, True)

    def norm_back(bank, l, branch, i, buf, kind):
        at_norm = 2 * l + branch

        @when(inner)
        def _():
            t_total(i)
            for u in range(2):
                lanes = slice(u * width, (u + 1) * width)
                scale = R["gn"][near_half + u, pl.ds(G_GAIN + at_norm, 1)]
                rs_unit(bank, i, u)

                def body(c):
                    here = at(i, c)
                    part = pl.ds(pl.multiple_of(c, CHUNK), CHUNK)
                    upstream = rs_sum(bank, i, u, part)
                    R["own"][bank, i, u, part] = upstream
                    first = R["vs"][0, part, 0:1] * (1.0 / D)
                    second = R["vs"][0, part, 64:65] * (1.0 / D)
                    normed = R["n"][at_norm, here, lanes]
                    grown = R["g"][here, lanes] + (
                        upstream * scale - first - normed * second
                    ) * R["spread"][at_norm, here]
                    R["g"][here, lanes] = grown
                    if buf is not None:
                        buf[here, cols(near_half + u)] = grown.astype(BF16)

                chunks(ROWS, body, True)
                if buf is not None:
                    ag_unit(buf, kind, i, u)

    def norm_sums(bank, l, branch, i, out_row):
        rs_drain(bank, i)
        t_drain(i)

        @when(inner)
        def _():
            for u in range(2):
                lanes = slice(u * width, (u + 1) * width)

                def body(c, carry):
                    c = c * CHUNK
                    here = at(i, c)
                    upstream = R["own"][bank, i, u, pl.ds(pl.multiple_of(c, CHUNK), CHUNK)]
                    normed = R["n"][2 * l + branch, here, lanes]
                    values = (upstream * normed, upstream, R["g"][here, lanes])
                    return tuple(
                        total + jnp.sum(value, axis=0, keepdims=True)
                        for total, value in zip(carry, values)
                    )

                zero = jnp.zeros((1, width), F32)
                sums = lax.fori_loop(0, ROWS // CHUNK, body, (zero,) * 3, unroll=True)
                small_add(l, u, V_GAIN + branch, sums[0])
                small_add(l, u, V_BIAS + branch, sums[1])
                if out_row is not None:
                    small_add(l, u, out_row, sums[2])

    def small_add(l, u, row, value):
        there = slice(row, row + 1)
        R["sh"][l, u, there] = R["sh"][l, u, there] + value

    def send_sums(at_norm, i, block_of):
        R["vs"][0, 0:ROWS] = jnp.zeros((ROWS, 128), F32)
        R["vs"][1, 0:ROWS] = jnp.zeros((ROWS, 128), F32)
        l, branch = at_norm

        def block(j):
            y = block_of(j)
            R["tmp"][...] = y
            scale = R["gn"][j, pl.ds(G_GAIN + 2 * l + branch, 1)]
            shift = R["gn"][j, pl.ds(G_BIAS + 2 * l + branch, 1)]

            def body(c):
                part = pl.ds(pl.multiple_of(c, CHUNK), CHUNK)
                value = R["tmp"][part]
                normed = R["act"][2 * l + branch, at(i, c), cols(j)].astype(F32) - shift
                first = value * scale
                second = value * normed
                for m in range(width // 128):
                    lanes = slice(m * 128, (m + 1) * 128)
                    R["vs"][0, part] = R["vs"][0, part] + first[:, lanes]
                    R["vs"][1, part] = R["vs"][1, part] + second[:, lanes]

            chunks(ROWS, body, True)
            return R["tmp"][...]

        return block

    factor = 1.0 / math.sqrt(HEAD_DIM)
    head_lanes = [slice(h * HEAD_DIM, (h + 1) * HEAD_DIM) for h in range(heads)]

    def attention(l, i):
        keys = pl.ds(i * KEYS, KEYS)
        column = lax.broadcasted_iota(jnp.int32, (ROWS, KEYS), 1)
        scores = [
            dot_t(R["q"][l, rows(i), lanes], R["k"][l, keys, lanes]) for lanes in head_lanes
        ]
        probs = []
        for h in range(heads):
            masked = jnp.where(column < SEQ, scores[h], -jnp.inf)
            top = jnp.max(masked, axis=1, keepdims=True)
            grown = jnp.exp(masked - top)
            prob = grown * (1.0 / jnp.sum(grown, axis=1, keepdims=True))
            R["prob"][(l * images + i) * heads + h] = prob
            probs.append(prob.astype(BF16))
        mixed = [dot(probs[h], R["v"][l, keys, head_lanes[h]]) for h in range(heads)]
        R["o"][l, rows(i)] = jnp.concatenate(mixed, axis=1).astype(BF16)

    def f1(l, i):
        buf = R["x"].at[0]

        @when(l > 0)
        def _():
            ag_finish(buf, 0, i)

        norm_in(buf, l, 0, i)
        act = R["act"].at[2 * l, rows(i)]
        kept = pl.ds(i * KEYS, ROWS)
        bq = R["bq_in"][l, 0:1]
        bv = R["bq_in"][l, 1:2]
        queries = (dot(act[...], R["wq"][l, 0]) + bq).astype(BF16).astype(F32) * factor
        R["q"][l, rows(i)] = queries.astype(BF16)
        R["k"][l, kept] = dot(act[...], R["wq"][l, 1]).astype(BF16)
        R["v"][l, kept] = (dot(act[...], R["wq"][l, 2]) + bv).astype(BF16)
        if i == 0:
            @when(l == 0)
            def _():
                w_relay(l, 1)

        attention(l, i)
        if i == 0:
            w_finish(l, 1)

        def block(j):
            return dot_t(R["o"][l, rows(i)], R["wp"][l, block_rows(j)])

        rs_blocks(0, i, block)
        norm_keep(l, 0, i)

    def f2(l, i):
        buf = R["x"].at[1]
        ag_finish(buf, 1, i)
        norm_in(buf, l, 1, i)

        def body(b, _):
            lanes = cols(b)
            pre = dot(R["act"][2 * l + 1, rows(i)], R["wf"][l, :, lanes])
            pre = pre + R["bu_in"][pl.ds(l, 1), lanes]
            cdf = 0.5 * (1.0 + lax.erf(pre * 0.7071067811865476))
            R["u"][l, rows(i), lanes] = (pre * cdf).astype(BF16)
            R["slope"][l, rows(i), lanes] = (
                cdf + pre * jnp.exp(-0.5 * pre * pre) * 0.3989422804014327
            )
            return 0

        lax.fori_loop(0, hidden // width, body, 0, unroll=True)
        if i == 0:
            w_finish(l, 3)

        def block(j):
            return dot_t(R["u"][l, rows(i)], R["wf"][l, block_rows(j), hidden : 2 * hidden])

        rs_blocks(1, i, block)
        norm_keep(l, 1, i)

    def residual(bank, i, bias_row, kind):
        @when(inner)
        def _():
            for u in range(2):
                lanes = slice(u * width, (u + 1) * width)
                bias = R["gn"][near_half + u, bias_row]
                rs_unit(bank, i, u)

                def body(c):
                    here = at(i, c)
                    part = pl.ds(pl.multiple_of(c, CHUNK), CHUNK)
                    grown = R["r"][here, lanes] + (rs_sum(bank, i, u, part) + bias)
                    R["r"][here, lanes] = grown
                    if kind is not None:
                        out = (grown - R["centre"][here]).astype(BF16)
                        R["x"][kind, here, cols(near_half + u)] = out

                chunks(ROWS, body, True)
                if kind is not None:
                    ag_unit(R["x"].at[kind], kind, i, u)

        rs_drain(bank, i)

    def fin_copy(which, i):
        source = (R["r"], R["g"])[which]
        there = pl.ds(pl.multiple_of((1 - inside) * width, 128), width)
        return remote(
            source.at[rows(i), there], R["held"].at[i, which],
            R["fin_s"].at[which, i], R["fin_r"].at[which, i], w, mate,
        )

    def fin_start(which, i):
        @when(inner)
        def _():
            fin_copy(which, i).start()

    def fin_end(which, i):
        source, result = ((R["r"], R["out"]), (R["g"], R["gin"]))[which]
        there = pl.ds(i * SEQ, SEQ)

        @when(inner)
        def _():
            here = pl.ds(pl.multiple_of(inside * width, 128), width)
            result[there] = source[pl.ds(i * ROWS, SEQ), here]
            fin_copy(which, i).wait_send()

        @when(outer)
        def _():
            fin_copy(which, i).wait_recv()
            result[there] = R["held"][i, which, 0:SEQ]

    def post_f1(l, i):
        @when(l > 0)
        def _():
            ag_drain(R["x"].at[0], 0, i)

        residual(0, i, pl.ds(G_OUT + l, 1), 1)

    def post_f2(l, i, last):
        ag_drain(R["x"].at[1], 1, i)
        residual(1, i, pl.ds(G_DOWN + l, 1), None if last else 0)
        if last:
            fin_start(0, i)

    def b2(l, i):
        e = R["e"].at[2 * l + 1]

        @when(l < LAYERS - 1)
        def _():
            ag_finish(e, 2, i)

        def body(b, _):
            lanes = cols(b)
            back = pl.ds(pl.multiple_of(hidden + b * width, 128), width)
            dz = dot(e[rows(i), :], R["wf"][l, :, back]) * R["slope"][l, rows(i), lanes]
            R["f"][rows(i), lanes] = dz.astype(BF16)
            row = pl.ds(V_UP + b, 1)
            R["sv"][l, row] = R["sv"][l, row] + jnp.sum(dz, axis=0, keepdims=True)
            return 0

        lax.fori_loop(0, hidden // width, body, 0, unroll=True)

        def block(j):
            return dot_t(R["f"][rows(i)], R["wf"][l, block_rows(j), 0:hidden])

        rs_blocks(0, i, send_sums((l, 1), i, block))
        t_send(i)
        add_down(l, i)

    def b1(l, i):
        e = R["e"].at[2 * l]
        ag_finish(e, 3, i)
        keys = pl.ds(i * KEYS, KEYS)
        R["do"][...] = dot(e[rows(i), :], R["wp"][l]).astype(BF16)
        if i == images - 1:
            grad_out(l)
        dos = [R["do"][:, lanes] for lanes in head_lanes]
        dps = [dot_t(dos[h], R["v"][l, keys, head_lanes[h]]) for h in range(heads)]
        dvs, dss = [], []
        for h in range(heads):
            prob = R["prob"][(l * images + i) * heads + h]
            dvs.append(t_dot(prob.astype(BF16), dos[h])[0:ROWS])
            delta = jnp.sum(prob * dps[h], axis=1, keepdims=True)
            dss.append((prob * (dps[h] - delta)).astype(BF16))
        dqs = [dot(dss[h], R["k"][l, keys, head_lanes[h]]) * factor for h in range(heads)]
        dks = [t_dot(dss[h], R["q"][l, rows(i), head_lanes[h]])[0:ROWS] for h in range(heads)]
        dq, dk, dv = [jnp.concatenate(parts, axis=1) for parts in (dqs, dks, dvs)]
        for part, value in ((0, dq), (1, dk), (2, dv)):
            R["d"][rows(i), part * width : (part + 1) * width] = value.astype(BF16)
        for row, value in ((V_QV, dq), (V_QV + 1, dv)):
            there = slice(row, row + 1)
            R["sv"][l, there] = R["sv"][l, there] + jnp.sum(value, axis=0, keepdims=True)

        def block(j):
            parts = [
                dot_t(R["d"][rows(i), m * width : (m + 1) * width], R["wq"][l, m, block_rows(j)])
                for m in range(3)
            ]
            return parts[0] + parts[1] + parts[2]

        rs_blocks(1, i, send_sums((l, 0), i, block))
        t_send(i)

    def add_down(l, i):
        @when(inner)
        def _():
            for u in range(2):
                lanes = slice(u * width, (u + 1) * width)

                def body(c, total):
                    value = R["g"][at(i, c * CHUNK), lanes]
                    return total + jnp.sum(value, axis=0, keepdims=True)

                zero = jnp.zeros((1, width), F32)
                total = lax.fori_loop(0, ROWS // CHUNK, body, zero, unroll=True)
                small_add(l, u, V_DOWN, total)

    def post_b2(l, i):
        @when(l < LAYERS - 1)
        def _():
            ag_drain(R["e"].at[2 * l + 1], 2, i)

        norm_back(0, l, 1, i, R["e"].at[2 * l], 3)
        norm_sums(0, l, 1, i, V_OUT)

    def post_b1(l, i):
        ag_drain(R["e"].at[2 * l], 3, i)

        @when(l > 0)
        def _():
            norm_back(1, l, 0, i, R["e"].at[2 * l - 1], 2)

        @when(l == 0)
        def _():
            norm_back(1, l, 0, i, None, None)
            fin_start(1, i)

        norm_sums(1, l, 0, i, None)

    def grad_block(b):
        block = (mine * 2 * per_row // 256 + 1 + b) % (D // 256)
        return block, pl.ds(pl.multiple_of(block * 256, 256), 256)

    def grad_ffn(l, first, last):
        def body(b, _):
            block, lanes = grad_block(b)
            up = t_dot(R["act"][2 * l + 1, :, lanes], R["f"][...])
            R["gf"][lanes, 0:hidden] = up.astype(BF16)
            down = t_dot(R["e"][2 * l + 1, :, lanes], R["u"][l])
            R["gf"][lanes, hidden : 2 * hidden] = down.astype(BF16)
            g_start(l, 1, block)
            return 0

        lax.fori_loop(first, last, body, 0)

    def grad_qkv(l):
        def body(b, _):
            block, lanes = grad_block(b)
            qkv = t_dot(R["act"][2 * l, :, lanes], R["d"][...])
            for m in range(3):
                R["gq"][m, lanes] = qkv[:, m * width : (m + 1) * width].astype(BF16)
            g_start(l, 0, block)
            return 0

        lax.fori_loop(0, D // 256, body, 0)

    def grad_out(l):
        def body(b, _):
            block, lanes = grad_block(b)
            out = t_dot(R["e"][2 * l, :, lanes], R["o"][l])
            R["go"][lanes] = out.astype(BF16)
            g_start(l, 2, block)
            return 0

        lax.fori_loop(0, D // 256, body, 0)

    def spread_rows(source, result):
        tokens = images * SEQ
        wide_rows = R["r"].at[:, 0:width]
        wide_rows[0:tokens] = source[...].astype(F32)
        row = lax.broadcasted_iota(jnp.int32, (ROWS, width), 0)
        for i in image:
            part = wide_rows[i * SEQ : i * SEQ + ROWS]
            result[rows(i), cols(z)] = jnp.where(row < SEQ, part, 0.0).astype(BF16)

    barrier = pltpu.get_barrier_semaphore()
    for j in range(1, wide):
        pl.semaphore_signal(barrier, 1, device_id=((w + j) % wide, z), device_id_type=MESH)
    for j in range(1, 4):
        pl.semaphore_signal(barrier, 1, device_id=(w, (z + j) % 4), device_id_type=MESH)
    image = range(images)
    first_x = R["x"].at[0]
    last_e = R["e"].at[2 * LAYERS - 1]
    R["r"][...] = jnp.zeros_like(R["r"])
    spread_rows(R["x_in"], first_x)
    for l in range(LAYERS):
        R["gb"][G_GAIN + 2 * l : G_GAIN + 2 * l + 2] = R["ng_in"][l]
        R["gb"][G_BIAS + 2 * l : G_BIAS + 2 * l + 2] = R["nb_in"][l]
    R["gb"][G_OUT : G_OUT + LAYERS] = R["bo_in"][...]
    R["gb"][G_DOWN : G_DOWN + LAYERS] = R["bd_in"][...]
    R["gn"][z] = R["gb"][...]
    for l in range(LAYERS):
        R["wo"][l] = R["wo_in"][l].T
    pl.semaphore_wait(barrier, 3 + wide - 1)

    w_start(0, 0)
    for i in image:
        a0_start(first_x, 0, i)

    def gn_copy(q, r, to):
        return remote(R["gb"], R["gn"].at[z], R["gn_s"].at[q], R["gn_r"].at[r], w, to)

    gn_copy(0, 0, mate).start()
    gn_copy(1, far, oi).start()
    gn_copy(2, far, oo).start()
    w_start(0, 1)
    for l in range(LAYERS):
        R["wd"][l] = R["wd_in"][l].T
    spread_rows(R["cot_in"], last_e)
    R["centre"][...] = jnp.zeros_like(R["centre"])
    R["sv"][...] = jnp.zeros_like(R["sv"])
    R["sh"][...] = jnp.zeros_like(R["sh"])
    R["vs"][...] = jnp.zeros_like(R["vs"])
    for name in ("k", "v"):
        for i in image:
            empty = jnp.zeros((LAYERS, KEYS - ROWS, width), BF16)
            R[name][:, i * KEYS + ROWS : (i + 1) * KEYS] = empty
    for i in image:
        a0_relay(first_x, 0, i)
    for i in image:
        a0_start(last_e, 1, i)
    w_start(0, 2)
    w_start(0, 3)
    for l in range(1, LAYERS):
        for piece in range(4):
            w_start(l, piece)
    for q in range(3):
        gn_copy(q, q, mate).wait_recv()
    for q in range(3):
        gn_copy(q, q, mate).wait_send()
    w_relay(0, 0)

    def arrived(i):
        a0_finish(first_x, 0, i)

        @when(inner)
        def _():
            R["r"][rows(i)] = first_x[rows(i), half_cols].astype(F32)

    arrived(0)
    w_finish(0, 0)
    for i in image:
        a0_relay(last_e, 1, i)

    def forward(l, _):
        f1(l, 0)

        @when(l > 0)
        def _():
            ag_relay(R["x"].at[0], 0, 1)

        rs_relay(0, 0)

        @when(l == 0)
        def _():
            for i in range(1, images):
                arrived(i)

        f1(l, 1)
        post_f1(l, 0)
        w_relay(l, 2)
        rs_relay(0, 1)
        ag_relay(R["x"].at[1], 1, 0)
        w_relay(l, 3)
        post_f1(l, 1)
        w_finish(l, 2)
        f2(l, 0)
        ag_relay(R["x"].at[1], 1, 1)
        rs_relay(1, 0)
        f2(l, 1)

        @when(l < LAYERS - 1)
        def _():
            w_relay(l + 1, 0)
            post_f2(l, 0, False)
            rs_relay(1, 1)
            ag_relay(R["x"].at[0], 0, 0)
            w_relay(l + 1, 1)
            post_f2(l, 1, False)
            w_finish(l + 1, 0)

        return 0

    lax.fori_loop(0, LAYERS, forward, 0)
    for i in image:
        a0_finish(last_e, 1, i)

    @when(inner)
    def _():
        R["g"][...] = last_e[:, half_cols].astype(F32)

    def backward(step, _):
        l = LAYERS - 1 - step
        top = l == LAYERS - 1
        e2 = R["e"].at[2 * l + 1]
        e1 = R["e"].at[2 * l]
        b2(l, 0)

        @when(top)
        def _():
            rs_relay(1, 1)

        @when(l < LAYERS - 1)
        def _():
            ag_relay(e2, 2, 1)

        rs_relay(0, 0)
        b2(l, 1)

        @when(top)
        def _():
            post_f2(l, 0, True)
            post_f2(l, 1, True)

        grad_ffn(l, 0, 2)
        post_b2(l, 0)
        grad_ffn(l, 2, 4)
        rs_relay(0, 1)

        @when(l < LAYERS - 1)
        def _():
            g_end(l + 1, 0)
            g_end(l + 1, 2)
            v_end(l + 1)
            h_end(l + 1)

        g_mid(l, 1)
        ag_relay(e1, 3, 0)
        post_b2(l, 1)
        b1(l, 0)
        ag_relay(e1, 3, 1)
        rs_relay(1, 0)

        b1(l, 1)
        post_b1(l, 0)
        grad_qkv(l)
        g_mid(l, 2)
        g_mid(l, 0)
        rs_relay(1, 1)

        @when(l > 0)
        def _():
            ag_relay(R["e"].at[2 * l - 1], 2, 0)

        g_end(l, 1)
        v_start(l)
        post_b1(l, 1)
        h_start(l)
        return 0

    lax.fori_loop(0, LAYERS, backward, 0)
    first = jnp.int32(0)
    g_end(first, 2)
    v_end(0)
    for i in image:
        fin_end(0, i)
    g_end(first, 0)
    for i in image:
        fin_end(1, i)
    h_end(0)
    for piece in range(3):
        for copy in r_copies(0, piece):
            copy.wait()


def deliver(*refs):
    count = (len(refs) - 2) // 3
    sources, results, rooms = (refs[i * count : (i + 1) * count] for i in range(3))
    came, gone = refs[3 * count :]

    def copy(i, inward):
        if inward:
            return pltpu.make_async_copy(sources[i], rooms[i], came.at[i])
        return pltpu.make_async_copy(rooms[i], results[i], gone.at[i])

    for i in range(count):
        copy(i, True).start()
    for i in range(count):
        copy(i, True).wait()
        copy(i, False).start()
    for i in range(count):
        copy(i, False).wait()


def body(wide, inputs, norm_gain, norm_bias, w_qkv, b_qv, w_out, b_out, w_up, b_up, w_down, b_down, cotangent):
    tokens, width = inputs.shape
    images = tokens // SEQ
    hidden = w_up.shape[2]
    per_row = w_up.shape[1]
    half = wide // 2
    scratch = scratch_of(half, per_row, width, hidden, images)
    names = IN_NAMES + OUT_NAMES + tuple(scratch)
    vmem = pl.BlockSpec(memory_space=pltpu.VMEM)
    anywhere = pl.BlockSpec(memory_space=pl.ANY)

    def shaped(*shape):
        return jax.ShapeDtypeStruct(shape, F32)

    results = pl.pallas_call(
        functools.partial(kernel, wide, images, width, hidden, names),
        out_shape=(
            shaped(tokens, width),
            shaped(tokens, width),
            shaped(LAYERS, 2, width),
            shaped(LAYERS, 2, width),
            shaped(LAYERS, 3, per_row, width),
            shaped(LAYERS, 2, width),
            shaped(LAYERS, width, per_row),
            shaped(LAYERS, width),
            shaped(LAYERS, per_row, hidden),
            shaped(LAYERS, hidden),
            shaped(LAYERS, hidden, per_row),
            shaped(LAYERS, width),
        ),
        in_specs=[vmem] * 10 + [anywhere] * 2,
        out_specs=(
            vmem, vmem, vmem, vmem, anywhere, vmem, anywhere, vmem, anywhere, vmem, anywhere, vmem,
        ),
        scratch_shapes=list(scratch.values()),
        compiler_params=pltpu.CompilerParams(
            collective_id=0, has_side_effects=True, vmem_limit_bytes=67043328
        ),
        name="encoder_step",
    )(
        inputs, cotangent, norm_gain, norm_bias, b_qv, b_out, b_up, b_down, w_out, w_down,
        w_qkv.transpose(0, 2, 1, 3), w_up,
    )
    shapes = [result.shape for result in results]
    count = len(shapes)
    done = pl.pallas_call(
        deliver,
        out_shape=[shaped(*shape) for shape in shapes],
        in_specs=[anywhere] * count,
        out_specs=[anywhere] * count,
        scratch_shapes=[pltpu.VMEM(shape, F32) for shape in shapes]
        + [pltpu.SemaphoreType.DMA((count,))] * 2,
        compiler_params=pltpu.CompilerParams(vmem_limit_bytes=67043328),
        name="deliver",
    )(*results)
    return (*done[:4], done[4].transpose(0, 2, 1, 3), *done[5:])


def solution(mesh):
    rows = P("wide", "narrow")
    vector2 = P(None, None, "narrow")
    vector = P(None, "narrow")
    down_cols = P(None, "narrow", "wide")
    up_rows = P(None, "wide", "narrow")
    qkv = P(None, "wide", None, "narrow")
    return jax.shard_map(
        functools.partial(body, mesh.shape["wide"]),
        mesh=mesh,
        in_specs=(
            rows, vector2, vector2, qkv, vector2, down_cols, vector, up_rows, vector, down_cols,
            vector, rows,
        ),
        out_specs=(
            rows, rows, vector2, vector2, qkv, vector2, down_cols, vector, up_rows, vector,
            down_cols, vector,
        ),
        check_vma=False,
    )
```

```python
import functools
import math

import jax
import jax.numpy as jnp
from jax import lax
from jax.experimental import pallas as pl
from jax.experimental.pallas import tpu as pltpu
from jax.sharding import PartitionSpec as P

D = 1024
HEAD_DIM = 64
SEQ = 197
LAYERS = 2
EPS = 1e-06
ROWS = 208
KEYS = 256
MESH = pl.DeviceIdType.MESH
F32 = jnp.float32
BF16 = jnp.bfloat16
CHUNK = 16
HIGHEST = lax.Precision.HIGHEST

V_GAIN, V_BIAS, V_OUT, V_DOWN = 0, 2, 4, 5
V_QV, V_UP = 0, 2
V_ROWS = 8
G_GAIN, G_BIAS, G_OUT, G_DOWN = 0, 4, 8, 10
G_ROWS = 16


def dot(a, b):
    return lax.dot_general(a, b, (((1,), (0,)), ((), ())), preferred_element_type=F32)


def dot_t(a, b):
    return lax.dot_general(a, b, (((1,), (1,)), ((), ())), preferred_element_type=F32)


def t_dot(a, b):
    return lax.dot_general(a, b, (((0,), (0,)), ((), ())), preferred_element_type=F32)


def exact_dot(a, b, dims):
    return lax.dot_general(a, b, (dims, ((), ())), precision=HIGHEST, preferred_element_type=F32)


def when(condition):
    return pl.when(condition)


def scratch_of(half, per_row, width, hidden, images):
    tall = images * ROWS
    dma = pltpu.SemaphoreType.DMA
    vm = pltpu.VMEM
    return dict(
        wq=vm((LAYERS, 3, D, width), BF16),
        wp=vm((LAYERS, D, width), BF16),
        wf=vm((LAYERS, D, 2 * hidden), BF16),
        gq=vm((3, D, width), BF16),
        go=vm((D, width), BF16),
        gf=vm((D, 2 * hidden), BF16),
        pq=vm((LAYERS * half, 3, per_row, width), BF16),
        po=vm((LAYERS * half, per_row, width), BF16),
        pf=vm((half, per_row, 2 * hidden), BF16),
        cq=vm((LAYERS * half, 3, per_row, width), BF16),
        co=vm((LAYERS * half, per_row, width), BF16),
        cf=vm((half, per_row, 2 * hidden), BF16),
        e=vm((2 * LAYERS, tall, D), BF16),
        act=vm((2 * LAYERS, tall, D), BF16),
        q=vm((LAYERS, tall, width), BF16),
        k=vm((LAYERS, images * KEYS, width), BF16),
        v=vm((LAYERS, images * KEYS, width), BF16),
        o=vm((LAYERS, tall, width), BF16),
        prob=vm((LAYERS * images * (width // HEAD_DIM), ROWS, KEYS), F32),
        slope=vm((LAYERS, tall, hidden), F32),
        u=vm((LAYERS, tall, hidden), BF16),
        n=vm((2 * LAYERS, tall, 2 * width), F32),
        spread=vm((2 * LAYERS, tall, 1), F32),
        centre=vm((tall, 1), F32),
        r=vm((tall, 2 * width), F32),
        g=vm((tall, 2 * width), F32),
        f=vm((tall, hidden), BF16),
        d=vm((tall, 3 * width), BF16),
        do=vm((ROWS, width), BF16),
        tmp=vm((ROWS, width), F32),
        stage=vm((2, images, 4, ROWS, width), BF16),
        slot=vm((2, images, 6, ROWS, width), BF16),
        held=vm((images, 2, ROWS, width), F32),
        own=vm((2, images, 2, ROWS, width), F32),
        vs=vm((2, KEYS, 128), F32),
        ts=vm((images, 8, KEYS), F32),
        tr=vm((images, 3, 8, KEYS), F32),
        gb=vm((G_ROWS, width), F32),
        gn=vm((4, G_ROWS, width), F32),
        rq=vm((3, per_row, width), F32),
        ro=vm((width, per_row), F32),
        ru=vm((per_row, hidden), F32),
        rd=vm((hidden, per_row), F32),
        wo=vm((LAYERS, per_row, width), BF16),
        wd=vm((LAYERS, per_row, hidden), BF16),
        sh=vm((LAYERS, 2, 8, width), F32),
        rh=vm((LAYERS, 2 * half, 8, width), F32),
        sv=vm((LAYERS, V_ROWS, width), F32),
        rv=vm((LAYERS, 2 * half, V_ROWS, width), F32),
        a0_s=dma((2, images, 4)),
        a0_r=dma((2, images, 3)),
        ag_s=dma((4, images, 6)),
        ag_r=dma((4, images, 4)),
        rs_s=dma((2, images, 4)),
        rs_r=dma((2, images, 6)),
        t_s=dma((images, 2)),
        t_r=dma((images, 3)),
        gn_s=dma((3,)),
        gn_r=dma((3,)),
        h_s=dma((LAYERS, 2, 2 * half)),
        h_r=dma((LAYERS, 2 * half)),
        fin_s=dma((2, images)),
        fin_r=dma((2, images)),
        w_l=dma((LAYERS, 4)),
        w_s=dma((LAYERS, 4, half)),
        w_r=dma((LAYERS, 4, half)),
        w_f=dma((LAYERS, 4, half)),
        w_g=dma((LAYERS, 4, half)),
        p_s=dma((3, half)),
        p_r=dma((LAYERS, 3, half)),
        c_s=dma((3, half)),
        c_r=dma((LAYERS, 3, half)),
        r_s=dma((LAYERS, 4)),
        v_s=dma((LAYERS, 2 * half)),
        v_r=dma((LAYERS, 2 * half)),
    )


IN_NAMES = (
    "x_in", "cot_in", "ng_in", "nb_in", "bq_in", "bo_in", "bu_in", "bd_in", "wo_in", "wd_in",
    "wq_in", "wu_in",
)
OUT_NAMES = (
    "out", "gin", "gng", "gnb", "gwq", "gbqv", "gwo", "gbo", "gwu", "gbup", "gwd", "gbd",
)


def kernel(wide, images, width, hidden, names, *refs):
    R = dict(zip(names, refs))
    R["x"] = R["e"].at[0:2]
    half = wide // 2
    per_row = D // wide
    heads = width // HEAD_DIM
    w = lax.axis_index("wide")
    z = lax.axis_index("narrow")
    upper = z // 2
    mate = z + 1 - 2 * (z % 2)
    oi = 2 - upper
    oo = 3 * (1 - upper)
    inner_n = (z + upper) % 2
    inner = inner_n == 1
    outer = inner_n == 0
    far = 2 - inner_n
    near_half = 2 * upper
    far_half = 2 - near_half
    inside = z % 2
    half_cols = pl.ds(pl.multiple_of(near_half * width, 128), 2 * width)
    par = w % 2
    mine = w // 2
    partner = w + 1 - 2 * par

    def rows(i):
        return pl.ds(i * ROWS, ROWS)

    def cols(j):
        return pl.ds(pl.multiple_of(j * width, 128), width)

    def block_rows(j):
        return pl.ds(pl.multiple_of(j * width, 128), width)

    def wrows(j):
        return pl.ds(pl.multiple_of(j * per_row, per_row), per_row)

    def remote(src, dst, s, r, wide_id, narrow_id):
        return pltpu.make_async_remote_copy(
            src_ref=src, dst_ref=dst, send_sem=s, recv_sem=r,
            device_id=(wide_id, narrow_id), device_id_type=MESH,
        )

    def chunks(count, body, unroll=False):
        lax.fori_loop(
            0, count // CHUNK, lambda c, _: (body(c * CHUNK), 0)[1], 0, unroll=unroll
        )

    def at(i, start, size=CHUNK):
        return pl.ds(pl.multiple_of(i * ROWS + start, CHUNK), size)

    def a0_copy(buf, kind, i, block, s, r, to):
        part = buf.at[rows(i), cols(block)]
        return remote(part, part, R["a0_s"].at[kind, i, s], R["a0_r"].at[kind, i, r], w, to)

    def a0_start(buf, kind, i):
        a0_copy(buf, kind, i, z, 1, far, oi).start()
        a0_copy(buf, kind, i, z, 0, 0, mate).start()

    def a0_relay(buf, kind, i):
        @when(inner)
        def _():
            for r, block in ((1, oi), (2, oo)):
                a0_copy(buf, kind, i, block, r + 1, r, mate).wait_recv()
                a0_copy(buf, kind, i, block, r + 1, r, mate).start()

    def a0_finish(buf, kind, i):
        a0_copy(buf, kind, i, mate, 0, 0, mate).wait_recv()

        @when(outer)
        def _():
            for r, block in ((1, oi), (2, oo)):
                a0_copy(buf, kind, i, block, r + 1, r, mate).wait_recv()

        a0_copy(buf, kind, i, z, 0, 0, mate).wait_send()
        a0_copy(buf, kind, i, z, 1, far, oi).wait_send()

        @when(inner)
        def _():
            for r, block in ((1, oi), (2, oo)):
                a0_copy(buf, kind, i, block, r + 1, r, mate).wait_send()

    def ag_copy(buf, kind, i, block, s, r, to):
        part = buf.at[rows(i), cols(block)]
        return remote(part, part, R["ag_s"].at[kind, i, s], R["ag_r"].at[kind, i, r], w, to)

    def ag_unit(buf, kind, i, u):
        ag_copy(buf, kind, i, near_half + u, u, u, oi).start()
        ag_copy(buf, kind, i, near_half + u, 2 + u, 2 + u, mate).start()

    def ag_relay(buf, kind, i):
        @when(inner)
        def _():
            for u in range(2):
                ag_copy(buf, kind, i, far_half + u, 4 + u, u, mate).wait_recv()
                ag_copy(buf, kind, i, far_half + u, 4 + u, u, mate).start()

    def ag_finish(buf, kind, i):
        @when(outer)
        def _():
            for u in range(2):
                ag_copy(buf, kind, i, near_half + u, 2 + u, 2 + u, mate).wait_recv()
            for u in range(2):
                ag_copy(buf, kind, i, far_half + u, 4 + u, u, mate).wait_recv()

    def ag_drain(buf, kind, i):
        @when(inner)
        def _():
            for u in range(2):
                ag_copy(buf, kind, i, near_half + u, u, u, oi).wait_send()
                ag_copy(buf, kind, i, near_half + u, 2 + u, 2 + u, mate).wait_send()
                ag_copy(buf, kind, i, far_half + u, 4 + u, u, mate).wait_send()

    def rs_copy(bank, i, q, slot, to):
        return remote(
            R["stage"].at[bank, i, q], R["slot"].at[bank, i, slot],
            R["rs_s"].at[bank, i, q], R["rs_r"].at[bank, i, slot], w, to,
        )

    def rs_blocks(bank, i, block):
        for q in range(4):
            y = block((far_half if q < 2 else near_half) + q % 2)

            @when(outer)
            def _():
                R["stage"][bank, i, q] = y.astype(BF16)
                rs_copy(bank, i, q, q, mate).start()

            @when(inner)
            def _():
                if q < 2:
                    R["held"][i, q] = y
                else:
                    R["own"][bank, i, q - 2] = y

    def rs_relay(bank, i):
        @when(inner)
        def _():
            for q in range(2):
                rs_copy(bank, i, q, q, mate).wait_recv()

                def body(c):
                    part = pl.ds(pl.multiple_of(c, CHUNK), CHUNK)
                    total = R["held"][i, q, part] + R["slot"][bank, i, q, part].astype(F32)
                    R["stage"][bank, i, q, part] = total.astype(BF16)

                chunks(ROWS, body, True)
                rs_copy(bank, i, q, 4 + q, oi).start()

    def rs_unit(bank, i, u):
        rs_copy(bank, i, 2 + u, 2 + u, mate).wait_recv()
        rs_copy(bank, i, u, 4 + u, oi).wait_recv()

    def rs_drain(bank, i):
        @when(inner)
        def _():
            for q in range(2):
                rs_copy(bank, i, q, 4 + q, oi).wait_send()

        @when(outer)
        def _():
            for q in range(4):
                rs_copy(bank, i, q, q, mate).wait_send()

    def rs_sum(bank, i, u, part):
        slots = R["slot"]
        return (
            R["own"][bank, i, u, part]
            + slots[bank, i, 2 + u, part].astype(F32)
            + slots[bank, i, 4 + u, part].astype(F32)
        )

    def t_copy(i, q, r, to):
        return remote(
            R["ts"].at[i], R["tr"].at[i, r], R["t_s"].at[i, q], R["t_r"].at[i, r], w, to
        )

    def t_send(i):
        lane = lax.broadcasted_iota(jnp.int32, (8, 128), 0)
        first = jnp.where(lane < 4, 1.0, 0.0).astype(F32)
        second = 1.0 - first
        R["ts"][i] = exact_dot(first, R["vs"][0], ((1,), (1,))) + exact_dot(
            second, R["vs"][1], ((1,), (1,))
        )
        @when(outer)
        def _():
            t_copy(i, 0, 0, mate).start()

        t_copy(i, 1, far, oi).start()

    def t_total(i):
        for q in range(3):
            t_copy(i, 0, q, mate).wait_recv()
        total = (R["ts"][i] + R["tr"][i, 0]) + (R["tr"][i, 1] + R["tr"][i, 2])
        row = lax.broadcasted_iota(jnp.int32, (8, 128), 0)
        lane = lax.broadcasted_iota(jnp.int32, (8, 128), 1)
        pick = ((row == 0) & (lane < 64)) | ((row == 4) & (lane >= 64))
        R["vs"][0] = exact_dot(total, jnp.where(pick, 1.0, 0.0).astype(F32), ((0,), (0,)))

    def t_drain(i):
        @when(outer)
        def _():
            t_copy(i, 0, 0, mate).wait_send()

        t_copy(i, 1, far, oi).wait_send()

    def weights(l, piece):
        if piece == 0:
            return R["wq"].at[l], R["wq_in"].at[l]
        if piece == 1:
            return R["wp"].at[l], R["wo"].at[l]
        if piece == 2:
            return R["wf"].at[l, :, 0:hidden], R["wu_in"].at[l]
        return R["wf"].at[l, :, hidden : 2 * hidden], R["wd"].at[l]

    def rows_of(ref, k):
        return ref.at[wrows(k)] if len(ref.shape) == 2 else ref.at[:, wrows(k)]

    def w_local(l, piece):
        full, shard = weights(l, piece)
        return pltpu.make_async_copy(shard, rows_of(full, w), R["w_l"].at[l, piece])

    def w_send(l, piece, s, to):
        full, shard = weights(l, piece)
        return remote(
            shard, rows_of(full, w), R["w_s"].at[l, piece, s], R["w_r"].at[l, piece, mine], to, z
        )

    def w_pair(l, piece):
        full, shard = weights(l, piece)
        return remote(
            shard, rows_of(full, w),
            R["w_s"].at[l, piece, half - 1], R["w_f"].at[l, piece, mine], partner, z,
        )

    def w_cross(l, piece, k, parity):
        full, _ = weights(l, piece)
        part = rows_of(full, 2 * k + parity)
        return remote(
            part, part, R["w_g"].at[l, piece, k], R["w_f"].at[l, piece, k], partner, z
        )

    def w_start(l, piece):
        for j in range(1, half):
            w_send(l, piece, j - 1, 2 * ((mine + j) % half) + par).start()
        w_pair(l, piece).start()
        w_local(l, piece).start()

    def w_relay(l, piece):
        full, shard = weights(l, piece)
        for j in range(1, half):
            k = (mine + half - j) % half
            remote(
                shard, rows_of(full, 2 * k + par),
                R["w_s"].at[l, piece, 0], R["w_r"].at[l, piece, k], partner, z,
            ).wait_recv()
            w_cross(l, piece, k, par).start()

    def w_finish(l, piece):
        for j in range(half):
            w_cross(l, piece, (mine + half - j) % half, 1 - par).wait_recv()
        w_local(l, piece).wait()
        for s in range(half - 1):
            w_send(l, piece, s, partner).wait_send()
        w_pair(l, piece).wait_send()
        for j in range(1, half):
            w_cross(l, piece, (mine + j) % half, par).wait_send()

    def grads(l, piece):
        if piece == 1:
            return R["gf"], R["pf"], R["cf"]
        room = pl.ds(l * half, half)
        if piece == 0:
            return R["gq"], R["pq"].at[room], R["cq"].at[room]
        return R["go"], R["po"].at[room], R["co"].at[room]

    def p_copy(l, piece, k):
        full, theirs, _ = grads(l, piece)
        return remote(
            rows_of(full, 2 * k + 1 - par), theirs.at[k],
            R["p_s"].at[piece, k], R["p_r"].at[l, piece, k], partner, z,
        )

    def c_copy(l, piece, k, source):
        full, _, came = grads(l, piece)
        return remote(
            rows_of(full, 2 * k + par), came.at[source],
            R["c_s"].at[piece, k], R["c_r"].at[l, piece, source], 2 * k + par, z,
        )

    def r_copies(l, piece):
        pairs = (
            ((R["rq"], R["gwq"]),),
            ((R["ru"], R["gwu"]), (R["rd"], R["gwd"])),
            ((R["ro"], R["gwo"]),),
        )[piece]
        return [
            pltpu.make_async_copy(total, result.at[l], R["r_s"].at[l, piece + 2 * q])
            for q, (total, result) in enumerate(pairs)
        ]

    def g_start(l, piece, b):
        pairs = half * 256 // D
        for k in range(pairs):
            p_copy(l, piece, b * pairs + k).start()

    def g_mid(l, piece):
        full, theirs, _ = grads(l, piece)
        for j in range(1, half + 1):
            k = (mine + j) % half
            p_copy(l, piece, k).wait_recv()

            def body(c):
                here = pl.ds(pl.multiple_of((2 * k + par) * per_row + c, CHUNK), CHUNK)
                part = pl.ds(pl.multiple_of(c, CHUNK), CHUNK)
                ours = full.at[:, here] if piece == 0 else full.at[here]
                other = theirs.at[k, :, part] if piece == 0 else theirs.at[k, part]
                ours[...] = (ours[...].astype(F32) + other[...].astype(F32)).astype(BF16)

            chunks(per_row, body)
            if j < half:
                c_copy(l, piece, k, mine).start()

    def g_end(l, piece):
        full, _, came = grads(l, piece)
        for j in range(1, half):
            k = (mine + half - j) % half
            c_copy(l, piece, k, k).wait_recv()

        @when(l < LAYERS - 1)
        def _():
            for copy in r_copies(l + 1, piece):
                copy.wait()

        others = [(mine + j) % half for j in range(1, half)]
        if piece != 2:
            def body(c):
                part = pl.ds(pl.multiple_of(c, CHUNK), CHUNK)
                here = pl.ds(pl.multiple_of(w * per_row + c, CHUNK), CHUNK)
                if piece == 0:
                    total = full[:, here].astype(F32)
                    for k in others:
                        total = total + came[k, :, part].astype(F32)
                    R["rq"][:, part] = total
                else:
                    total = full[here, 0:hidden].astype(F32)
                    for k in others:
                        total = total + came[k, part, 0:hidden].astype(F32)
                    R["ru"][part] = total

            chunks(per_row, body)
        if piece != 0:
            first = hidden if piece == 1 else 0
            result = R["rd"] if piece == 1 else R["ro"]
            for c in range(0, result.shape[0], 256):
                lanes = slice(first + c, first + c + 256)
                total = full[wrows(w), lanes].astype(F32)
                for k in others:
                    total = total + came[k, :, lanes].astype(F32)
                result[c : c + 256] = total.T
        for copy in r_copies(l, piece):
            copy.start()
        for k in range(half):
            p_copy(l, piece, k).wait_send()
        for j in range(1, half):
            c_copy(l, piece, (mine + j) % half, mine).wait_send()

    def v_copy(l, j, source):
        to = (w + j) % wide
        return remote(
            R["sv"].at[l], R["rv"].at[l, source],
            R["v_s"].at[l, j], R["v_r"].at[l, source], to, z,
        )

    def h_copy(l, j, source, to_mate):
        to = (w + j) % wide
        block, narrow = (1 - inside, mate) if to_mate else (inside, z)
        return remote(
            R["sh"].at[l, block], R["rh"].at[l, source],
            R["h_s"].at[l, 1 if to_mate else 0, j], R["h_r"].at[l, source], to, narrow,
        )

    def v_start(l):
        for j in range(1, wide):
            v_copy(l, j, w).start()

    def h_start(l):
        @when(inner)
        def _():
            for j in range(wide):
                if j > 0:
                    h_copy(l, j, w, False).start()
                h_copy(l, j, w, True).start()
            R["rh"][l, w] = R["sh"][l, inside]

    def v_end(l):
        total = R["sv"][l]
        for j in range(1, wide):
            source = (w + j) % wide
            v_copy(l, j, source).wait_recv()
            total = total + R["rv"][l, source]
        R["gbqv"][l] = total[0:2]
        for b in range(hidden // width):
            R["gbup"][pl.ds(l, 1), b * width : (b + 1) * width] = total[2 + b : 3 + b]
        for j in range(1, wide):
            v_copy(l, j, w).wait_send()

    def h_end(l):
        @when(outer)
        def _():
            h_copy(l, 0, w, True).wait_recv()

        total = R["rh"][l, w]
        for j in range(1, wide):
            source = (w + j) % wide
            h_copy(l, j, source, True).wait_recv()
            total = total + R["rh"][l, source]
        R["gng"][l] = total[V_GAIN : V_GAIN + 2]
        R["gnb"][l] = total[V_BIAS : V_BIAS + 2]
        R["gbo"][pl.ds(l, 1)] = total[V_OUT : V_OUT + 1]
        R["gbd"][pl.ds(l, 1)] = total[V_DOWN : V_DOWN + 1]

        @when(inner)
        def _():
            for j in range(wide):
                if j > 0:
                    h_copy(l, j, w, False).wait_send()
                h_copy(l, j, w, True).wait_send()

    def norm_in(buf, l, branch, i):
        at_norm = 2 * l + branch
        scale = [R["gn"][j, pl.ds(G_GAIN + at_norm, 1)] for j in range(4)]
        shift = [R["gn"][j, pl.ds(G_BIAS + at_norm, 1)] for j in range(4)]
        scale = jnp.concatenate(scale, axis=1)
        shift = jnp.concatenate(shift, axis=1)

        def body(c):
            here = at(i, c)
            raw = buf[here, :].astype(F32)
            mean = jnp.sum(raw, axis=1, keepdims=True) * (1.0 / D)
            square = jnp.sum(raw * raw, axis=1, keepdims=True) * (1.0 / D)
            s = lax.rsqrt(square - mean * mean + EPS)
            R["act"][at_norm, here] = ((raw - mean) * s * scale + shift).astype(BF16)
            R["centre"][here] = R["centre"][here] + mean
            R["spread"][at_norm, here] = s

        chunks(ROWS, body, True)

    def norm_keep(l, branch, i):
        at_norm = 2 * l + branch

        @when(inner)
        def _():
            def body(c):
                here = at(i, c)
                R["n"][at_norm, here] = (R["r"][here] - R["centre"][here]) * R["spread"][
                    at_norm, here
                ]

            chunks(ROWS, body, True)

    def norm_back(bank, l, branch, i, buf, kind):
        at_norm = 2 * l + branch

        @when(inner)
        def _():
            t_total(i)
            for turn in range(2):
                u = turn
                if buf is None:
                    u = 1 - inside if turn == 0 else inside
                lanes = pl.ds(pl.multiple_of(u * width, 128), width)
                scale = R["gn"][near_half + u, pl.ds(G_GAIN + at_norm, 1)]
                rs_unit(bank, i, u)

                def body(c):
                    here = at(i, c)
                    part = pl.ds(pl.multiple_of(c, CHUNK), CHUNK)
                    upstream = rs_sum(bank, i, u, part)
                    R["own"][bank, i, u, part] = upstream
                    first = R["vs"][0, part, 0:1] * (1.0 / D)
                    second = R["vs"][0, part, 64:65] * (1.0 / D)
                    normed = R["n"][at_norm, here, lanes]
                    grown = R["g"][here, lanes] + (
                        upstream * scale - first - normed * second
                    ) * R["spread"][at_norm, here]
                    R["g"][here, lanes] = grown
                    if buf is not None:
                        buf[here, cols(near_half + u)] = grown.astype(BF16)

                chunks(ROWS, body, True)
                if buf is not None:
                    ag_unit(buf, kind, i, u)
                elif turn == 0:
                    fin_copy(1, i).start()

    def norm_sums(bank, l, branch, i, out_row):
        rs_drain(bank, i)
        t_drain(i)

        @when(inner)
        def _():
            for u in range(2):
                lanes = slice(u * width, (u + 1) * width)

                def body(c, carry):
                    c = c * CHUNK
                    here = at(i, c)
                    upstream = R["own"][bank, i, u, pl.ds(pl.multiple_of(c, CHUNK), CHUNK)]
                    normed = R["n"][2 * l + branch, here, lanes]
                    values = (upstream * normed, upstream, R["g"][here, lanes])
                    return tuple(
                        total + jnp.sum(value, axis=0, keepdims=True)
                        for total, value in zip(carry, values)
                    )

                zero = jnp.zeros((1, width), F32)
                sums = lax.fori_loop(0, ROWS // CHUNK, body, (zero,) * 3, unroll=True)
                small_add(l, u, V_GAIN + branch, sums[0])
                small_add(l, u, V_BIAS + branch, sums[1])
                if out_row is not None:
                    small_add(l, u, out_row, sums[2])

    def small_add(l, u, row, value):
        there = slice(row, row + 1)
        R["sh"][l, u, there] = R["sh"][l, u, there] + value

    def send_sums(at_norm, i, block_of):
        R["vs"][0, 0:ROWS] = jnp.zeros((ROWS, 128), F32)
        R["vs"][1, 0:ROWS] = jnp.zeros((ROWS, 128), F32)
        l, branch = at_norm

        def block(j):
            y = block_of(j)
            R["tmp"][...] = y
            scale = R["gn"][j, pl.ds(G_GAIN + 2 * l + branch, 1)]
            shift = R["gn"][j, pl.ds(G_BIAS + 2 * l + branch, 1)]

            def body(c):
                part = pl.ds(pl.multiple_of(c, CHUNK), CHUNK)
                value = R["tmp"][part]
                normed = R["act"][2 * l + branch, at(i, c), cols(j)].astype(F32) - shift
                first = value * scale
                second = value * normed
                for m in range(width // 128):
                    lanes = slice(m * 128, (m + 1) * 128)
                    R["vs"][0, part] = R["vs"][0, part] + first[:, lanes]
                    R["vs"][1, part] = R["vs"][1, part] + second[:, lanes]

            chunks(ROWS, body, True)
            return R["tmp"][...]

        return block

    factor = 1.0 / math.sqrt(HEAD_DIM)
    head_lanes = [slice(h * HEAD_DIM, (h + 1) * HEAD_DIM) for h in range(heads)]

    def attention(l, i):
        keys = pl.ds(i * KEYS, KEYS)
        column = lax.broadcasted_iota(jnp.int32, (ROWS, KEYS), 1)
        scores = [
            dot_t(R["q"][l, rows(i), lanes], R["k"][l, keys, lanes]) for lanes in head_lanes
        ]
        probs = []
        for h in range(heads):
            masked = jnp.where(column < SEQ, scores[h], -jnp.inf)
            top = jnp.max(masked, axis=1, keepdims=True)
            grown = jnp.exp(masked - top)
            prob = grown * (1.0 / jnp.sum(grown, axis=1, keepdims=True))
            R["prob"][(l * images + i) * heads + h] = prob
            probs.append(prob.astype(BF16))
        mixed = [dot(probs[h], R["v"][l, keys, head_lanes[h]]) for h in range(heads)]
        R["o"][l, rows(i)] = jnp.concatenate(mixed, axis=1).astype(BF16)

    def f1(l, i):
        buf = R["x"].at[0]

        @when(l > 0)
        def _():
            ag_finish(buf, 0, i)

        norm_in(buf, l, 0, i)
        act = R["act"].at[2 * l, rows(i)]
        kept = pl.ds(i * KEYS, ROWS)
        bq = R["bq_in"][l, 0:1]
        bv = R["bq_in"][l, 1:2]
        queries = (dot(act[...], R["wq"][l, 0]) + bq).astype(BF16).astype(F32) * factor
        R["q"][l, rows(i)] = queries.astype(BF16)
        R["k"][l, kept] = dot(act[...], R["wq"][l, 1]).astype(BF16)
        R["v"][l, kept] = (dot(act[...], R["wq"][l, 2]) + bv).astype(BF16)
        if i == 0:
            @when(l == 0)
            def _():
                w_relay(l, 1)

        attention(l, i)
        if i == 0:
            w_finish(l, 1)

        def block(j):
            return dot_t(R["o"][l, rows(i)], R["wp"][l, block_rows(j)])

        rs_blocks(0, i, block)
        norm_keep(l, 0, i)

    def f2(l, i):
        buf = R["x"].at[1]
        ag_finish(buf, 1, i)
        norm_in(buf, l, 1, i)

        def body(b, _):
            lanes = cols(b)
            pre = dot(R["act"][2 * l + 1, rows(i)], R["wf"][l, :, lanes])
            pre = pre + R["bu_in"][pl.ds(l, 1), lanes]
            cdf = 0.5 * (1.0 + lax.erf(pre * 0.7071067811865476))
            R["u"][l, rows(i), lanes] = (pre * cdf).astype(BF16)
            R["slope"][l, rows(i), lanes] = (
                cdf + pre * jnp.exp(-0.5 * pre * pre) * 0.3989422804014327
            )
            return 0

        lax.fori_loop(0, hidden // width, body, 0, unroll=True)
        if i == 0:
            w_finish(l, 3)

        def block(j):
            return dot_t(R["u"][l, rows(i)], R["wf"][l, block_rows(j), hidden : 2 * hidden])

        rs_blocks(1, i, block)
        norm_keep(l, 1, i)

    def residual(bank, i, bias_row, kind):
        @when(inner)
        def _():
            for u in range(2):
                lanes = slice(u * width, (u + 1) * width)
                bias = R["gn"][near_half + u, bias_row]
                rs_unit(bank, i, u)

                def body(c):
                    here = at(i, c)
                    part = pl.ds(pl.multiple_of(c, CHUNK), CHUNK)
                    grown = R["r"][here, lanes] + (rs_sum(bank, i, u, part) + bias)
                    R["r"][here, lanes] = grown
                    if kind is not None:
                        out = (grown - R["centre"][here]).astype(BF16)
                        R["x"][kind, here, cols(near_half + u)] = out

                chunks(ROWS, body, True)
                if kind is not None:
                    ag_unit(R["x"].at[kind], kind, i, u)

        rs_drain(bank, i)

    def fin_copy(which, i):
        source = (R["r"], R["g"])[which]
        there = pl.ds(pl.multiple_of((1 - inside) * width, 128), width)
        return remote(
            source.at[rows(i), there], R["held"].at[i, which],
            R["fin_s"].at[which, i], R["fin_r"].at[which, i], w, mate,
        )

    def fin_start(which, i):
        @when(inner)
        def _():
            fin_copy(which, i).start()

    def fin_end(which, i):
        source, result = ((R["r"], R["out"]), (R["g"], R["gin"]))[which]
        there = pl.ds(i * SEQ, SEQ)

        @when(inner)
        def _():
            here = pl.ds(pl.multiple_of(inside * width, 128), width)
            result[there] = source[pl.ds(i * ROWS, SEQ), here]
            fin_copy(which, i).wait_send()

        @when(outer)
        def _():
            fin_copy(which, i).wait_recv()
            result[there] = R["held"][i, which, 0:SEQ]

    def post_f1(l, i):
        @when(l > 0)
        def _():
            ag_drain(R["x"].at[0], 0, i)

        residual(0, i, pl.ds(G_OUT + l, 1), 1)

    def post_f2(l, i, last):
        ag_drain(R["x"].at[1], 1, i)
        residual(1, i, pl.ds(G_DOWN + l, 1), None if last else 0)
        if last:
            fin_start(0, i)

    def b2(l, i):
        e = R["e"].at[2 * l + 1]

        @when(l < LAYERS - 1)
        def _():
            ag_finish(e, 2, i)

        def body(b, _):
            lanes = cols(b)
            back = pl.ds(pl.multiple_of(hidden + b * width, 128), width)
            dz = dot(e[rows(i), :], R["wf"][l, :, back]) * R["slope"][l, rows(i), lanes]
            R["f"][rows(i), lanes] = dz.astype(BF16)
            row = pl.ds(V_UP + b, 1)
            R["sv"][l, row] = R["sv"][l, row] + jnp.sum(dz, axis=0, keepdims=True)
            return 0

        lax.fori_loop(0, hidden // width, body, 0, unroll=True)

        def block(j):
            return dot_t(R["f"][rows(i)], R["wf"][l, block_rows(j), 0:hidden])

        rs_blocks(0, i, send_sums((l, 1), i, block))
        t_send(i)
        add_down(l, i)

    def b1(l, i):
        e = R["e"].at[2 * l]
        ag_finish(e, 3, i)
        keys = pl.ds(i * KEYS, KEYS)
        R["do"][...] = dot(e[rows(i), :], R["wp"][l]).astype(BF16)
        if i == images - 1:
            grad_out(l)
        dos = [R["do"][:, lanes] for lanes in head_lanes]
        dps = [dot_t(dos[h], R["v"][l, keys, head_lanes[h]]) for h in range(heads)]
        dvs, dss = [], []
        for h in range(heads):
            prob = R["prob"][(l * images + i) * heads + h]
            dvs.append(t_dot(prob.astype(BF16), dos[h])[0:ROWS])
            delta = jnp.sum(prob * dps[h], axis=1, keepdims=True)
            dss.append((prob * (dps[h] - delta)).astype(BF16))
        dqs = [dot(dss[h], R["k"][l, keys, head_lanes[h]]) * factor for h in range(heads)]
        dks = [t_dot(dss[h], R["q"][l, rows(i), head_lanes[h]])[0:ROWS] for h in range(heads)]
        dq, dk, dv = [jnp.concatenate(parts, axis=1) for parts in (dqs, dks, dvs)]
        for part, value in ((0, dq), (1, dk), (2, dv)):
            R["d"][rows(i), part * width : (part + 1) * width] = value.astype(BF16)
        for row, value in ((V_QV, dq), (V_QV + 1, dv)):
            there = slice(row, row + 1)
            R["sv"][l, there] = R["sv"][l, there] + jnp.sum(value, axis=0, keepdims=True)

        def block(j):
            parts = [
                dot_t(R["d"][rows(i), m * width : (m + 1) * width], R["wq"][l, m, block_rows(j)])
                for m in range(3)
            ]
            return parts[0] + parts[1] + parts[2]

        rs_blocks(1, i, send_sums((l, 0), i, block))
        t_send(i)

    def add_down(l, i):
        @when(inner)
        def _():
            for u in range(2):
                lanes = slice(u * width, (u + 1) * width)

                def body(c, total):
                    value = R["g"][at(i, c * CHUNK), lanes]
                    return total + jnp.sum(value, axis=0, keepdims=True)

                zero = jnp.zeros((1, width), F32)
                total = lax.fori_loop(0, ROWS // CHUNK, body, zero, unroll=True)
                small_add(l, u, V_DOWN, total)

    def post_b2(l, i):
        @when(l < LAYERS - 1)
        def _():
            ag_drain(R["e"].at[2 * l + 1], 2, i)

        norm_back(0, l, 1, i, R["e"].at[2 * l], 3)
        norm_sums(0, l, 1, i, V_OUT)

    def post_b1(l, i):
        ag_drain(R["e"].at[2 * l], 3, i)

        @when(l > 0)
        def _():
            norm_back(1, l, 0, i, R["e"].at[2 * l - 1], 2)

        @when(l == 0)
        def _():
            norm_back(1, l, 0, i, None, None)

        norm_sums(1, l, 0, i, None)

    def grad_block(b):
        block = (mine * 2 * per_row // 256 + 1 + b) % (D // 256)
        return block, pl.ds(pl.multiple_of(block * 256, 256), 256)

    def grad_ffn(l, first, last):
        def body(b, _):
            block, lanes = grad_block(b)
            up = t_dot(R["act"][2 * l + 1, :, lanes], R["f"][...])
            R["gf"][lanes, 0:hidden] = up.astype(BF16)
            down = t_dot(R["e"][2 * l + 1, :, lanes], R["u"][l])
            R["gf"][lanes, hidden : 2 * hidden] = down.astype(BF16)
            g_start(l, 1, block)
            return 0

        lax.fori_loop(first, last, body, 0)

    def grad_qkv(l):
        def body(b, _):
            block, lanes = grad_block(b)
            qkv = t_dot(R["act"][2 * l, :, lanes], R["d"][...])
            for m in range(3):
                R["gq"][m, lanes] = qkv[:, m * width : (m + 1) * width].astype(BF16)
            g_start(l, 0, block)
            return 0

        lax.fori_loop(0, D // 256, body, 0)

    def grad_out(l):
        def body(b, _):
            block, lanes = grad_block(b)
            out = t_dot(R["e"][2 * l, :, lanes], R["o"][l])
            R["go"][lanes] = out.astype(BF16)
            g_start(l, 2, block)
            return 0

        lax.fori_loop(0, D // 256, body, 0)

    def spread_rows(source, result):
        tokens = images * SEQ
        wide_rows = R["r"].at[:, 0:width]
        wide_rows[0:tokens] = source[...].astype(F32)
        row = lax.broadcasted_iota(jnp.int32, (ROWS, width), 0)
        for i in image:
            part = wide_rows[i * SEQ : i * SEQ + ROWS]
            result[rows(i), cols(z)] = jnp.where(row < SEQ, part, 0.0).astype(BF16)

    barrier = pltpu.get_barrier_semaphore()
    for j in range(1, wide):
        pl.semaphore_signal(barrier, 1, device_id=((w + j) % wide, z), device_id_type=MESH)
    for j in range(1, 4):
        pl.semaphore_signal(barrier, 1, device_id=(w, (z + j) % 4), device_id_type=MESH)
    image = range(images)
    first_x = R["x"].at[0]
    last_e = R["e"].at[2 * LAYERS - 1]
    R["r"][...] = jnp.zeros_like(R["r"])
    spread_rows(R["x_in"], first_x)
    for l in range(LAYERS):
        R["gb"][G_GAIN + 2 * l : G_GAIN + 2 * l + 2] = R["ng_in"][l]
        R["gb"][G_BIAS + 2 * l : G_BIAS + 2 * l + 2] = R["nb_in"][l]
    R["gb"][G_OUT : G_OUT + LAYERS] = R["bo_in"][...]
    R["gb"][G_DOWN : G_DOWN + LAYERS] = R["bd_in"][...]
    R["gn"][z] = R["gb"][...]
    for l in range(LAYERS):
        R["wo"][l] = R["wo_in"][l].T
    pl.semaphore_wait(barrier, 3 + wide - 1)

    w_start(0, 0)
    for i in image:
        a0_start(first_x, 0, i)

    def gn_copy(q, r, to):
        return remote(R["gb"], R["gn"].at[z], R["gn_s"].at[q], R["gn_r"].at[r], w, to)

    gn_copy(0, 0, mate).start()
    gn_copy(1, far, oi).start()
    gn_copy(2, far, oo).start()
    w_start(0, 1)
    for l in range(LAYERS):
        R["wd"][l] = R["wd_in"][l].T
    spread_rows(R["cot_in"], last_e)
    R["centre"][...] = jnp.zeros_like(R["centre"])
    R["sv"][...] = jnp.zeros_like(R["sv"])
    R["sh"][...] = jnp.zeros_like(R["sh"])
    R["vs"][...] = jnp.zeros_like(R["vs"])
    for name in ("k", "v"):
        for i in image:
            empty = jnp.zeros((LAYERS, KEYS - ROWS, width), BF16)
            R[name][:, i * KEYS + ROWS : (i + 1) * KEYS] = empty
    for i in image:
        a0_relay(first_x, 0, i)
    for i in image:
        a0_start(last_e, 1, i)
    w_start(0, 2)
    w_start(0, 3)
    for l in range(1, LAYERS):
        for piece in range(4):
            w_start(l, piece)
    for q in range(3):
        gn_copy(q, q, mate).wait_recv()
    for q in range(3):
        gn_copy(q, q, mate).wait_send()
    w_relay(0, 0)

    def arrived(i):
        a0_finish(first_x, 0, i)

        @when(inner)
        def _():
            R["r"][rows(i)] = first_x[rows(i), half_cols].astype(F32)

    arrived(0)
    w_finish(0, 0)
    for i in image:
        a0_relay(last_e, 1, i)

    def forward(l, _):
        f1(l, 0)

        @when(l > 0)
        def _():
            ag_relay(R["x"].at[0], 0, 1)

        rs_relay(0, 0)

        @when(l == 0)
        def _():
            for i in range(1, images):
                arrived(i)

        f1(l, 1)
        post_f1(l, 0)
        w_relay(l, 2)
        rs_relay(0, 1)
        ag_relay(R["x"].at[1], 1, 0)
        w_relay(l, 3)
        post_f1(l, 1)
        w_finish(l, 2)
        f2(l, 0)
        ag_relay(R["x"].at[1], 1, 1)
        rs_relay(1, 0)
        f2(l, 1)

        @when(l < LAYERS - 1)
        def _():
            w_relay(l + 1, 0)
            post_f2(l, 0, False)
            rs_relay(1, 1)
            ag_relay(R["x"].at[0], 0, 0)
            w_relay(l + 1, 1)
            post_f2(l, 1, False)
            w_finish(l + 1, 0)

        return 0

    lax.fori_loop(0, LAYERS, forward, 0)
    for i in image:
        a0_finish(last_e, 1, i)

    @when(inner)
    def _():
        R["g"][...] = last_e[:, half_cols].astype(F32)

    def backward(step, _):
        l = LAYERS - 1 - step
        top = l == LAYERS - 1
        e2 = R["e"].at[2 * l + 1]
        e1 = R["e"].at[2 * l]
        b2(l, 0)

        @when(top)
        def _():
            post_f2(l, 0, True)
            rs_relay(1, 1)

        @when(l < LAYERS - 1)
        def _():
            ag_relay(e2, 2, 1)

        rs_relay(0, 0)
        b2(l, 1)

        @when(top)
        def _():
            post_f2(l, 1, True)

        grad_ffn(l, 0, 2)
        post_b2(l, 0)
        grad_ffn(l, 2, 4)
        rs_relay(0, 1)

        @when(l < LAYERS - 1)
        def _():
            g_end(l + 1, 0)
            g_end(l + 1, 2)
            v_end(l + 1)
            h_end(l + 1)

        g_mid(l, 1)
        ag_relay(e1, 3, 0)
        post_b2(l, 1)
        b1(l, 0)
        ag_relay(e1, 3, 1)
        rs_relay(1, 0)

        b1(l, 1)
        post_b1(l, 0)
        grad_qkv(l)
        g_mid(l, 2)
        g_mid(l, 0)
        rs_relay(1, 1)

        @when(l > 0)
        def _():
            ag_relay(R["e"].at[2 * l - 1], 2, 0)

        g_end(l, 1)
        v_start(l)
        post_b1(l, 1)
        h_start(l)
        return 0

    lax.fori_loop(0, LAYERS, backward, 0)
    first = jnp.int32(0)
    g_end(first, 2)
    v_end(0)
    for i in image:
        fin_end(0, i)
    g_end(first, 0)
    for i in image:
        fin_end(1, i)
    h_end(0)
    for piece in range(3):
        for copy in r_copies(0, piece):
            copy.wait()


def deliver(*refs):
    count = (len(refs) - 2) // 3
    sources, results, rooms = (refs[i * count : (i + 1) * count] for i in range(3))
    came, gone = refs[3 * count :]

    def copy(i, inward):
        if inward:
            return pltpu.make_async_copy(sources[i], rooms[i], came.at[i])
        return pltpu.make_async_copy(rooms[i], results[i], gone.at[i])

    for i in range(count):
        copy(i, True).start()
    for i in range(count):
        copy(i, True).wait()
        copy(i, False).start()
    for i in range(count):
        copy(i, False).wait()


def body(wide, inputs, norm_gain, norm_bias, w_qkv, b_qv, w_out, b_out, w_up, b_up, w_down, b_down, cotangent):
    tokens, width = inputs.shape
    images = tokens // SEQ
    hidden = w_up.shape[2]
    per_row = w_up.shape[1]
    half = wide // 2
    scratch = scratch_of(half, per_row, width, hidden, images)
    names = IN_NAMES + OUT_NAMES + tuple(scratch)
    vmem = pl.BlockSpec(memory_space=pltpu.VMEM)
    anywhere = pl.BlockSpec(memory_space=pl.ANY)

    def shaped(*shape):
        return jax.ShapeDtypeStruct(shape, F32)

    results = pl.pallas_call(
        functools.partial(kernel, wide, images, width, hidden, names),
        out_shape=(
            shaped(tokens, width),
            shaped(tokens, width),
            shaped(LAYERS, 2, width),
            shaped(LAYERS, 2, width),
            shaped(LAYERS, 3, per_row, width),
            shaped(LAYERS, 2, width),
            shaped(LAYERS, width, per_row),
            shaped(LAYERS, width),
            shaped(LAYERS, per_row, hidden),
            shaped(LAYERS, hidden),
            shaped(LAYERS, hidden, per_row),
            shaped(LAYERS, width),
        ),
        in_specs=[vmem] * 10 + [anywhere] * 2,
        out_specs=(
            vmem, vmem, vmem, vmem, anywhere, vmem, anywhere, vmem, anywhere, vmem, anywhere, vmem,
        ),
        scratch_shapes=list(scratch.values()),
        compiler_params=pltpu.CompilerParams(
            collective_id=0, has_side_effects=True, vmem_limit_bytes=67043328
        ),
        name="encoder_step",
    )(
        inputs, cotangent, norm_gain, norm_bias, b_qv, b_out, b_up, b_down, w_out, w_down,
        w_qkv.transpose(0, 2, 1, 3), w_up,
    )
    shapes = [result.shape for result in results]
    count = len(shapes)
    done = pl.pallas_call(
        deliver,
        out_shape=[shaped(*shape) for shape in shapes],
        in_specs=[anywhere] * count,
        out_specs=[anywhere] * count,
        scratch_shapes=[pltpu.VMEM(shape, F32) for shape in shapes]
        + [pltpu.SemaphoreType.DMA((count,))] * 2,
        compiler_params=pltpu.CompilerParams(vmem_limit_bytes=67043328),
        name="deliver",
    )(*results)
    return (*done[:4], done[4].transpose(0, 2, 1, 3), *done[5:])


def solution(mesh):
    rows = P("wide", "narrow")
    vector2 = P(None, None, "narrow")
    vector = P(None, "narrow")
    down_cols = P(None, "narrow", "wide")
    up_rows = P(None, "wide", "narrow")
    qkv = P(None, "wide", None, "narrow")
    return jax.shard_map(
        functools.partial(body, mesh.shape["wide"]),
        mesh=mesh,
        in_specs=(
            rows, vector2, vector2, qkv, vector2, down_cols, vector, up_rows, vector, down_cols,
            vector, rows,
        ),
        out_specs=(
            rows, rows, vector2, vector2, qkv, vector2, down_cols, vector, up_rows, vector,
            down_cols, vector,
        ),
        check_vma=False,
    )
```
